32 devices in a mesh: rep: 1 (over z), mp: 4 (over y), tok: 8 (over x, core).
Axes of the slice: x: 4, y: 4, z: 1, core: 2. Of those that a mesh axis runs over, the one named last changes fastest.
The devices are a block of a 4x4x8 slice.
Arguments:
- hidden_in: bfloat16 [32768, 768], P(('rep', 'tok', 'mp'))
- seg_ids: int32 [32768], P(('rep', 'tok', 'mp'))
- expert_ids: int32 [32768, 2], P(('rep', 'tok', 'mp'))
- expert_gates: float32 [32768, 2], P(('rep', 'tok', 'mp'))
- w_query: bfloat16 [2, 768, 12, 64], P(None, 'tok', 'mp')
- w_key: bfloat16 [2, 768, 12, 64], P(None, 'tok', 'mp')
- w_value: bfloat16 [2, 768, 12, 64], P(None, 'tok', 'mp')
- w_out: bfloat16 [2, 12, 64, 768], P(None, 'mp', None, 'tok')
- w_gate: bfloat16 [2, 8, 768, 3072], P(None, None, 'tok', 'mp')
- w_up: bfloat16 [2, 8, 768, 3072], P(None, None, 'tok', 'mp')
- w_down: bfloat16 [2, 8, 3072, 768], P(None, None, 'mp', 'tok')
- gain_attn: bfloat16 [2, 768], replicated
- gain_mlp: bfloat16 [2, 768], replicated
Outputs:
- output: float32 [32768, 768], P(('rep', 'tok', 'mp'))
All inputs are finite; a program needn't handle non-finite values.
Results may differ from the reference program's by a relative error of at most 0.0101596.
Values are sent between devices in bfloat16 or wider.
A program may use at most 768 MiB of HBM per device.

```python
import jax
import jax.numpy as jnp
from jax import lax

TOKENS = 32768
SHARDS = 8
HIDDEN = 768
FFN_WIDTH = 3072
Q_HEADS = 12
KV_HEADS = 12
HEAD_DIM = 64
EXPERTS = 8
NUM_LAYERS = 2
REQ_CUTS = 3

SHARD_LEN = TOKENS // SHARDS
QUERY_BLOCK = min(SHARD_LEN, 256)
EPS = 1e-5
ROPE_BASE = 10000.0


def normal_weight(key, shape, scale):
    return (jax.random.normal(key, shape, jnp.float32) * scale).astype(jnp.bfloat16)


def setup_inputs(seed: int = 0, part: int = 0) -> dict:
    base_key = jax.random.key(seed)
    part_keys = jax.random.split(jax.random.fold_in(base_key, part), 5)
    weight_keys = jax.random.split(jax.random.key(seed + 1), 9)
    hidden_in = jax.random.normal(part_keys[0], (TOKENS, HIDDEN), jnp.float32).astype(jnp.bfloat16)
    cut_points = jax.random.randint(part_keys[1], (SHARDS, 1, REQ_CUTS), 1, SHARD_LEN)
    token_pos = jnp.arange(SHARD_LEN, dtype=jnp.int32)[None, :, None]
    req_index = jnp.sum((token_pos >= cut_points).astype(jnp.int32), axis=-1)
    shard_base = jnp.arange(SHARDS, dtype=jnp.int32)[:, None] * (REQ_CUTS + 1)
    seg_ids = (shard_base + req_index).reshape(TOKENS).astype(jnp.int32)
    first_pick = jax.random.permutation(part_keys[2], jnp.arange(TOKENS, dtype=jnp.int32) % EXPERTS)
    pick_shift = jax.random.randint(part_keys[3], (TOKENS,), 1, EXPERTS)
    second_pick = (first_pick + pick_shift) % EXPERTS
    expert_ids = jnp.stack([first_pick, second_pick], axis=1).astype(jnp.int32)
    top_share = jax.random.uniform(part_keys[4], (TOKENS,), jnp.float32, 0.3, 0.9)
    expert_gates = jnp.stack([top_share, 1.0 - top_share], axis=1)
    qk_scale = 1.4 * HIDDEN ** -0.5
    return {
        'hidden_in': hidden_in,
        'seg_ids': seg_ids,
        'expert_ids': expert_ids,
        'expert_gates': expert_gates,
        'w_query': normal_weight(weight_keys[0], (NUM_LAYERS, HIDDEN, Q_HEADS, HEAD_DIM), qk_scale),
        'w_key': normal_weight(weight_keys[1], (NUM_LAYERS, HIDDEN, KV_HEADS, HEAD_DIM), qk_scale),
        'w_value': normal_weight(weight_keys[2], (NUM_LAYERS, HIDDEN, KV_HEADS, HEAD_DIM), HIDDEN ** -0.5),
        'w_out': normal_weight(weight_keys[3], (NUM_LAYERS, Q_HEADS, HEAD_DIM, HIDDEN), 2.0 * (Q_HEADS * HEAD_DIM) ** -0.5),
        'w_gate': normal_weight(weight_keys[4], (NUM_LAYERS, EXPERTS, HIDDEN, FFN_WIDTH), HIDDEN ** -0.5),
        'w_up': normal_weight(weight_keys[5], (NUM_LAYERS, EXPERTS, HIDDEN, FFN_WIDTH), HIDDEN ** -0.5),
        'w_down': normal_weight(weight_keys[6], (NUM_LAYERS, EXPERTS, FFN_WIDTH, HIDDEN), FFN_WIDTH ** -0.5),
        'gain_attn': jax.random.uniform(weight_keys[7], (NUM_LAYERS, HIDDEN), jnp.float32, 0.5, 1.5).astype(jnp.bfloat16),
        'gain_mlp': jax.random.uniform(weight_keys[8], (NUM_LAYERS, HIDDEN), jnp.float32, 0.5, 1.5).astype(jnp.bfloat16),
    }


def rms_norm(residual, gain):
    inv_rms = lax.rsqrt(jnp.mean(residual * residual, axis=-1, keepdims=True) + EPS)
    return (residual * inv_rms * gain.astype(jnp.float32)).astype(jnp.bfloat16)


def request_positions(seg_shard):
    token_index = jnp.arange(SHARD_LEN, dtype=jnp.int32)
    is_start = jnp.concatenate([jnp.ones((1,), dtype=jnp.bool_), seg_shard[1:] != seg_shard[:-1]])
    start_index = lax.cummax(jnp.where(is_start, token_index, 0), axis=0)
    return token_index - start_index


def apply_rope(vectors, positions):
    half_dim = HEAD_DIM // 2
    inv_freq = jnp.power(ROPE_BASE, -jnp.arange(half_dim, dtype=jnp.float32) * 2.0 / HEAD_DIM)
    angles = positions.astype(jnp.float32)[:, None, None] * inv_freq
    cosines = jnp.cos(angles)
    sines = jnp.sin(angles)
    first_half = vectors[..., :half_dim]
    second_half = vectors[..., half_dim:]
    return jnp.concatenate([first_half * cosines - second_half * sines, second_half * cosines + first_half * sines], axis=-1)


def shard_attention(h_shard, seg_shard, q_weight, k_weight, v_weight):
    groups = Q_HEADS // KV_HEADS
    positions = request_positions(seg_shard)
    q_proj = jnp.dot(h_shard, q_weight.reshape(HIDDEN, Q_HEADS * HEAD_DIM), preferred_element_type=jnp.float32)
    k_proj = jnp.dot(h_shard, k_weight.reshape(HIDDEN, KV_HEADS * HEAD_DIM), preferred_element_type=jnp.float32)
    v_proj = jnp.dot(h_shard, v_weight.reshape(HIDDEN, KV_HEADS * HEAD_DIM), preferred_element_type=jnp.float32)
    q_rot = apply_rope(q_proj.reshape(SHARD_LEN, Q_HEADS, HEAD_DIM), positions).astype(jnp.bfloat16)
    k_rot = apply_rope(k_proj.reshape(SHARD_LEN, KV_HEADS, HEAD_DIM), positions).astype(jnp.bfloat16)
    keys32 = k_rot.astype(jnp.float32)
    values32 = v_proj.astype(jnp.bfloat16).astype(jnp.float32).reshape(SHARD_LEN, KV_HEADS, HEAD_DIM)
    token_index = jnp.arange(SHARD_LEN, dtype=jnp.int32)
    num_blocks = SHARD_LEN // QUERY_BLOCK
    q_blocks = q_rot.reshape(num_blocks, QUERY_BLOCK, KV_HEADS, groups, HEAD_DIM)

    def one_block(block_in):
        q_block, seg_block, index_block = block_in
        scores = jnp.einsum('bhgd,shd->hgbs', q_block.astype(jnp.float32), keys32) * HEAD_DIM ** -0.5
        allowed = (seg_block[:, None] == seg_shard[None, :]) & (token_index[None, :] <= index_block[:, None])
        attn_prob = jax.nn.softmax(jnp.where(allowed, scores, -1e30), axis=-1)
        attn_prob = attn_prob.astype(jnp.bfloat16).astype(jnp.float32)
        attn_out = jnp.einsum('hgbs,shd->bhgd', attn_prob, values32)
        return attn_out.astype(jnp.bfloat16).reshape(QUERY_BLOCK, Q_HEADS * HEAD_DIM)

    block_outs = lax.map(one_block, (q_blocks, seg_shard.reshape(num_blocks, QUERY_BLOCK), token_index.reshape(num_blocks, QUERY_BLOCK)))
    return block_outs.reshape(SHARD_LEN, Q_HEADS * HEAD_DIM)


def expert_mix(normed, expert_ids, expert_gates, gate_weight, up_weight, down_weight):
    def one_expert(mix_sum, expert_in):
        gate_mat, up_mat, down_mat, expert_num = expert_in
        gate_pre = jnp.dot(normed, gate_mat, preferred_element_type=jnp.float32)
        up_pre = jnp.dot(normed, up_mat, preferred_element_type=jnp.float32)
        hidden_act = (jax.nn.silu(gate_pre) * up_pre).astype(jnp.bfloat16)
        down_out = jnp.dot(hidden_act, down_mat, preferred_element_type=jnp.float32)
        route_weight = jnp.sum(jnp.where(expert_ids == expert_num, expert_gates, 0.0), axis=1)
        return mix_sum + route_weight[:, None] * down_out, None

    start_sum = jnp.zeros((normed.shape[0], HIDDEN), jnp.float32)
    mix_sum, _ = lax.scan(one_expert, start_sum, (gate_weight, up_weight, down_weight, jnp.arange(EXPERTS, dtype=jnp.int32)))
    return mix_sum


def reference(hidden_in, seg_ids, expert_ids, expert_gates, w_query, w_key, w_value, w_out, w_gate, w_up, w_down, gain_attn, gain_mlp):
    seg_shards = seg_ids.reshape(SHARDS, SHARD_LEN)

    def one_layer(residual, layer_in):
        q_weight, k_weight, v_weight, o_weight, gate_weight, up_weight, down_weight, attn_gain, mlp_gain = layer_in
        normed = rms_norm(residual, attn_gain).reshape(SHARDS, SHARD_LEN, HIDDEN)
        attn_out = lax.map(lambda shard_in: shard_attention(shard_in[0], shard_in[1], q_weight, k_weight, v_weight), (normed, seg_shards))
        attn_out = attn_out.reshape(TOKENS, Q_HEADS * HEAD_DIM)
        residual = residual + jnp.dot(attn_out, o_weight.reshape(Q_HEADS * HEAD_DIM, HIDDEN), preferred_element_type=jnp.float32)
        normed = rms_norm(residual, mlp_gain)
        residual = residual + expert_mix(normed, expert_ids, expert_gates, gate_weight, up_weight, down_weight)
        return residual, None

    final, _ = lax.scan(one_layer, hidden_in.astype(jnp.float32), (w_query, w_key, w_value, w_out, w_gate, w_up, w_down, gain_attn, gain_mlp))
    return final
```

```python
import functools

import jax
import jax.numpy as jnp
from jax import lax
from jax.experimental import pallas as pl
from jax.experimental.pallas import tpu as pltpu
from jax.sharding import PartitionSpec as P


EPS = 1e-5
ROPE_BASE = 10000.0
NEG = -1e30
VMEM_LIMIT = 60 * 1024 * 1024
F32 = jnp.float32
BF16 = jnp.bfloat16
NT = (((1,), (1,)), ((), ()))


def rms_norm(residual, gain):
    inv_rms = lax.rsqrt(jnp.mean(residual * residual, axis=-1, keepdims=True) + EPS)
    return (residual * inv_rms * gain.astype(F32)).astype(BF16)


def request_starts(seg_rows):
    token_index = jnp.arange(seg_rows.shape[0], dtype=jnp.int32)
    is_start = jnp.concatenate([jnp.ones((1,), dtype=jnp.bool_), seg_rows[1:] != seg_rows[:-1]])
    return lax.cummax(jnp.where(is_start, token_index, 0), axis=0)


def attention_kernel(heads, head_dim, bounds_ref, h_ref, w_ref, cos_ref, sin_ref, start_ref, out_ref, q_sc, k_sc, v_sc, m_sc, l_sc, acc_sc):
    tile = pl.program_id(0)
    rows = h_ref.shape[0]
    width = heads * head_dim
    half = head_dim // 2
    qkv = lax.dot_general(w_ref[...], h_ref[...], NT, preferred_element_type=F32)
    cosines = cos_ref[...]
    sines = sin_ref[...]

    def rotate(base):
        first = qkv[base:base + half]
        second = qkv[base + half:base + head_dim]
        return jnp.concatenate([first * cosines - second * sines, second * cosines + first * sines], axis=0)

    scale = head_dim ** -0.5
    for head in range(heads):
        base = head * head_dim
        q_sc[head] = (rotate(base).astype(BF16).astype(F32) * scale).astype(BF16)
        k_sc[tile, head] = rotate(width + base).T.astype(BF16)
    v_sc[tile] = qkv[2 * width:3 * width].astype(BF16)
    m_sc[...] = jnp.full(m_sc.shape, NEG, F32)
    l_sc[...] = jnp.zeros(l_sc.shape, F32)
    acc_sc[...] = jnp.zeros(acc_sc.shape, F32)

    def block(key_tile, masked):
        if masked:
            key_index = key_tile * rows + lax.broadcasted_iota(jnp.int32, (rows, rows), 0)
            query_index = tile * rows + lax.broadcasted_iota(jnp.int32, (1, rows), 1)
            allowed = (key_index >= start_ref[...]) & (key_index <= query_index)
        for head in range(heads):
            scores = jnp.dot(k_sc[key_tile, head], q_sc[head], preferred_element_type=F32)
            if masked:
                scores = jnp.where(allowed, scores, NEG)
            old_max = m_sc[head]
            new_max = jnp.maximum(old_max, jnp.max(scores, axis=0, keepdims=True))
            prob = jnp.exp(scores - new_max)
            fade = jnp.exp(old_max - new_max)
            m_sc[head] = new_max
            l_sc[head] = fade * l_sc[head] + jnp.sum(prob, axis=0, keepdims=True)
            part = jnp.dot(v_sc[key_tile, head * head_dim:(head + 1) * head_dim], prob.astype(BF16), preferred_element_type=F32)
            acc_sc[head] = acc_sc[head] * fade + part

    def masked_step(key_tile, carry):
        block(key_tile, True)
        return carry

    def open_step(key_tile, carry):
        block(key_tile, False)
        return carry

    first_tile = bounds_ref[0, tile]
    open_tile = bounds_ref[1, tile]
    lax.fori_loop(first_tile, open_tile, masked_step, 0)
    lax.fori_loop(open_tile, tile, open_step, 0)
    block(tile, True)
    for head in range(heads):
        out_ref[0, head * head_dim:(head + 1) * head_dim] = (acc_sc[head] / l_sc[head]).astype(BF16)


def attention(normed, w_rows, cosines, sines, starts, parts, heads, head_dim, rows):
    seq_len, hidden = normed.shape
    tiles = seq_len // rows
    width = heads * head_dim
    per_part = tiles // parts
    first_start = starts[::rows]
    last_start = starts[rows - 1::rows]
    tile_index = jnp.arange(tiles, dtype=jnp.int32)
    bounds = jnp.stack([first_start // rows, jnp.minimum((last_start + rows - 1) // rows, tile_index)])
    grid_spec = pltpu.PrefetchScalarGridSpec(
        num_scalar_prefetch=1,
        grid=(tiles,),
        in_specs=[
            pl.BlockSpec((rows, hidden), lambda i, b: (i, 0)),
            pl.BlockSpec((3 * width, hidden), lambda i, b: (0, 0)),
            pl.BlockSpec((head_dim // 2, rows), lambda i, b: (0, i)),
            pl.BlockSpec((head_dim // 2, rows), lambda i, b: (0, i)),
            pl.BlockSpec((1, rows), lambda i, b: (0, i)),
        ],
        out_specs=pl.BlockSpec((1, width, rows), lambda i, b: (i // per_part, 0, i % per_part)),
        scratch_shapes=[
            pltpu.VMEM((heads, head_dim, rows), BF16),
            pltpu.VMEM((tiles, heads, rows, head_dim), BF16),
            pltpu.VMEM((tiles, width, rows), BF16),
            pltpu.VMEM((heads, 1, rows), F32),
            pltpu.VMEM((heads, 1, rows), F32),
            pltpu.VMEM((heads, head_dim, rows), F32),
        ],
    )
    flops = 2 * seq_len * hidden * 3 * width + 2 * seq_len * seq_len * width
    return pl.pallas_call(
        functools.partial(attention_kernel, heads, head_dim),
        grid_spec=grid_spec,
        out_shape=jax.ShapeDtypeStruct((parts, width, seq_len // parts), BF16),
        compiler_params=pltpu.CompilerParams(dimension_semantics=('arbitrary',), vmem_limit_bytes=VMEM_LIMIT),
        cost_estimate=pl.CostEstimate(flops=flops, bytes_accessed=4 * seq_len * hidden, transcendentals=seq_len * seq_len * heads // 2),
        name='attention',
    )(bounds, normed, w_rows, cosines, sines, starts[None, :])


def project_kernel(o_ref, w_ref, r_ref, gain_ref, res_ref, h_ref):
    parts = o_ref.shape[0]
    total = jnp.dot(w_ref[0], o_ref[0], preferred_element_type=F32)
    for part in range(1, parts):
        total = total + jnp.dot(w_ref[part], o_ref[part], preferred_element_type=F32)
    residual = r_ref[...].astype(F32) + total.T
    res_ref[...] = residual
    h_ref[...] = rms_norm(residual, gain_ref[...])


def project(heads_out, w_out, residual, gain, rows):
    parts, width, tokens = heads_out.shape
    hidden = residual.shape[1]
    return pl.pallas_call(
        project_kernel,
        grid=(tokens // rows,),
        in_specs=[
            pl.BlockSpec((parts, width, rows), lambda i: (0, 0, i)),
            pl.BlockSpec((parts, hidden, width), lambda i: (0, 0, 0)),
            pl.BlockSpec((rows, hidden), lambda i: (i, 0)),
            pl.BlockSpec((1, hidden), lambda i: (0, 0)),
        ],
        out_specs=[pl.BlockSpec((rows, hidden), lambda i: (i, 0)), pl.BlockSpec((rows, hidden), lambda i: (i, 0))],
        out_shape=[jax.ShapeDtypeStruct((tokens, hidden), F32), jax.ShapeDtypeStruct((tokens, hidden), BF16)],
        compiler_params=pltpu.CompilerParams(dimension_semantics=('arbitrary',), vmem_limit_bytes=VMEM_LIMIT),
        cost_estimate=pl.CostEstimate(flops=2 * tokens * hidden * parts * width, bytes_accessed=12 * tokens * hidden, transcendentals=0),
        name='project',
    )(heads_out, w_out, residual, gain)


def expert_kernel(tile_rows, h_ref, route_ref, gate_ref, up_ref, down_ref, out_ref):
    expert = pl.program_id(0)
    parts, part_rows, hidden = h_ref.shape
    shards, _, depth, width = gate_ref.shape
    gate_w = gate_ref[...].reshape(shards * depth, width)
    up_w = up_ref[...].reshape(shards * depth, width)
    down_w = down_ref[...].reshape(shards * depth, width)
    lanes = route_ref.shape[-1]
    lane_index = lax.broadcasted_iota(jnp.int32, (tile_rows, lanes), 1)
    group = tile_rows // part_rows
    for tile in range(parts // group):
        span = slice(tile * group, (tile + 1) * group)
        rows = h_ref[span].reshape(tile_rows, hidden)
        route = route_ref[span].reshape(tile_rows, lanes)
        share = jnp.sum(jnp.where(lane_index == expert, route, 0.0), axis=1, keepdims=True)
        gate_pre = jnp.dot(rows, gate_w, preferred_element_type=F32)
        up_pre = jnp.dot(rows, up_w, preferred_element_type=F32)
        act = (gate_pre * (1.0 / (1.0 + jnp.exp(-gate_pre))) * up_pre).astype(BF16)
        mixed = (share * lax.dot_general(act, down_w, NT, preferred_element_type=F32)).reshape(group, part_rows, hidden)

        @pl.when(expert == 0)
        def _():
            out_ref[span] = mixed

        @pl.when(expert > 0)
        def _():
            out_ref[span] += mixed


def expert_mix(normed, route, sub, gate_weight, up_weight, down_weight):
    parts, part_rows, hidden = normed.shape
    shards, num_experts, depth, width = gate_weight.shape
    lanes = route.shape[-1]
    tokens = parts * part_rows
    weight_spec = pl.BlockSpec((shards, 1, depth, width), lambda e: (0, e, 0, 0))
    return pl.pallas_call(
        functools.partial(expert_kernel, 2 * part_rows),
        grid=(num_experts,),
        in_specs=[
            pl.BlockSpec((parts, part_rows, hidden), lambda e: (0, 0, 0)),
            pl.BlockSpec((parts, None, part_rows, lanes), lambda e: (0, sub, 0, 0)),
            weight_spec,
            weight_spec,
            weight_spec,
        ],
        out_specs=pl.BlockSpec((parts, part_rows, hidden), lambda e: (0, 0, 0)),
        out_shape=jax.ShapeDtypeStruct((parts, part_rows, hidden), F32),
        compiler_params=pltpu.CompilerParams(dimension_semantics=('arbitrary',), vmem_limit_bytes=VMEM_LIMIT),
        cost_estimate=pl.CostEstimate(
            flops=6 * tokens * hidden * width * num_experts,
            bytes_accessed=6 * num_experts * hidden * width + 6 * tokens * hidden,
            transcendentals=tokens * width * num_experts,
        ),
        name='experts',
    )(normed, route, gate_weight, up_weight, down_weight)


def solution(mesh):
    token_spec = P(('rep', 'tok', 'mp'))
    row_spec = P(('rep', 'tok', 'mp'), None)
    head_weight = P(None, 'tok', 'mp', None)
    in_specs = (row_spec, token_spec, row_spec, row_spec, head_weight, head_weight, head_weight, P(None, 'mp', None, 'tok'), P(None, None, 'tok', 'mp'), P(None, None, 'tok', 'mp'), P(None, None, 'mp', 'tok'), P(None, None), P(None, None))
    parts = mesh.shape['mp']

    def device_step(hidden_in, seg_ids, expert_ids, expert_gates, w_query, w_key, w_value, w_out, w_gate, w_up, w_down, gain_attn, gain_mlp):
        num_layers, depth, heads, head_dim = w_query.shape
        tokens, hidden = hidden_in.shape
        seq_len = tokens * parts
        width = heads * head_dim
        subs = 4
        sub_rows = tokens // subs

        qkv_local = jnp.concatenate([w[layer].reshape(depth, width) for layer in range(num_layers) for w in (w_query, w_key, w_value)], axis=1)
        qkv_all = lax.all_gather(qkv_local, 'tok', axis=0, tiled=True)
        out_local = jnp.concatenate([w_out[layer].reshape(width, depth).T for layer in range(num_layers)], axis=1)
        out_all = lax.all_gather(out_local, ('mp', 'tok'), axis=0, tiled=True).reshape(parts, hidden, num_layers * width)
        ints = lax.all_gather(jnp.concatenate([seg_ids[:, None], expert_ids], axis=1).T, 'mp', axis=0)
        gates = lax.all_gather(expert_gates.T, 'mp', axis=0)
        starts = request_starts(ints[:, 0].reshape(seq_len))
        positions = (jnp.arange(seq_len, dtype=jnp.int32) - starts).astype(F32)
        inv_freq = jnp.power(ROPE_BASE, -jnp.arange(head_dim // 2, dtype=F32) * 2.0 / head_dim)
        angles = inv_freq[:, None] * positions[None, :]
        cosines = jnp.cos(angles)
        sines = jnp.sin(angles)
        expert_lane = jnp.arange(128, dtype=jnp.int32)
        route = jnp.zeros((parts, tokens, 128), F32)
        for choice in range(expert_ids.shape[1]):
            route = route + jnp.where(ints[:, 1 + choice][..., None] == expert_lane, gates[:, choice][..., None], 0.0)
        route = route.reshape(parts, subs, sub_rows, 128)

        residual = hidden_in.astype(F32)
        for layer in range(num_layers):
            gate_weight = lax.all_gather(w_gate[layer], 'tok', axis=0)
            up_weight = lax.all_gather(w_up[layer], 'tok', axis=0)
            down_weight = lax.all_gather(jnp.swapaxes(w_down[layer], 1, 2), 'tok', axis=0)
            w_rows = qkv_all[:, layer * 3 * width:(layer + 1) * 3 * width].T
            o_weight = out_all[:, :, layer * width:(layer + 1) * width]
            normed = lax.all_gather(rms_norm(residual, gain_attn[layer]), 'mp', axis=0, tiled=True)
            heads_out = attention(normed, w_rows, cosines, sines, starts, parts, heads, head_dim, min(512, tokens))
            heads_out = lax.all_to_all(heads_out, 'mp', 0, 0)
            residual, normed = project(heads_out, o_weight, residual, gain_mlp[layer][None, :], min(256, tokens))
            sums = []
            for sub in range(subs):
                rows = slice(sub * sub_rows, (sub + 1) * sub_rows)
                sub_normed = lax.all_gather(normed[rows], 'mp', axis=0)
                mixed = expert_mix(sub_normed, route, sub, gate_weight, up_weight, down_weight)
                sums.append(residual[rows] + lax.psum_scatter(mixed.reshape(parts * sub_rows, hidden), 'mp', scatter_dimension=0, tiled=True))
            residual = jnp.concatenate(sums, axis=0)
        return residual

    return jax.shard_map(device_step, mesh=mesh, in_specs=in_specs, out_specs=row_spec, check_vma=False)
```

```python
import functools

import jax
import jax.numpy as jnp
from jax import lax
from jax.experimental import pallas as pl
from jax.experimental.pallas import tpu as pltpu
from jax.sharding import PartitionSpec as P

EPS = 1e-5
ROPE_BASE = 10000.0
NEG = -1e30
VMEM_LIMIT = 63 * 1024 * 1024
F32 = jnp.float32
BF16 = jnp.bfloat16
NT = (((1,), (1,)), ((), ()))
MESH = pl.DeviceIdType.MESH


def rms_norm(residual, gain):
    inv_rms = lax.rsqrt(jnp.mean(residual * residual, axis=-1, keepdims=True) + EPS)
    return (residual * inv_rms * gain.astype(F32)).astype(BF16)


def request_starts(seg_rows):
    token_index = jnp.arange(seg_rows.shape[0], dtype=jnp.int32)
    is_start = jnp.concatenate([jnp.ones((1,), dtype=jnp.bool_), seg_rows[1:] != seg_rows[:-1]])
    return lax.cummax(jnp.where(is_start, token_index, 0), axis=0)


class Wire:
    def __init__(self, send_sem, recv_sem):
        self.send_sem = send_sem
        self.recv_sem = recv_sem

    def copy(self, slot, src, dst, device):
        return pltpu.make_async_remote_copy(src_ref=src, dst_ref=dst, send_sem=self.send_sem.at[slot], recv_sem=self.recv_sem.at[slot], device_id=device, device_id_type=MESH)


def ring(axis, size):
    me = lax.axis_index(axis)
    return me, lax.rem(me + size - 1, size), lax.rem(me + 1, size), lax.rem(me + size // 2, size)


def meet(devices):
    barrier = pltpu.get_barrier_semaphore()
    for device in devices:
        pl.semaphore_signal(barrier, inc=1, device_id=device, device_id_type=MESH)
    pl.semaphore_wait(barrier, len(devices))


def row_gather(wire, base, own, rows_all, left, right, me):
    half = own.shape[0] // 2
    low, high = pl.ds(0, half), pl.ds(half, half)
    to_right, to_left = {'mp': right}, {'mp': left}
    return {
        'right_low': wire.copy(base, own.at[low], rows_all.at[me, low], to_right),
        'right_high': wire.copy(base + 1, own.at[high], rows_all.at[me, high], to_right),
        'left_high': wire.copy(base + 2, own.at[high], rows_all.at[me, high], to_left),
        'left_low': wire.copy(base + 3, own.at[low], rows_all.at[me, low], to_left),
        'on_right': wire.copy(base + 4, rows_all.at[left, low], rows_all.at[left, low], to_right),
        'on_left': wire.copy(base + 5, rows_all.at[right, high], rows_all.at[right, high], to_left),
    }


FIRST = ('right_low', 'left_high', 'right_high', 'left_low')


def gather_kernel(parts, shards, hidden_ref, gain_ref, ints_ref, gates_ref, qkv_ref, out_ref, rows_all, ints_all, gates_all, qkv_all, out_all, own, send_sem, recv_sem, local_sem):
    me, left, right, _ = ring('mp', parts)
    tok = lax.axis_index('tok')
    partner = tok + 1 - 2 * lax.rem(tok, 2)
    strides = [2 * step for step in range(1, shards // 2)]
    peers = [{'tok': lax.rem(tok + stride, shards)} for stride in strides]
    to_left, to_right, to_partner = {'mp': left}, {'mp': right}, {'tok': partner}
    meet([to_left, to_right, to_partner] + peers)
    wire = Wire(send_sem, recv_sem)
    small = [
        wire.copy(0, out_ref, out_all.at[tok, me], to_right),
        wire.copy(1, out_ref, out_all.at[tok, me], to_left),
        wire.copy(2, ints_ref, ints_all.at[me], to_right),
        wire.copy(3, ints_ref, ints_all.at[me], to_left),
        wire.copy(4, gates_ref, gates_all.at[me], to_right),
        wire.copy(5, gates_ref, gates_all.at[me], to_left),
    ]
    local = [
        pltpu.make_async_copy(out_ref, out_all.at[tok, me], local_sem.at[0]),
        pltpu.make_async_copy(ints_ref, ints_all.at[me], local_sem.at[1]),
        pltpu.make_async_copy(gates_ref, gates_all.at[me], local_sem.at[2]),
        pltpu.make_async_copy(qkv_ref, qkv_all.at[tok], local_sem.at[3]),
    ]
    slot = 6
    qkv_out = []
    for peer in peers:
        qkv_out.append(wire.copy(slot, qkv_ref, qkv_all.at[tok], peer))
        slot += 1
    qkv_cross = [wire.copy(slot, qkv_ref, qkv_all.at[tok], to_partner)]
    slot += 1
    for stride in strides:
        source = lax.rem(tok + shards - stride, shards)
        qkv_cross.append(wire.copy(slot, qkv_all.at[source], qkv_all.at[source], to_partner))
        slot += 1
    for copy in small + local + qkv_out + qkv_cross[:1]:
        copy.start()
    own[...] = rms_norm(hidden_ref[...].astype(F32), gain_ref[...])
    rows = row_gather(wire, slot, own, rows_all, left, right, me)
    slot += 6
    rows_local = pltpu.make_async_copy(own, rows_all.at[me], local_sem.at[4])
    for name in FIRST:
        rows[name].start()
    rows_local.start()
    onward = [
        wire.copy(slot, out_all.at[tok, left], out_all.at[tok, left], to_right),
        wire.copy(slot + 1, ints_all.at[left], ints_all.at[left], to_right),
        wire.copy(slot + 2, gates_all.at[right], gates_all.at[right], to_left),
    ]
    slot += 3
    for copy in small:
        copy.wait_recv()
    for copy in onward:
        copy.start()
    for copy, after in zip(qkv_cross[1:], qkv_out):
        after.wait_recv()
        copy.start()
    onward[0].wait_recv()
    local[0].wait()
    out_out = []
    for peer in peers:
        out_out.append(wire.copy(slot, out_all.at[tok], out_all.at[tok], peer))
        slot += 1
    out_cross = [wire.copy(slot, out_all.at[tok], out_all.at[tok], to_partner)]
    slot += 1
    for stride in strides:
        source = lax.rem(tok + shards - stride, shards)
        out_cross.append(wire.copy(slot, out_all.at[source], out_all.at[source], to_partner))
        slot += 1
    for copy in out_out + out_cross[:1]:
        copy.start()
    for copy, after in zip(out_cross[1:], out_out):
        after.wait_recv()
        copy.start()
    rows['right_low'].wait_recv()
    rows['on_right'].start()
    rows['left_high'].wait_recv()
    rows['on_left'].start()
    for copy in onward[1:] + qkv_cross + out_cross:
        copy.wait_recv()
    for name in ('right_high', 'left_low', 'on_right', 'on_left'):
        rows[name].wait_recv()
    for copy in small + onward + qkv_out + qkv_cross + out_out + out_cross + list(rows.values()):
        copy.wait_send()
    for copy in local[1:] + [rows_local]:
        copy.wait()


def gather_start(hidden_in, gain, ints, gates, qkv_local, out_local, parts, shards):
    tokens, hidden = hidden_in.shape
    copies = 6 + 2 * (shards - 2) // 2 + 1 + 6 + 3 + 2 * (shards - 2) // 2 + 1
    anywhere = pl.BlockSpec(memory_space=pl.ANY)
    vmem = pl.BlockSpec(memory_space=pltpu.VMEM)
    return pl.pallas_call(
        functools.partial(gather_kernel, parts, shards),
        in_specs=[vmem, vmem, vmem, vmem, vmem, vmem],
        out_specs=[anywhere] * 5,
        out_shape=[
            jax.ShapeDtypeStruct((parts, tokens, hidden), BF16),
            jax.ShapeDtypeStruct((parts,) + ints.shape, jnp.int32),
            jax.ShapeDtypeStruct((parts,) + gates.shape, F32),
            jax.ShapeDtypeStruct((shards,) + qkv_local.shape, BF16),
            jax.ShapeDtypeStruct((shards, parts) + out_local.shape, BF16),
        ],
        scratch_shapes=[
            pltpu.VMEM((tokens, hidden), BF16),
            pltpu.SemaphoreType.DMA((copies,)),
            pltpu.SemaphoreType.DMA((copies,)),
            pltpu.SemaphoreType.DMA((5,)),
        ],
        compiler_params=pltpu.CompilerParams(collective_id=0, has_side_effects=True, vmem_limit_bytes=VMEM_LIMIT),
        cost_estimate=pl.CostEstimate(flops=20_000_000_000, bytes_accessed=2 * parts * tokens * hidden, transcendentals=0),
        name='gather_start',
    )(hidden_in, gain, ints, gates, qkv_local, out_local)


def attention_kernel(heads, head_dim, bounds_ref, h_ref, w_ref, cos_ref, sin_ref, start_ref, out_ref, w_sc, q_sc, k_sc, v_sc, m_sc, l_sc, acc_sc):
    tile = pl.program_id(0)
    rows = h_ref.shape[0]
    width = heads * head_dim
    half = head_dim // 2

    @pl.when(tile == 0)
    def _():
        w_sc[...] = w_ref[:, 0].reshape(w_sc.shape[1], 3 * width).astype(F32).T.astype(BF16)

    qkv = lax.dot_general(w_sc[...], h_ref[...], NT, preferred_element_type=F32)
    cosines = cos_ref[...]
    sines = sin_ref[...]

    def rotate(base):
        first = qkv[base:base + half]
        second = qkv[base + half:base + head_dim]
        return jnp.concatenate([first * cosines - second * sines, second * cosines + first * sines], axis=0)

    scale = head_dim ** -0.5
    for head in range(heads):
        base = head * head_dim
        q_sc[head] = (rotate(base).astype(BF16).astype(F32) * scale).astype(BF16)
        k_sc[tile, head] = rotate(width + base).T.astype(BF16)
    v_sc[tile] = qkv[2 * width:3 * width].astype(BF16)
    m_sc[...] = jnp.full(m_sc.shape, NEG, F32)
    l_sc[...] = jnp.zeros(l_sc.shape, F32)
    acc_sc[...] = jnp.zeros(acc_sc.shape, F32)

    def block(key_tile, masked):
        if masked:
            key_index = key_tile * rows + lax.broadcasted_iota(jnp.int32, (rows, rows), 0)
            query_index = tile * rows + lax.broadcasted_iota(jnp.int32, (1, rows), 1)
            allowed = (key_index >= start_ref[...]) & (key_index <= query_index)
        for head in range(heads):
            scores = jnp.dot(k_sc[key_tile, head], q_sc[head], preferred_element_type=F32)
            if masked:
                scores = jnp.where(allowed, scores, NEG)
            old_max = m_sc[head]
            new_max = jnp.maximum(old_max, jnp.max(scores, axis=0, keepdims=True))
            prob = jnp.exp(scores - new_max)
            fade = jnp.exp(old_max - new_max)
            m_sc[head] = new_max
            l_sc[head] = fade * l_sc[head] + jnp.sum(prob, axis=0, keepdims=True)
            part = jnp.dot(v_sc[key_tile, head * head_dim:(head + 1) * head_dim], prob.astype(BF16), preferred_element_type=F32)
            acc_sc[head] = acc_sc[head] * fade + part

    def masked_step(key_tile, carry):
        block(key_tile, True)
        return carry

    def open_step(key_tile, carry):
        block(key_tile, False)
        return carry

    first_tile = bounds_ref[0, tile]
    open_tile = bounds_ref[1, tile]
    lax.fori_loop(first_tile, open_tile, masked_step, 0)
    lax.fori_loop(open_tile, tile, open_step, 0)
    block(tile, True)
    for head in range(heads):
        out_ref[0, head * head_dim:(head + 1) * head_dim] = (acc_sc[head] / l_sc[head]).astype(BF16)


def attention(normed, w_all, layer, cosines, sines, starts, parts, heads, head_dim, rows):
    seq_len, hidden = normed.shape
    tiles = seq_len // rows
    width = heads * head_dim
    per_part = tiles // parts
    shards, _, depth, _ = w_all.shape
    first_start = starts[::rows]
    last_start = starts[rows - 1::rows]
    tile_index = jnp.arange(tiles, dtype=jnp.int32)
    bounds = jnp.stack([first_start // rows, jnp.minimum((last_start + rows - 1) // rows, tile_index)])
    grid_spec = pltpu.PrefetchScalarGridSpec(
        num_scalar_prefetch=1,
        grid=(tiles,),
        in_specs=[
            pl.BlockSpec((rows, hidden), lambda i, b: (i, 0)),
            pl.BlockSpec((shards, 1, depth, 3 * width), lambda i, b: (0, layer, 0, 0)),
            pl.BlockSpec((head_dim // 2, rows), lambda i, b: (0, i)),
            pl.BlockSpec((head_dim // 2, rows), lambda i, b: (0, i)),
            pl.BlockSpec((1, rows), lambda i, b: (0, i)),
        ],
        out_specs=pl.BlockSpec((1, width, rows), lambda i, b: (i // per_part, 0, i % per_part)),
        scratch_shapes=[
            pltpu.VMEM((3 * width, hidden), BF16),
            pltpu.VMEM((heads, head_dim, rows), BF16),
            pltpu.VMEM((tiles, heads, rows, head_dim), BF16),
            pltpu.VMEM((tiles, width, rows), BF16),
            pltpu.VMEM((heads, 1, rows), F32),
            pltpu.VMEM((heads, 1, rows), F32),
            pltpu.VMEM((heads, head_dim, rows), F32),
        ],
    )
    flops = 2 * seq_len * hidden * 3 * width + 2 * seq_len * seq_len * width
    return pl.pallas_call(
        functools.partial(attention_kernel, heads, head_dim),
        grid_spec=grid_spec,
        out_shape=jax.ShapeDtypeStruct((parts, width, seq_len // parts), BF16),
        compiler_params=pltpu.CompilerParams(dimension_semantics=('arbitrary',), vmem_limit_bytes=VMEM_LIMIT),
        cost_estimate=pl.CostEstimate(flops=flops, bytes_accessed=4 * seq_len * hidden, transcendentals=seq_len * seq_len * heads // 2),
        name='attention',
    )(bounds, normed, w_all, cosines, sines, starts[None, :])


LAYER_COPIES = 24
SLOTS = 3


def layer_kernel(layer, parts, has_next, o_hbm, wo_hbm, r_ref, gain_mlp, gain_next, ints_ref, gates_ref, gate_hbm, up_hbm, down_hbm, *rest):
    if has_next:
        res_ref, rows_all, hbuf, own_o, wo_ref, obuf, relay, wbuf, acc, inbox, route, own, send_sem, recv_sem, w_sem, local_sem = rest
    else:
        res_ref, hbuf, own_o, wo_ref, obuf, relay, wbuf, acc, inbox, route, send_sem, recv_sem, w_sem, local_sem = rest
    me, left, right, far = ring('mp', parts)
    to_left, to_right = {'mp': left}, {'mp': right}
    wire = Wire(send_sem, recv_sem)
    _, num_experts, _, ffn = gate_hbm.shape
    width = o_hbm.shape[1]
    tokens, hidden = res_ref.shape
    half = tokens // 2
    low, high = pl.ds(0, half), pl.ds(half, half)
    o_low, o_high = pl.ds(0, width // 2), pl.ds(width // 2, width // 2)

    def weight_copies(step):
        expert = lax.rem(step, num_experts)
        slot = lax.rem(step, SLOTS)
        return [pltpu.make_async_copy(hbm.at[:, expert], wbuf.at[slot, index], w_sem.at[slot, index]) for index, hbm in enumerate((gate_hbm, up_hbm, down_hbm))]

    for step in range(SLOTS - 1):
        for copy in weight_copies(step):
            copy.start()
    own_copy = pltpu.make_async_copy(o_hbm.at[me], own_o, local_sem.at[0])
    own_copy.start()
    wo_copy = pltpu.make_async_copy(wo_hbm.at[:, :, layer], wo_ref, local_sem.at[1])
    wo_copy.start()
    meet([to_left, to_right])

    exchange = [
        wire.copy(0, o_hbm.at[far, o_low], relay.at[0], to_right),
        wire.copy(1, o_hbm.at[far, o_high], relay.at[1], to_left),
        wire.copy(2, o_hbm.at[right], obuf.at[0], to_right),
        wire.copy(3, o_hbm.at[left], obuf.at[1], to_left),
        wire.copy(4, relay.at[0], obuf.at[2, o_low], to_right),
        wire.copy(5, relay.at[1], obuf.at[2, o_high], to_left),
    ]
    for copy in exchange[:4]:
        copy.start()

    expert_row = lax.broadcasted_iota(jnp.int32, (num_experts, 1), 0)
    for part in range(parts):
        share = jnp.zeros((num_experts, tokens), F32)
        for choice in range(2):
            share = share + jnp.where(ints_ref[part, 1 + choice:2 + choice] == expert_row, gates_ref[part, choice:choice + 1], 0.0)
        route[part] = share.T

    exchange[0].wait_recv()
    exchange[4].start()
    exchange[1].wait_recv()
    exchange[5].start()
    own_copy.wait()
    wo_copy.wait()
    for copy in exchange[2:]:
        copy.wait_recv()

    chunk = min(256, tokens)

    def project(index, carry):
        span = pl.ds(pl.multiple_of(index * chunk, chunk), chunk)
        total = None
        for source, piece in ((me, own_o), (left, obuf.at[0]), (right, obuf.at[1]), (far, obuf.at[2])):
            weight = wo_ref[:, source].reshape(hidden, width)
            term = jnp.dot(weight, piece[:, span], preferred_element_type=F32)
            total = term if total is None else total + term
        residual = r_ref[span].astype(F32) + total.T
        res_ref[span] = residual
        hbuf[me, span] = rms_norm(residual, gain_mlp[...])
        return carry

    lax.fori_loop(0, tokens // chunk, project, 0)

    rows = row_gather(wire, 6, hbuf.at[me], hbuf, left, right, me)
    for name in FIRST:
        rows[name].start()

    sends = {
        1: wire.copy(12, acc.at[1], inbox.at[0], to_left),
        2: wire.copy(13, acc.at[2], inbox.at[1], to_right),
        3: wire.copy(14, acc.at[3], inbox.at[2], to_right),
        4: wire.copy(15, acc.at[4], inbox.at[3], to_left),
        5: wire.copy(16, acc.at[5], inbox.at[4], to_right),
        6: wire.copy(17, acc.at[6], inbox.at[5], to_left),
    }
    tile_rows = min(256, half)
    tiles = half // tile_rows
    lane = lax.broadcasted_iota(jnp.int32, (tile_rows, num_experts), 1)
    steps = 8 * num_experts

    def expert_step(step, carry):
        phase = step // num_experts
        expert = lax.rem(step, num_experts)
        slot = lax.rem(step, SLOTS)
        late = phase // 4
        near = phase + late * (7 - 2 * phase)
        is_zero = ((3 - near) * (2 - near) * (1 - near)) // 6
        is_one = (near * (3 - near) * (2 - near)) // 2
        is_two = (near * (3 - near) * (near - 1)) // 2
        shift = near - 1 + is_zero + 3 * is_one
        source = lax.rem(me + shift, parts)
        top = is_two + late * (1 - 2 * is_two)
        start = pl.multiple_of(top * half, half)

        @pl.when(step + SLOTS - 1 < steps)
        def _():
            for copy in weight_copies(step + SLOTS - 1):
                copy.start()

        @pl.when(expert == 0)
        def _():
            acc[phase] = jnp.zeros((half, hidden), F32)

            @pl.when(phase == 1)
            def _():
                rows['right_low'].wait_recv()
                rows['on_right'].start()

            @pl.when(phase == 2)
            def _():
                sends[1].start()
                rows['left_high'].wait_recv()
                rows['on_left'].start()

            @pl.when(phase == 3)
            def _():
                sends[2].start()
                rows['on_right'].wait_recv()

            @pl.when(phase == 4)
            def _():
                sends[3].start()
                rows['on_left'].wait_recv()

            @pl.when(phase == 5)
            def _():
                sends[4].start()
                rows['left_low'].wait_recv()

            @pl.when(phase == 6)
            def _():
                rows['right_high'].wait_recv()

            @pl.when(phase == 7)
            def _():
                sends[3].wait_recv()
                acc[5] += inbox[2]
                sends[5].start()
                sends[4].wait_recv()
                acc[6] += inbox[3]
                sends[6].start()

        for copy in weight_copies(step):
            copy.wait()

        def activate(tile):
            gate_w = wbuf[slot, 0].reshape(hidden, ffn)
            up_w = wbuf[slot, 1].reshape(hidden, ffn)
            x = hbuf[source, pl.ds(start + tile * tile_rows, tile_rows)]
            gate_pre = jnp.dot(x, gate_w, preferred_element_type=F32)
            up_pre = jnp.dot(x, up_w, preferred_element_type=F32)
            return (gate_pre * (1.0 / (1.0 + jnp.exp(-gate_pre))) * up_pre).astype(BF16)

        def contract(tile, act):
            down_w = wbuf[slot, 2].reshape(hidden, ffn)
            part_share = route[source, pl.ds(start + tile * tile_rows, tile_rows)]
            share = jnp.sum(jnp.where(lane == expert, part_share, 0.0), axis=1, keepdims=True)
            mixed = lax.dot_general(act, down_w, NT, preferred_element_type=F32)
            acc[phase, tile * tile_rows:(tile + 1) * tile_rows] += share * mixed

        act = activate(0)
        for tile in range(tiles):
            following = activate(tile + 1) if tile + 1 < tiles else None
            contract(tile, act)
            act = following
        return carry

    lax.fori_loop(0, steps, expert_step, 0)

    sends[1].wait_recv()
    res_ref[low] += acc[0] + inbox[0]
    sends[2].wait_recv()
    res_ref[high] += acc[7] + inbox[1]
    sends[5].wait_recv()
    res_ref[low] += inbox[4]
    if has_next:
        own[low] = rms_norm(res_ref[low], gain_next[...])
    sends[6].wait_recv()
    res_ref[high] += inbox[5]
    for copy in exchange + list(rows.values()) + list(sends.values()):
        copy.wait_send()
    if has_next:
        own[high] = rms_norm(res_ref[high], gain_next[...])
        rows_next = row_gather(wire, 18, own, rows_all, left, right, me)
        for name in FIRST:
            rows_next[name].start()
        rows_local = pltpu.make_async_copy(own, rows_all.at[me], local_sem.at[2])
        rows_local.start()
        rows_next['right_low'].wait_recv()
        rows_next['on_right'].start()
        rows_next['left_high'].wait_recv()
        rows_next['on_left'].start()
        for name in ('right_high', 'left_low', 'on_right', 'on_left'):
            rows_next[name].wait_recv()
        for copy in rows_next.values():
            copy.wait_send()
        rows_local.wait()


def layer_rest(layer, has_next, parts, heads_out, out_all, residual, gain_mlp, gain_next, ints_all, gates_all, gate_weight, up_weight, down_weight):
    _, width, tokens = heads_out.shape
    hidden = residual.shape[1]
    shards, num_experts, depth, ffn = gate_weight.shape
    half = tokens // 2
    anywhere = pl.BlockSpec(memory_space=pl.ANY)
    vmem = pl.BlockSpec(memory_space=pltpu.VMEM)
    out_shape = [jax.ShapeDtypeStruct((tokens, hidden), F32)]
    out_specs = [vmem]
    scratch = [
        pltpu.VMEM((parts, tokens, hidden), BF16),
        pltpu.VMEM((width, tokens), BF16),
        pltpu.VMEM((shards, parts, depth, width), BF16),
        pltpu.VMEM((3, width, tokens), BF16),
        pltpu.VMEM((2, width // 2, tokens), BF16),
        pltpu.VMEM((SLOTS, 3, shards, depth, ffn), BF16),
        pltpu.VMEM((8, half, hidden), F32),
        pltpu.VMEM((6, half, hidden), F32),
        pltpu.VMEM((parts, tokens, num_experts), F32),
    ]
    if has_next:
        out_shape.append(jax.ShapeDtypeStruct((parts, tokens, hidden), BF16))
        out_specs.append(anywhere)
        scratch.append(pltpu.VMEM((tokens, hidden), BF16))
    scratch += [
        pltpu.SemaphoreType.DMA((LAYER_COPIES,)),
        pltpu.SemaphoreType.DMA((LAYER_COPIES,)),
        pltpu.SemaphoreType.DMA((SLOTS, 3)),
        pltpu.SemaphoreType.DMA((3,)),
    ]
    return pl.pallas_call(
        functools.partial(layer_kernel, layer, parts, has_next),
        in_specs=[
            anywhere, anywhere,
            vmem, vmem, vmem, vmem, vmem,
            anywhere, anywhere, anywhere,
        ],
        out_specs=out_specs,
        out_shape=out_shape,
        scratch_shapes=scratch,
        compiler_params=pltpu.CompilerParams(collective_id=1 + layer, has_side_effects=True, vmem_limit_bytes=VMEM_LIMIT),
        cost_estimate=pl.CostEstimate(
            flops=6 * parts * tokens * hidden * ffn * num_experts,
            bytes_accessed=8 * 6 * num_experts * hidden * ffn,
            transcendentals=parts * tokens * ffn * num_experts,
        ),
        name='layer_rest',
    )(heads_out, out_all, residual, gain_mlp, gain_next, ints_all, gates_all, gate_weight, up_weight, down_weight)


def solution(mesh):
    token_spec = P(('rep', 'tok', 'mp'))
    row_spec = P(('rep', 'tok', 'mp'), None)
    head_weight = P(None, 'tok', 'mp', None)
    in_specs = (row_spec, token_spec, row_spec, row_spec, head_weight, head_weight, head_weight, P(None, 'mp', None, 'tok'), P(None, None, 'tok', 'mp'), P(None, None, 'tok', 'mp'), P(None, None, 'mp', 'tok'), P(None, None), P(None, None))
    parts = mesh.shape['mp']
    shards = mesh.shape['tok']

    def device_step(hidden_in, seg_ids, expert_ids, expert_gates, w_query, w_key, w_value, w_out, w_gate, w_up, w_down, gain_attn, gain_mlp):
        num_layers, depth, heads, head_dim = w_query.shape
        tokens, hidden = hidden_in.shape
        seq_len = tokens * parts
        width = heads * head_dim

        weights = []
        for layer in range(num_layers):
            gate_weight = lax.all_gather(w_gate[layer], 'tok', axis=0)
            up_weight = lax.all_gather(w_up[layer], 'tok', axis=0)
            down_weight = lax.all_gather(jnp.swapaxes(w_down[layer], 1, 2), 'tok', axis=0)
            weights.append((gate_weight, up_weight, down_weight))

        qkv_local = jnp.concatenate([w.reshape(num_layers, depth, width) for w in (w_query, w_key, w_value)], axis=2)
        out_local = jnp.swapaxes(w_out.reshape(num_layers, width, depth), 1, 2)
        ints = jnp.concatenate([seg_ids[None, :], expert_ids.T, jnp.zeros((5, tokens), jnp.int32)], axis=0)
        gates = jnp.concatenate([expert_gates.T, jnp.zeros((6, tokens), F32)], axis=0)
        rows_all, ints_all, gates_all, qkv_all, out_all = gather_start(hidden_in, gain_attn[:1], ints, gates, qkv_local, out_local, parts, shards)

        starts = request_starts(ints_all[:, 0].reshape(seq_len))
        positions = (jnp.arange(seq_len, dtype=jnp.int32) - starts).astype(F32)
        inv_freq = jnp.power(ROPE_BASE, -jnp.arange(head_dim // 2, dtype=F32) * 2.0 / head_dim)
        angles = inv_freq[:, None] * positions[None, :]
        cosines = jnp.cos(angles)
        sines = jnp.sin(angles)

        residual = hidden_in
        for layer in range(num_layers):
            has_next = layer + 1 < num_layers
            heads_out = attention(rows_all.reshape(seq_len, hidden), qkv_all, layer, cosines, sines, starts, parts, heads, head_dim, min(512, tokens))
            following = gain_attn[layer + 1:layer + 2] if has_next else gain_attn[layer:layer + 1]
            outs = layer_rest(layer, has_next, parts, heads_out, out_all, residual, gain_mlp[layer:layer + 1], following, ints_all, gates_all, *weights[layer])
            residual = outs[0]
            rows_all = outs[1] if has_next else None
        return residual

    return jax.shard_map(device_step, mesh=mesh, in_specs=in_specs, out_specs=row_spec, check_vma=False)
```

```python
import functools

import jax
import jax.numpy as jnp
from jax import lax
from jax.experimental import pallas as pl
from jax.experimental.pallas import tpu as pltpu
from jax.sharding import PartitionSpec as P

EPS = 1e-5
ROPE_BASE = 10000.0
NEG = -1e30
VMEM_LIMIT = 63 * 1024 * 1024
F32 = jnp.float32
BF16 = jnp.bfloat16
NT = (((1,), (1,)), ((), ()))
MESH = pl.DeviceIdType.MESH
AHEAD = 2


def rms_norm(residual, gain):
    inv_rms = lax.rsqrt(jnp.mean(residual * residual, axis=-1, keepdims=True) + EPS)
    return (residual * inv_rms * gain.astype(F32)).astype(BF16)


def request_starts(seg_rows):
    token_index = jnp.arange(seg_rows.shape[0], dtype=jnp.int32)
    is_start = jnp.concatenate([jnp.ones((1,), dtype=jnp.bool_), seg_rows[1:] != seg_rows[:-1]])
    return lax.cummax(jnp.where(is_start, token_index, 0), axis=0)


class Wire:
    def __init__(self, send_sem, recv_sem):
        self.send_sem = send_sem
        self.recv_sem = recv_sem

    def copy(self, slot, src, dst, device):
        return pltpu.make_async_remote_copy(src_ref=src, dst_ref=dst, send_sem=self.send_sem.at[slot], recv_sem=self.recv_sem.at[slot], device_id=device, device_id_type=MESH)


def ring(axis, size):
    me = lax.axis_index(axis)
    return me, lax.rem(me + size - 1, size), lax.rem(me + 1, size), lax.rem(me + size // 2, size)


def meet(devices):
    barrier = pltpu.get_barrier_semaphore()
    for device in devices:
        pl.semaphore_signal(barrier, inc=1, device_id=device, device_id_type=MESH)
    pl.semaphore_wait(barrier, len(devices))


def ring_gather(wire, base, own, rows_all, axis, left, right, me):
    half = own.shape[0] // 2
    low, high = pl.ds(0, half), pl.ds(half, half)
    to_right, to_left = {axis: right}, {axis: left}
    return {
        'right_low': wire.copy(base, own.at[low], rows_all.at[me, low], to_right),
        'right_high': wire.copy(base + 1, own.at[high], rows_all.at[me, high], to_right),
        'left_high': wire.copy(base + 2, own.at[high], rows_all.at[me, high], to_left),
        'left_low': wire.copy(base + 3, own.at[low], rows_all.at[me, low], to_left),
        'on_right': wire.copy(base + 4, rows_all.at[left, low], rows_all.at[left, low], to_right),
        'on_left': wire.copy(base + 5, rows_all.at[right, high], rows_all.at[right, high], to_left),
    }


FIRST = ('right_low', 'left_high', 'right_high', 'left_low')


class ShardGather:
    COPIES = 10

    def __init__(self, wire, base, own, blocks, shards):
        tok = lax.axis_index('tok')
        self.left = lax.rem(tok + shards - 2, shards)
        self.right = lax.rem(tok + 2, shards)
        far = lax.rem(tok + shards // 2, shards)
        partner = {'tok': tok + 1 - 2 * lax.rem(tok, 2)}
        self.rows = ring_gather(wire, base, own, blocks, 'tok', self.left, self.right, tok)
        self.cross = [wire.copy(base + 6, own, blocks.at[tok], partner)]
        for index, source in enumerate((self.left, self.right, far)):
            self.cross.append(wire.copy(base + 7 + index, blocks.at[source], blocks.at[source], partner))
        self.devices = [partner, {'tok': self.left}, {'tok': self.right}]

    def start(self):
        for name in FIRST:
            self.rows[name].start()
        self.cross[0].start()

    def onward(self):
        self.rows['right_low'].wait_recv()
        self.rows['on_right'].start()
        self.rows['left_high'].wait_recv()
        self.rows['on_left'].start()

    def share(self):
        self.rows['right_high'].wait_recv()
        self.cross[1].start()
        self.rows['left_low'].wait_recv()
        self.cross[2].start()
        self.rows['on_right'].wait_recv()
        self.rows['on_left'].wait_recv()
        self.cross[3].start()

    def arrive(self):
        for copy in self.cross:
            copy.wait_recv()

    def sent(self):
        for copy in list(self.rows.values()) + self.cross:
            copy.wait_send()


def gather_kernel(parts, shards, hidden_ref, gain_ref, ints_ref, gates_ref, qkv_ref, out_ref, rows_all, ints_all, gates_all, qkv_all, out_all, own, send_sem, recv_sem, local_sem):
    me, left, right, _ = ring('mp', parts)
    tok = lax.axis_index('tok')
    to_left, to_right = {'mp': left}, {'mp': right}
    wire = Wire(send_sem, recv_sem)
    qkv = ShardGather(wire, 15, qkv_ref, qkv_all, shards)
    out = ShardGather(wire, 25, out_all.at[tok], out_all, shards)
    meet([to_left, to_right] + qkv.devices)
    small = [
        wire.copy(0, out_ref, out_all.at[tok, me], to_right),
        wire.copy(1, out_ref, out_all.at[tok, me], to_left),
        wire.copy(2, ints_ref, ints_all.at[me], to_right),
        wire.copy(3, ints_ref, ints_all.at[me], to_left),
        wire.copy(4, gates_ref, gates_all.at[me], to_right),
        wire.copy(5, gates_ref, gates_all.at[me], to_left),
    ]
    onward = [
        wire.copy(6, out_all.at[tok, left], out_all.at[tok, left], to_right),
        wire.copy(7, ints_all.at[left], ints_all.at[left], to_right),
        wire.copy(8, gates_all.at[right], gates_all.at[right], to_left),
    ]
    local = [
        pltpu.make_async_copy(out_ref, out_all.at[tok, me], local_sem.at[0]),
        pltpu.make_async_copy(ints_ref, ints_all.at[me], local_sem.at[1]),
        pltpu.make_async_copy(gates_ref, gates_all.at[me], local_sem.at[2]),
        pltpu.make_async_copy(qkv_ref, qkv_all.at[tok], local_sem.at[3]),
    ]
    for copy in small + local:
        copy.start()
    qkv.start()
    own[...] = rms_norm(hidden_ref[...].astype(F32), gain_ref[...])
    rows = ring_gather(wire, 9, own, rows_all, 'mp', left, right, me)
    rows_local = pltpu.make_async_copy(own, rows_all.at[me], local_sem.at[4])
    for name in FIRST:
        rows[name].start()
    rows_local.start()
    for copy in small:
        copy.wait_recv()
    for copy in onward:
        copy.start()
    onward[0].wait_recv()
    local[0].wait()
    out.start()
    qkv.onward()
    rows['right_low'].wait_recv()
    rows['on_right'].start()
    rows['left_high'].wait_recv()
    rows['on_left'].start()
    out.onward()
    qkv.share()
    out.share()
    for name in ('right_high', 'left_low', 'on_right', 'on_left'):
        rows[name].wait_recv()
    for copy in onward[1:]:
        copy.wait_recv()
    qkv.arrive()
    out.arrive()
    for copy in small + onward + list(rows.values()):
        copy.wait_send()
    qkv.sent()
    out.sent()
    for copy in local[1:] + [rows_local]:
        copy.wait()


def gather_start(hidden_in, gain, ints, gates, qkv_local, out_local, parts, shards):
    tokens, hidden = hidden_in.shape
    copies = 15 + 2 * ShardGather.COPIES
    anywhere = pl.BlockSpec(memory_space=pl.ANY)
    vmem = pl.BlockSpec(memory_space=pltpu.VMEM)
    return pl.pallas_call(
        functools.partial(gather_kernel, parts, shards),
        in_specs=[vmem, vmem, vmem, vmem, vmem, vmem],
        out_specs=[anywhere] * 5,
        out_shape=[
            jax.ShapeDtypeStruct((parts, tokens, hidden), BF16),
            jax.ShapeDtypeStruct((parts,) + ints.shape, jnp.int32),
            jax.ShapeDtypeStruct((parts,) + gates.shape, F32),
            jax.ShapeDtypeStruct((shards,) + qkv_local.shape, BF16),
            jax.ShapeDtypeStruct((shards, parts) + out_local.shape, BF16),
        ],
        scratch_shapes=[
            pltpu.VMEM((tokens, hidden), BF16),
            pltpu.SemaphoreType.DMA((copies,)),
            pltpu.SemaphoreType.DMA((copies,)),
            pltpu.SemaphoreType.DMA((5,)),
        ],
        compiler_params=pltpu.CompilerParams(collective_id=0, has_side_effects=True, vmem_limit_bytes=VMEM_LIMIT),
        cost_estimate=pl.CostEstimate(flops=20_000_000_000, bytes_accessed=2 * parts * tokens * hidden, transcendentals=0),
        name='gather_start',
    )(hidden_in, gain, ints, gates, qkv_local, out_local)


def attention_kernel(heads, head_dim, bounds_ref, h_ref, w_ref, cos_ref, sin_ref, start_ref, out_ref, w_sc, q_sc, k_sc, v_sc, m_sc, l_sc, acc_sc, s_sc):
    tile = pl.program_id(0)
    rows = h_ref.shape[0]
    span = q_sc.shape[-1]
    pieces = rows // span
    width = heads * head_dim
    half = head_dim // 2
    units = [(head, piece) for head in range(heads) for piece in range(pieces)]

    @pl.when(tile == 0)
    def _():
        w_sc[...] = w_ref[:, 0].reshape(w_sc.shape[1], 3 * width).astype(F32).T.astype(BF16)

    qkv = lax.dot_general(w_sc[...], h_ref[...], NT, preferred_element_type=F32)
    cosines = cos_ref[...]
    sines = sin_ref[...]

    def rotate(base):
        first = qkv[base:base + half]
        second = qkv[base + half:base + head_dim]
        return jnp.concatenate([first * cosines - second * sines, second * cosines + first * sines], axis=0)

    scale = head_dim ** -0.5
    for head in range(heads):
        base = head * head_dim
        query = (rotate(base).astype(BF16).astype(F32) * scale).astype(BF16)
        for piece in range(pieces):
            q_sc[head * pieces + piece] = query[:, piece * span:(piece + 1) * span]
        k_sc[tile, head] = rotate(width + base).T.astype(BF16)
    v_sc[tile] = qkv[2 * width:3 * width].astype(BF16)
    m_sc[...] = jnp.full(m_sc.shape, NEG, F32)
    l_sc[...] = jnp.zeros(l_sc.shape, F32)
    acc_sc[...] = jnp.zeros(acc_sc.shape, F32)
    first_tile = bounds_ref[0, tile]
    open_tile = bounds_ref[1, tile]

    def score(unit, key_tile, keys):
        head, _ = units[unit]
        return jnp.dot(k_sc[key_tile, head, :keys], q_sc[unit], preferred_element_type=F32)

    def absorb(unit, scores, key_tile, causal, bounded):
        head, piece = units[unit]
        keys = scores.shape[0]
        if causal or bounded:
            key_row = lax.broadcasted_iota(jnp.int32, (keys, span), 0)
            allowed = None
            if bounded:
                allowed = key_row >= start_ref[:, piece * span:(piece + 1) * span] - key_tile * rows
            if causal:
                query_row = lax.broadcasted_iota(jnp.int32, (keys, span), 1) + piece * span
                inside = key_row <= query_row
                allowed = inside if allowed is None else allowed & inside
            scores = jnp.where(allowed, scores, NEG)
        old_max = m_sc[unit]
        new_max = jnp.maximum(old_max, jnp.max(scores, axis=0, keepdims=True))
        prob = jnp.exp(scores - new_max)
        fade = jnp.exp(old_max - new_max)
        m_sc[unit] = new_max
        l_sc[unit] = fade * l_sc[unit] + jnp.sum(prob, axis=0, keepdims=True)
        value = v_sc[key_tile, head * head_dim:(head + 1) * head_dim, :keys]
        return fade, jnp.dot(value, prob.astype(BF16), preferred_element_type=F32)

    def block(key_tile, diagonal, bounded):
        def keys_of(unit):
            return (units[unit][1] + 1) * span if diagonal else rows

        waiting = [s_sc[unit, :keys_of(unit)] for unit in range(AHEAD)]
        for unit in range(len(units)):
            if unit + AHEAD < len(units):
                waiting.append(score(unit + AHEAD, key_tile, keys_of(unit + AHEAD)))
            elif not diagonal:
                s_sc[unit + AHEAD - len(units)] = score(unit + AHEAD - len(units), key_tile + 1, rows)
            fade, part = absorb(unit, waiting.pop(0), key_tile, diagonal, bounded)
            acc_sc[unit] = acc_sc[unit] * fade + part

    def bounded_step(key_tile, carry):
        block(key_tile, False, True)
        return carry

    def open_step(key_tile, carry):
        block(key_tile, False, False)
        return carry

    for unit in range(AHEAD):
        s_sc[unit] = score(unit, first_tile, rows)
    lax.fori_loop(first_tile, open_tile, bounded_step, 0)
    lax.fori_loop(open_tile, tile, open_step, 0)
    block(tile, True, True)
    for unit, (head, piece) in enumerate(units):
        out_ref[0, head * head_dim:(head + 1) * head_dim, piece * span:(piece + 1) * span] = (acc_sc[unit] / l_sc[unit]).astype(BF16)


def attention(normed, w_all, layer, cosines, sines, starts, parts, heads, head_dim, rows):
    seq_len, hidden = normed.shape
    tiles = seq_len // rows
    width = heads * head_dim
    per_part = tiles // parts
    span = min(256, rows)
    units = heads * rows // span
    shards, _, depth, _ = w_all.shape
    first_start = starts[::rows]
    last_start = starts[rows - 1::rows]
    tile_index = jnp.arange(tiles, dtype=jnp.int32)
    bounds = jnp.stack([first_start // rows, jnp.minimum((last_start + rows - 1) // rows, tile_index)])
    grid_spec = pltpu.PrefetchScalarGridSpec(
        num_scalar_prefetch=1,
        grid=(tiles,),
        in_specs=[
            pl.BlockSpec((rows, hidden), lambda i, b: (i, 0)),
            pl.BlockSpec((shards, 1, depth, 3 * width), lambda i, b: (0, layer, 0, 0)),
            pl.BlockSpec((head_dim // 2, rows), lambda i, b: (0, i)),
            pl.BlockSpec((head_dim // 2, rows), lambda i, b: (0, i)),
            pl.BlockSpec((1, rows), lambda i, b: (0, i)),
        ],
        out_specs=pl.BlockSpec((1, width, rows), lambda i, b: (i // per_part, 0, i % per_part)),
        scratch_shapes=[
            pltpu.VMEM((3 * width, hidden), BF16),
            pltpu.VMEM((units, head_dim, span), BF16),
            pltpu.VMEM((tiles, heads, rows, head_dim), BF16),
            pltpu.VMEM((tiles, width, rows), BF16),
            pltpu.VMEM((units, 1, span), F32),
            pltpu.VMEM((units, 1, span), F32),
            pltpu.VMEM((units, head_dim, span), F32),
            pltpu.VMEM((AHEAD, rows, span), F32),
        ],
    )
    flops = 2 * seq_len * hidden * 3 * width + 2 * seq_len * seq_len * width
    return pl.pallas_call(
        functools.partial(attention_kernel, heads, head_dim),
        grid_spec=grid_spec,
        out_shape=jax.ShapeDtypeStruct((parts, width, seq_len // parts), BF16),
        compiler_params=pltpu.CompilerParams(dimension_semantics=('arbitrary',), vmem_limit_bytes=VMEM_LIMIT),
        cost_estimate=pl.CostEstimate(flops=flops, bytes_accessed=4 * seq_len * hidden, transcendentals=seq_len * seq_len * heads // 2),
        name='attention',
    )(bounds, normed, w_all, cosines, sines, starts[None, :])


LAYER_COPIES = 24 + ShardGather.COPIES
SLOTS = 3


def layer_kernel(layer, parts, has_next, fetch, o_hbm, wo_hbm, r_ref, gain_mlp, gain_next, ints_ref, gates_ref, gate_hbm, up_hbm, down_hbm, *rest):
    if fetch:
        local_down = down_hbm
        res_ref, rows_all, down_hbm, hbuf, own_o, wo_ref, obuf, relay, wbuf, acc, inbox, route, own, send_sem, recv_sem, w_sem, local_sem = rest
    elif has_next:
        res_ref, rows_all, hbuf, own_o, wo_ref, obuf, relay, wbuf, acc, inbox, route, own, send_sem, recv_sem, w_sem, local_sem = rest
    else:
        res_ref, hbuf, own_o, wo_ref, obuf, relay, wbuf, acc, inbox, route, send_sem, recv_sem, w_sem, local_sem = rest
    me, left, right, far = ring('mp', parts)
    to_left, to_right = {'mp': left}, {'mp': right}
    wire = Wire(send_sem, recv_sem)
    shards, num_experts, _, ffn = gate_hbm.shape
    width = o_hbm.shape[1]
    tokens, hidden = res_ref.shape
    half = tokens // 2
    low, high = pl.ds(0, half), pl.ds(half, half)
    o_low, o_high = pl.ds(0, width // 2), pl.ds(width // 2, width // 2)

    def weight_copies(step):
        expert = lax.rem(step, num_experts)
        slot = lax.rem(step, SLOTS)
        return [pltpu.make_async_copy(hbm.at[:, expert], wbuf.at[slot, index], w_sem.at[slot, index]) for index, hbm in enumerate((gate_hbm, up_hbm, down_hbm))]

    ready = 2 if fetch else 3
    for step in range(SLOTS - 1):
        for copy in weight_copies(step)[:ready]:
            copy.start()
    devices = [to_left, to_right]
    if fetch:
        tok = lax.axis_index('tok')
        down_own = wbuf.at[SLOTS - 1, 0, pl.ds(0, num_experts)]
        down_load = pltpu.make_async_copy(local_down.at[layer], down_own, local_sem.at[3])
        down_load.start()
        down = ShardGather(wire, 24, down_own, down_hbm, shards)
        devices = devices + down.devices
    own_copy = pltpu.make_async_copy(o_hbm.at[me], own_o, local_sem.at[0])
    own_copy.start()
    wo_copy = pltpu.make_async_copy(wo_hbm.at[:, :, layer], wo_ref, local_sem.at[1])
    wo_copy.start()
    meet(devices)

    exchange = [
        wire.copy(0, o_hbm.at[far, o_low], relay.at[0], to_right),
        wire.copy(1, o_hbm.at[far, o_high], relay.at[1], to_left),
        wire.copy(2, o_hbm.at[right], obuf.at[0], to_right),
        wire.copy(3, o_hbm.at[left], obuf.at[1], to_left),
        wire.copy(4, relay.at[0], obuf.at[2, o_low], to_right),
        wire.copy(5, relay.at[1], obuf.at[2, o_high], to_left),
    ]
    for copy in exchange[:4]:
        copy.start()
    if fetch:
        down_load.wait()
        down.start()
        down_store = pltpu.make_async_copy(down_own, down_hbm.at[tok], local_sem.at[4])
        down_store.start()

    expert_row = lax.broadcasted_iota(jnp.int32, (num_experts, 1), 0)
    for part in range(parts):
        share = jnp.zeros((num_experts, tokens), F32)
        for choice in range(2):
            share = share + jnp.where(ints_ref[part, 1 + choice:2 + choice] == expert_row, gates_ref[part, choice:choice + 1], 0.0)
        route[part] = share.T

    exchange[0].wait_recv()
    exchange[4].start()
    exchange[1].wait_recv()
    exchange[5].start()
    own_copy.wait()
    wo_copy.wait()
    if fetch:
        down.onward()
    for copy in exchange[2:]:
        copy.wait_recv()

    chunk = min(256, tokens)

    def project(index, carry):
        span = pl.ds(pl.multiple_of(index * chunk, chunk), chunk)
        total = None
        for source, piece in ((me, own_o), (left, obuf.at[0]), (right, obuf.at[1]), (far, obuf.at[2])):
            weight = wo_ref[:, source].reshape(hidden, width)
            term = jnp.dot(weight, piece[:, span], preferred_element_type=F32)
            total = term if total is None else total + term
        residual = r_ref[span].astype(F32) + total.T
        res_ref[span] = residual
        hbuf[me, span] = rms_norm(residual, gain_mlp[...])
        return carry

    lax.fori_loop(0, tokens // chunk, project, 0)

    rows = ring_gather(wire, 6, hbuf.at[me], hbuf, 'mp', left, right, me)
    for name in FIRST:
        rows[name].start()
    if fetch:
        down.share()
        down.arrive()
        down.sent()
        down_store.wait()
        for step in range(SLOTS - 1):
            weight_copies(step)[2].start()

    sends = {
        1: wire.copy(12, acc.at[1], inbox.at[0], to_left),
        2: wire.copy(13, acc.at[2], inbox.at[1], to_right),
        3: wire.copy(14, acc.at[3], inbox.at[2], to_right),
        4: wire.copy(15, acc.at[4], inbox.at[3], to_left),
        5: wire.copy(16, acc.at[5], inbox.at[4], to_right),
        6: wire.copy(17, acc.at[6], inbox.at[5], to_left),
    }
    tile_rows = min(256, half)
    tiles = half // tile_rows
    lane = lax.broadcasted_iota(jnp.int32, (tile_rows, num_experts), 1)
    steps = 8 * num_experts

    def expert_step(step, carry):
        phase = step // num_experts
        expert = lax.rem(step, num_experts)
        slot = lax.rem(step, SLOTS)
        late = phase // 4
        near = phase + late * (7 - 2 * phase)
        is_zero = ((3 - near) * (2 - near) * (1 - near)) // 6
        is_one = (near * (3 - near) * (2 - near)) // 2
        is_two = (near * (3 - near) * (near - 1)) // 2
        shift = near - 1 + is_zero + 3 * is_one
        source = lax.rem(me + shift, parts)
        top = is_two + late * (1 - 2 * is_two)
        start = pl.multiple_of(top * half, half)

        @pl.when(step + SLOTS - 1 < steps)
        def _():
            for copy in weight_copies(step + SLOTS - 1):
                copy.start()

        @pl.when(expert == 0)
        def _():
            acc[phase] = jnp.zeros((half, hidden), F32)

            @pl.when(phase == 1)
            def _():
                rows['right_low'].wait_recv()
                rows['on_right'].start()

            @pl.when(phase == 2)
            def _():
                sends[1].start()
                rows['left_high'].wait_recv()
                rows['on_left'].start()

            @pl.when(phase == 3)
            def _():
                sends[2].start()
                rows['on_right'].wait_recv()

            @pl.when(phase == 4)
            def _():
                sends[3].start()
                rows['on_left'].wait_recv()

            @pl.when(phase == 5)
            def _():
                sends[4].start()
                rows['left_low'].wait_recv()

            @pl.when(phase == 6)
            def _():
                rows['right_high'].wait_recv()

            @pl.when(phase == 7)
            def _():
                sends[3].wait_recv()
                acc[5] += inbox[2]
                sends[5].start()
                sends[4].wait_recv()
                acc[6] += inbox[3]
                sends[6].start()

        for copy in weight_copies(step):
            copy.wait()

        def activate(tile):
            gate_w = wbuf[slot, 0].reshape(hidden, ffn)
            up_w = wbuf[slot, 1].reshape(hidden, ffn)
            x = hbuf[source, pl.ds(start + tile * tile_rows, tile_rows)]
            gate_pre = jnp.dot(x, gate_w, preferred_element_type=F32)
            up_pre = jnp.dot(x, up_w, preferred_element_type=F32)
            return (gate_pre * (1.0 / (1.0 + jnp.exp(-gate_pre))) * up_pre).astype(BF16)

        def contract(tile, act):
            down_w = wbuf[slot, 2].reshape(hidden, ffn)
            part_share = route[source, pl.ds(start + tile * tile_rows, tile_rows)]
            share = jnp.sum(jnp.where(lane == expert, part_share, 0.0), axis=1, keepdims=True)
            mixed = lax.dot_general(act, down_w, NT, preferred_element_type=F32)
            acc[phase, tile * tile_rows:(tile + 1) * tile_rows] += share * mixed

        act = activate(0)
        for tile in range(tiles):
            following = activate(tile + 1) if tile + 1 < tiles else None
            contract(tile, act)
            act = following
        return carry

    lax.fori_loop(0, steps, expert_step, 0)

    sends[1].wait_recv()
    res_ref[low] += acc[0] + inbox[0]
    sends[2].wait_recv()
    res_ref[high] += acc[7] + inbox[1]
    sends[5].wait_recv()
    res_ref[low] += inbox[4]
    if has_next:
        own[low] = rms_norm(res_ref[low], gain_next[...])
    sends[6].wait_recv()
    res_ref[high] += inbox[5]
    for copy in exchange + list(rows.values()) + list(sends.values()):
        copy.wait_send()
    if has_next:
        own[high] = rms_norm(res_ref[high], gain_next[...])
        rows_next = ring_gather(wire, 18, own, rows_all, 'mp', left, right, me)
        for name in FIRST:
            rows_next[name].start()
        rows_local = pltpu.make_async_copy(own, rows_all.at[me], local_sem.at[2])
        rows_local.start()
        rows_next['right_low'].wait_recv()
        rows_next['on_right'].start()
        rows_next['left_high'].wait_recv()
        rows_next['on_left'].start()
        for name in ('right_high', 'left_low', 'on_right', 'on_left'):
            rows_next[name].wait_recv()
        for copy in rows_next.values():
            copy.wait_send()
        rows_local.wait()


def layer_rest(layer, has_next, fetch, parts, heads_out, out_all, residual, gain_mlp, gain_next, ints_all, gates_all, gate_weight, up_weight, down_weight):
    _, width, tokens = heads_out.shape
    hidden = residual.shape[1]
    shards, num_experts, depth, ffn = gate_weight.shape
    half = tokens // 2
    anywhere = pl.BlockSpec(memory_space=pl.ANY)
    vmem = pl.BlockSpec(memory_space=pltpu.VMEM)
    out_shape = [jax.ShapeDtypeStruct((tokens, hidden), F32)]
    out_specs = [vmem]
    scratch = [
        pltpu.VMEM((parts, tokens, hidden), BF16),
        pltpu.VMEM((width, tokens), BF16),
        pltpu.VMEM((shards, parts, depth, width), BF16),
        pltpu.VMEM((3, width, tokens), BF16),
        pltpu.VMEM((2, width // 2, tokens), BF16),
        pltpu.VMEM((SLOTS, 3, shards, depth, ffn), BF16),
        pltpu.VMEM((8, half, hidden), F32),
        pltpu.VMEM((6, half, hidden), F32),
        pltpu.VMEM((parts, tokens, num_experts), F32),
    ]
    if has_next:
        out_shape.append(jax.ShapeDtypeStruct((parts, tokens, hidden), BF16))
        out_specs.append(anywhere)
        scratch.append(pltpu.VMEM((tokens, hidden), BF16))
    if fetch:
        out_shape.append(jax.ShapeDtypeStruct((shards, num_experts, depth, ffn), BF16))
        out_specs.append(anywhere)
    scratch += [
        pltpu.SemaphoreType.DMA((LAYER_COPIES,)),
        pltpu.SemaphoreType.DMA((LAYER_COPIES,)),
        pltpu.SemaphoreType.DMA((SLOTS, 3)),
        pltpu.SemaphoreType.DMA((5,)),
    ]
    return pl.pallas_call(
        functools.partial(layer_kernel, layer, parts, has_next, fetch),
        in_specs=[
            anywhere, anywhere,
            vmem, vmem, vmem, vmem, vmem,
            anywhere, anywhere, anywhere,
        ],
        out_specs=out_specs,
        out_shape=out_shape,
        scratch_shapes=scratch,
        compiler_params=pltpu.CompilerParams(collective_id=1 + layer, has_side_effects=True, vmem_limit_bytes=VMEM_LIMIT),
        cost_estimate=pl.CostEstimate(
            flops=6 * parts * tokens * hidden * ffn * num_experts,
            bytes_accessed=8 * 6 * num_experts * hidden * ffn,
            transcendentals=parts * tokens * ffn * num_experts,
        ),
        name='layer_rest',
    )(heads_out, out_all, residual, gain_mlp, gain_next, ints_all, gates_all, gate_weight, up_weight, down_weight)


def solution(mesh):
    token_spec = P(('rep', 'tok', 'mp'))
    row_spec = P(('rep', 'tok', 'mp'), None)
    head_weight = P(None, 'tok', 'mp', None)
    in_specs = (row_spec, token_spec, row_spec, row_spec, head_weight, head_weight, head_weight, P(None, 'mp', None, 'tok'), P(None, None, 'tok', 'mp'), P(None, None, 'tok', 'mp'), P(None, None, 'mp', 'tok'), P(None, None), P(None, None))
    parts = mesh.shape['mp']
    shards = mesh.shape['tok']

    def device_step(hidden_in, seg_ids, expert_ids, expert_gates, w_query, w_key, w_value, w_out, w_gate, w_up, w_down, gain_attn, gain_mlp):
        num_layers, depth, heads, head_dim = w_query.shape
        tokens, hidden = hidden_in.shape
        seq_len = tokens * parts
        width = heads * head_dim

        def fetch(layer, w_gate, w_up, w_down):
            gate_weight = lax.all_gather(w_gate[layer], 'tok', axis=0)
            up_weight = lax.all_gather(w_up[layer], 'tok', axis=0)
            down_weight = lax.all_gather(jnp.swapaxes(w_down[layer], 1, 2), 'tok', axis=0) if layer else jnp.swapaxes(w_down, 2, 3)
            return gate_weight, up_weight, down_weight

        weights = [fetch(0, w_gate, w_up, w_down)]

        qkv_local = jnp.concatenate([w.reshape(num_layers, depth, width) for w in (w_query, w_key, w_value)], axis=2)
        out_local = jnp.swapaxes(w_out.reshape(num_layers, width, depth), 1, 2)
        ints = jnp.concatenate([seg_ids[None, :], expert_ids.T, jnp.zeros((5, tokens), jnp.int32)], axis=0)
        gates = jnp.concatenate([expert_gates.T, jnp.zeros((6, tokens), F32)], axis=0)
        rows_all, ints_all, gates_all, qkv_all, out_all = gather_start(hidden_in, gain_attn[:1], ints, gates, qkv_local, out_local, parts, shards)

        ints_all, *later = lax.optimization_barrier((ints_all, w_gate, w_up, w_down))
        for layer in range(1, num_layers):
            weights.append(fetch(layer, *later))

        starts = request_starts(ints_all[:, 0].reshape(seq_len))
        positions = (jnp.arange(seq_len, dtype=jnp.int32) - starts).astype(F32)
        inv_freq = jnp.power(ROPE_BASE, -jnp.arange(head_dim // 2, dtype=F32) * 2.0 / head_dim)
        angles = inv_freq[:, None] * positions[None, :]
        cosines = jnp.cos(angles)
        sines = jnp.sin(angles)

        residual = hidden_in
        for layer in range(num_layers):
            has_next = layer + 1 < num_layers
            heads_out = attention(rows_all.reshape(seq_len, hidden), qkv_all, layer, cosines, sines, starts, parts, heads, head_dim, min(512, tokens))
            following = gain_attn[layer + 1:layer + 2] if has_next else gain_attn[layer:layer + 1]
            outs = layer_rest(layer, has_next, layer == 0, parts, heads_out, out_all, residual, gain_mlp[layer:layer + 1], following, ints_all, gates_all, *weights[layer])
            residual = outs[0]
            rows_all = outs[1] if has_next else None
        return residual

    return jax.shard_map(device_step, mesh=mesh, in_specs=in_specs, out_specs=row_spec, check_vma=False)
```

```python
import functools

import jax
import jax.numpy as jnp
from jax import lax
from jax.experimental import pallas as pl
from jax.experimental.pallas import tpu as pltpu
from jax.sharding import PartitionSpec as P

EPS = 1e-5
ROPE_BASE = 10000.0
NEG = -1e30
VMEM_LIMIT = 63 * 1024 * 1024
AHEAD = 2
SLOTS = 3
F32 = jnp.float32
BF16 = jnp.bfloat16
NT = (((1,), (1,)), ((), ()))
MESH = pl.DeviceIdType.MESH
FIRST = ('right_low', 'left_high', 'right_high', 'left_low')


def rms_norm(residual, gain):
    inv_rms = lax.rsqrt(jnp.mean(residual * residual, axis=-1, keepdims=True) + EPS)
    return (residual * inv_rms * gain.astype(F32)).astype(BF16)


class Wire:
    def __init__(self, send_sem, recv_sem):
        self.send_sem = send_sem
        self.recv_sem = recv_sem

    def copy(self, slot, src, dst, device):
        return pltpu.make_async_remote_copy(src_ref=src, dst_ref=dst, send_sem=self.send_sem.at[slot], recv_sem=self.recv_sem.at[slot], device_id=device, device_id_type=MESH)


def ring(axis, size):
    me = lax.axis_index(axis)
    return me, lax.rem(me + size - 1, size), lax.rem(me + 1, size), lax.rem(me + size // 2, size)


def meet(devices):
    barrier = pltpu.get_barrier_semaphore()
    for device in devices:
        pl.semaphore_signal(barrier, inc=1, device_id=device, device_id_type=MESH)
    pl.semaphore_wait(barrier, len(devices))


def ring_gather(wire, base, own, rows_all, axis, left, right, me):
    half = own.shape[0] // 2
    low, high = pl.ds(0, half), pl.ds(half, half)
    to_right, to_left = {axis: right}, {axis: left}
    return {
        'right_low': wire.copy(base, own.at[low], rows_all.at[me, low], to_right),
        'right_high': wire.copy(base + 1, own.at[high], rows_all.at[me, high], to_right),
        'left_high': wire.copy(base + 2, own.at[high], rows_all.at[me, high], to_left),
        'left_low': wire.copy(base + 3, own.at[low], rows_all.at[me, low], to_left),
        'on_right': wire.copy(base + 4, rows_all.at[left, low], rows_all.at[left, low], to_right),
        'on_left': wire.copy(base + 5, rows_all.at[right, high], rows_all.at[right, high], to_left),
    }


def tok_devices(shards):
    tok = lax.axis_index('tok')
    return [{'tok': tok + 1 - 2 * lax.rem(tok, 2)}, {'tok': lax.rem(tok + shards - 2, shards)}, {'tok': lax.rem(tok + 2, shards)}]


class ShardGather:
    COPIES = 10

    def __init__(self, wire, base, own, blocks, shards, store_sem=None):
        tok = lax.axis_index('tok')
        left = lax.rem(tok + shards - 2, shards)
        right = lax.rem(tok + 2, shards)
        far = lax.rem(tok + shards // 2, shards)
        partner = {'tok': tok + 1 - 2 * lax.rem(tok, 2)}
        self.rows = ring_gather(wire, base, own, blocks, 'tok', left, right, tok)
        self.cross = [wire.copy(base + 6, own, blocks.at[tok], partner)]
        for index, source in enumerate((left, right, far)):
            self.cross.append(wire.copy(base + 7 + index, blocks.at[source], blocks.at[source], partner))
        self.store = None if store_sem is None else pltpu.make_async_copy(own, blocks.at[tok], store_sem)

    def start(self):
        for name in FIRST:
            self.rows[name].start()
        self.cross[0].start()
        if self.store is not None:
            self.store.start()

    def onward(self):
        self.rows['right_low'].wait_recv()
        self.rows['on_right'].start()
        self.rows['left_high'].wait_recv()
        self.rows['on_left'].start()

    def share_near(self):
        self.rows['right_high'].wait_recv()
        self.cross[1].start()
        self.rows['left_low'].wait_recv()
        self.cross[2].start()

    def share_far(self):
        self.rows['on_right'].wait_recv()
        self.rows['on_left'].wait_recv()
        self.cross[3].start()

    def finish(self):
        for copy in self.cross:
            copy.wait_recv()
        for copy in list(self.rows.values()) + self.cross:
            copy.wait_send()
        if self.store is not None:
            self.store.wait()


def request_tables(parts, ints, inv_ref, cos_ref, sin_ref, start_ref):
    tokens = ints.shape[-1]
    half = tokens // 2
    lane = lax.broadcasted_iota(jnp.int32, (8, tokens), 1)
    carry = last = None
    for part in range(parts):
        seg = jnp.broadcast_to(ints[part, 0:1], (8, tokens))
        before = pltpu.roll(seg, 1, 1)
        if part == 0:
            fresh = (lane == 0) | (seg != before)
        else:
            fresh = seg != jnp.where(lane == 0, last, before)
        start = jnp.where(fresh, lane + part * tokens, 0)
        shift = 1
        while shift < tokens:
            start = jnp.maximum(start, jnp.where(lane >= shift, pltpu.roll(start, shift, 1), 0))
            shift *= 2
        if carry is not None:
            start = jnp.maximum(start, carry)
        carry = jnp.broadcast_to(start[:, tokens - 1:], (8, tokens))
        last = jnp.broadcast_to(seg[:, tokens - 1:], (8, tokens))
        angles = inv_ref[...] * (lane + part * tokens - start)[0:1].astype(F32)
        cosines = jnp.cos(angles)
        sines = jnp.sin(angles)
        for piece in range(2):
            span = slice(piece * half, (piece + 1) * half)
            start_ref[2 * part + piece] = start[:, span]
            cos_ref[2 * part + piece] = cosines[:, span]
            sin_ref[2 * part + piece] = sines[:, span]


def exchange_heads(wire, base, o_all, obuf, relay, me, left, right, far):
    width = o_all.shape[1]
    low, high = pl.ds(0, width // 2), pl.ds(width // 2, width // 2)
    to_left, to_right = {'mp': left}, {'mp': right}
    return [
        wire.copy(base, o_all.at[far, low], relay.at[0], to_right),
        wire.copy(base + 1, o_all.at[far, high], relay.at[1], to_left),
        wire.copy(base + 2, o_all.at[right], obuf.at[0], to_right),
        wire.copy(base + 3, o_all.at[left], obuf.at[1], to_left),
        wire.copy(base + 4, relay.at[0], obuf.at[2, low], to_right),
        wire.copy(base + 5, relay.at[1], obuf.at[2, high], to_left),
    ]


def own_blocks(experts, keys):
    group = experts[0].shape[1] // 2
    return [experts[matrix].at[layer, pl.ds(side * group, group)] for layer, matrix, side in keys]


def attend_kernel(first, layer, parts, shards, heads, head_dim, fetch_keys, *refs):
    refs = list(refs)
    num_fetch = len(fetch_keys)
    r_ref, gain_attn, gain_mlp = refs[:3]
    del refs[:3]
    if first:
        inv_ref, ints_ref, gates_ref, qkv_ref, out_ref = refs[:5]
        del refs[:5]
    else:
        cos_in, sin_in, start_in, qkv_all, out_all = refs[:5]
        del refs[:5]
    fetch_own = own_blocks(refs[:3], fetch_keys)
    del refs[:3]
    res_ref, h_ref = refs[:2]
    del refs[:2]
    if first:
        ints_all, gates_all, qkv_all, out_all, cos_ref, sin_ref, start_ref = refs[:7]
        del refs[:7]
    fetch_all = refs[:num_fetch]
    del refs[:num_fetch]
    if not first:
        cos_ref, sin_ref, start_ref = refs[:3]
        del refs[:3]
    if first:
        ints_out = ints_all
        ints_all = refs.pop(0)
    hbuf, w_raw, w_sc, q_sc, k_sc, v_sc, m_sc, l_sc, acc_sc, s_sc, o_all, obuf, relay, wo_ref = refs[:14]
    send_sem, recv_sem, local_sem = refs[14:]

    me, left, right, far = ring('mp', parts)
    tok = lax.axis_index('tok')
    to_left, to_right = {'mp': left}, {'mp': right}
    wire = Wire(send_sem, recv_sem)
    tokens, hidden = res_ref.shape
    rows = tokens // 2
    width = heads * head_dim
    span = q_sc.shape[-1]
    pieces = rows // span
    tiles = 2 * parts
    units = [(head, piece) for head in range(heads) for piece in range(pieces)]

    fetches = [ShardGather(wire, 41 + index * ShardGather.COPIES, own, blocks, shards, local_sem.at[8 + index]) for index, (own, blocks) in enumerate(zip(fetch_own, fetch_all))]
    if first:
        qkv = ShardGather(wire, 21, qkv_ref, qkv_all, shards, local_sem.at[3])
        out = ShardGather(wire, 31, out_all.at[tok], out_all, shards)
    meet([to_left, to_right] + tok_devices(shards))
    if first:
        qkv.start()
        small = [
            wire.copy(0, ints_ref, ints_all.at[me], to_right),
            wire.copy(1, ints_ref, ints_all.at[me], to_left),
            wire.copy(2, gates_ref, gates_all.at[me], to_right),
            wire.copy(3, gates_ref, gates_all.at[me], to_left),
            wire.copy(4, out_ref, out_all.at[tok, me], to_right),
            wire.copy(5, out_ref, out_all.at[tok, me], to_left),
        ]
        onward = [
            wire.copy(6, ints_all.at[left], ints_all.at[left], to_right),
            wire.copy(7, gates_all.at[right], gates_all.at[right], to_left),
            wire.copy(8, out_all.at[tok, left], out_all.at[tok, left], to_right),
        ]
        ints_all[me] = ints_ref[...]
        local = [
            pltpu.make_async_copy(gates_ref, gates_all.at[me], local_sem.at[1]),
            pltpu.make_async_copy(out_ref, out_all.at[tok, me], local_sem.at[2]),
        ]
        for copy in small + local:
            copy.start()
    else:
        local = [
            pltpu.make_async_copy(qkv_all.at[:, layer], w_raw, local_sem.at[3]),
            pltpu.make_async_copy(cos_in, cos_ref, local_sem.at[0]),
            pltpu.make_async_copy(sin_in, sin_ref, local_sem.at[1]),
            pltpu.make_async_copy(start_in, start_ref, local_sem.at[2]),
        ]
        for copy in local:
            copy.start()
    hbuf[me] = rms_norm(r_ref[...].astype(F32), gain_attn[...])
    rows_in = ring_gather(wire, 9, hbuf.at[me], hbuf, 'mp', left, right, me)
    for name in FIRST:
        rows_in[name].start()
    if first:
        for copy in small:
            copy.wait_recv()
        for copy in onward:
            copy.start()
        qkv.onward()
        onward[0].wait_recv()
        request_tables(parts, ints_all, inv_ref, cos_ref, sin_ref, start_ref)
        ints_out[...] = ints_all[...]
        onward[2].wait_recv()
        local[1].wait()
        out.start()
        for fetch in fetches:
            fetch.start()
        qkv.share_near()
        qkv.share_far()
        qkv.finish()
        load = pltpu.make_async_copy(qkv_all.at[:, layer], w_raw, local_sem.at[4])
        load.start()
        load.wait()
    else:
        for fetch in fetches:
            fetch.start()
        for copy in local:
            copy.wait()
    w_sc[...] = w_raw[...].reshape(hidden, 3 * width).astype(F32).T.astype(BF16)

    half_dim = head_dim // 2
    scale = head_dim ** -0.5

    def tile_of(index):
        pair = index // 2
        odd = lax.rem(index, 2)
        between = (pair * (3 - pair)) // 2
        last_pair = (pair * (pair - 1) * (pair - 2)) // 6
        third = (pair * (pair - 1) * (3 - pair)) // 2
        chunk = lax.rem(me + between * (3 - 2 * odd) + 2 * last_pair, parts)
        side = odd + third * (1 - 2 * odd)
        return chunk, side

    def score(unit, query_tile, key_tile, keys):
        head, _ = units[unit]
        return jnp.dot(k_sc[key_tile, head, :keys], q_sc[query_tile, unit], preferred_element_type=F32)

    def absorb(unit, scores, query_tile, key_tile, causal):
        head, piece = units[unit]
        keys = scores.shape[0]
        key_row = lax.broadcasted_iota(jnp.int32, (keys, span), 0)
        allowed = key_row >= start_ref[query_tile, 0:1, piece * span:(piece + 1) * span] - key_tile * rows
        if causal:
            allowed = allowed & (key_row <= lax.broadcasted_iota(jnp.int32, (keys, span), 1) + piece * span)
        scores = jnp.where(allowed, scores, NEG)
        old_max = m_sc[query_tile, unit:unit + 1]
        new_max = jnp.maximum(old_max, jnp.max(scores, axis=0, keepdims=True))
        prob = jnp.exp(scores - new_max)
        fade = jnp.exp(old_max - new_max)
        m_sc[query_tile, unit:unit + 1] = new_max
        l_sc[query_tile, unit:unit + 1] = fade * l_sc[query_tile, unit:unit + 1] + jnp.sum(prob, axis=0, keepdims=True)
        value = v_sc[key_tile, head * head_dim:(head + 1) * head_dim, :keys]
        part = jnp.dot(value, prob.astype(BF16), preferred_element_type=F32)
        acc_sc[query_tile, unit] = acc_sc[query_tile, unit] * fade + part

    def block(query_tile, key_tile, following):
        diagonal = following is None

        def keys_of(unit):
            return (units[unit][1] + 1) * span if diagonal else rows

        waiting = [s_sc[unit, :keys_of(unit)] for unit in range(AHEAD)]
        for unit in range(len(units)):
            ahead = unit + AHEAD
            if ahead < len(units):
                waiting.append(score(ahead, query_tile, key_tile, keys_of(ahead)))
            elif not diagonal:
                s_sc[ahead - len(units)] = score(ahead - len(units), following[0], following[1], rows)
            absorb(unit, waiting.pop(0), query_tile, key_tile, diagonal)

    def arrive(index, carry):
        chunk, side = tile_of(index)
        tile = 2 * chunk + side

        @pl.when(index == 2)
        def _():
            rows_in['right_low'].wait_recv()
            rows_in['on_right'].start()

        @pl.when(index == 3)
        def _():
            rows_in['left_high'].wait_recv()
            rows_in['on_left'].start()
            if first:
                out.onward()

        @pl.when(index == 4)
        def _():
            rows_in['right_high'].wait_recv()

        @pl.when(index == 5)
        def _():
            rows_in['left_low'].wait_recv()

        @pl.when(index == 6)
        def _():
            rows_in['on_right'].wait_recv()
            for fetch in fetches:
                fetch.onward()
            if first:
                out.share_near()
                out.share_far()

        @pl.when(index == 7)
        def _():
            rows_in['on_left'].wait_recv()

        x = hbuf[chunk, pl.ds(pl.multiple_of(side * rows, rows), rows)]
        qkv_rows = lax.dot_general(w_sc[...], x, NT, preferred_element_type=F32)
        cosines = cos_ref[tile]
        sines = sin_ref[tile]

        def rotate(base):
            one = qkv_rows[base:base + half_dim]
            two = qkv_rows[base + half_dim:base + head_dim]
            return jnp.concatenate([one * cosines - two * sines, two * cosines + one * sines], axis=0)

        for head in range(heads):
            base = head * head_dim
            query = (rotate(base).astype(BF16).astype(F32) * scale).astype(BF16)
            for piece in range(pieces):
                q_sc[tile, head * pieces + piece] = query[:, piece * span:(piece + 1) * span]
            k_sc[tile, head] = rotate(width + base).T.astype(BF16)
        v_sc[tile] = qkv_rows[2 * width:3 * width].astype(BF16)
        m_sc[tile] = jnp.full(m_sc.shape[1:], NEG, F32)
        l_sc[tile] = jnp.zeros(l_sc.shape[1:], F32)
        acc_sc[tile] = jnp.zeros(acc_sc.shape[1:], F32)

        def ordered(other):
            other_chunk, other_side = tile_of(other)
            other_tile = 2 * other_chunk + other_side
            ahead = (tile - other_tile + tiles) // tiles
            upper = other_tile + ahead * (tile - other_tile)
            return upper, tile + other_tile - upper

        upper, lower = ordered(jnp.int32(0))
        for unit in range(AHEAD):
            s_sc[unit] = score(unit, upper, lower, rows)

        def pair(other, inner):
            query_tile, key_tile = ordered(other)
            block(query_tile, key_tile, ordered(other + 1))
            return inner

        lax.fori_loop(0, index, pair, 0)
        block(tile, tile, None)
        return carry

    lax.fori_loop(0, tiles, arrive, 0)
    wo_copy = pltpu.make_async_copy(out_all.at[:, :, layer], wo_ref, local_sem.at[5])
    if first:
        out.finish()
    wo_copy.start()
    for tile in range(tiles):
        for unit, (head, piece) in enumerate(units):
            top = head * head_dim
            edge = (tile % 2) * rows + piece * span
            o_all[tile // 2, top:top + head_dim, edge:edge + span] = (acc_sc[tile, unit] / l_sc[tile, unit:unit + 1]).astype(BF16)

    exchange = exchange_heads(wire, 15, o_all, obuf, relay, me, left, right, far)
    for copy in exchange[:4]:
        copy.start()
    for fetch in fetches:
        fetch.share_near()
    exchange[0].wait_recv()
    exchange[4].start()
    exchange[1].wait_recv()
    exchange[5].start()
    wo_copy.wait()
    chunk = min(256, tokens)

    def project(sources, last):
        def step(index, carry):
            lanes = pl.ds(pl.multiple_of(index * chunk, chunk), chunk)
            total = None
            for source, piece in sources:
                weight = wo_ref[:, source].reshape(hidden, width)
                term = jnp.dot(weight, piece[:, lanes], preferred_element_type=F32)
                total = term if total is None else total + term
            residual = (res_ref[lanes] if last else r_ref[lanes].astype(F32)) + total.T
            res_ref[lanes] = residual
            if last:
                h_ref[lanes] = rms_norm(residual, gain_mlp[...])
            return carry

        lax.fori_loop(0, tokens // chunk, step, 0)

    project([(me, o_all.at[me])], False)
    exchange[2].wait_recv()
    exchange[3].wait_recv()
    exchange[4].wait_recv()
    exchange[5].wait_recv()
    project([(left, obuf.at[0]), (right, obuf.at[1]), (far, obuf.at[2])], True)

    for fetch in fetches:
        fetch.share_far()
    for fetch in fetches:
        fetch.finish()
    for copy in exchange + list(rows_in.values()):
        copy.wait_send()
    if first:
        onward[1].wait_recv()
        for copy in small + onward:
            copy.wait_send()
        local[0].wait()


def attend(first, layer, parts, shards, heads, head_dim, residual, gain_attn, gain_mlp, side_inputs, experts, fetch_keys, gathered_shape, ints_shape):
    tokens, hidden = residual.shape
    rows = tokens // 2
    width = heads * head_dim
    tiles = 2 * parts
    span = min(256, rows)
    units = heads * rows // span
    depth = hidden // shards
    anywhere = pl.BlockSpec(memory_space=pl.ANY)
    vmem = pl.BlockSpec(memory_space=pltpu.VMEM)
    num_fetch = len(fetch_keys)
    in_specs = [vmem] * 3 + ([vmem] * 3 + [vmem] * 2 if first else [anywhere] * 5) + [anywhere] * 3
    out_shape = [jax.ShapeDtypeStruct((tokens, hidden), F32), jax.ShapeDtypeStruct((tokens, hidden), BF16)]
    out_specs = [vmem, vmem]
    tables = [((tiles, head_dim // 2, rows), F32), ((tiles, head_dim // 2, rows), F32), ((tiles, 8, rows), jnp.int32)]
    if first:
        out_shape += [
            jax.ShapeDtypeStruct((parts,) + ints_shape, jnp.int32),
            jax.ShapeDtypeStruct((parts,) + ints_shape, F32),
            jax.ShapeDtypeStruct((shards,) + side_inputs[3].shape, BF16),
            jax.ShapeDtypeStruct((shards, parts) + side_inputs[4].shape, BF16),
        ] + [jax.ShapeDtypeStruct(shape, dtype) for shape, dtype in tables]
        out_specs += [vmem, anywhere, anywhere, anywhere] + [vmem] * 3
    out_shape += [jax.ShapeDtypeStruct((shards,) + gathered_shape, BF16)] * num_fetch
    out_specs += [anywhere] * num_fetch
    scratch = [pltpu.VMEM((parts,) + ints_shape, jnp.int32)] if first else [pltpu.VMEM(shape, dtype) for shape, dtype in tables]
    copies = 41 + num_fetch * ShardGather.COPIES
    scratch += [
        pltpu.VMEM((parts, tokens, hidden), BF16),
        pltpu.VMEM((shards, depth, 3 * width), BF16),
        pltpu.VMEM((3 * width, hidden), BF16),
        pltpu.VMEM((tiles, units, head_dim, span), BF16),
        pltpu.VMEM((tiles, heads, rows, head_dim), BF16),
        pltpu.VMEM((tiles, width, rows), BF16),
        pltpu.VMEM((tiles, max(8, units), span), F32),
        pltpu.VMEM((tiles, max(8, units), span), F32),
        pltpu.VMEM((tiles, units, head_dim, span), F32),
        pltpu.VMEM((AHEAD, rows, span), F32),
        pltpu.VMEM((parts, width, tokens), BF16),
        pltpu.VMEM((3, width, tokens), BF16),
        pltpu.VMEM((2, width // 2, tokens), BF16),
        pltpu.VMEM((shards, parts, depth, width), BF16),
        pltpu.SemaphoreType.DMA((copies,)),
        pltpu.SemaphoreType.DMA((copies,)),
        pltpu.SemaphoreType.DMA((8 + max(1, num_fetch),)),
    ]
    seq_len = parts * tokens
    return pl.pallas_call(
        functools.partial(attend_kernel, first, layer, parts, shards, heads, head_dim, tuple(fetch_keys)),
        in_specs=in_specs,
        out_specs=out_specs,
        out_shape=out_shape,
        scratch_shapes=scratch,
        compiler_params=pltpu.CompilerParams(collective_id=2 * layer, has_side_effects=True, vmem_limit_bytes=VMEM_LIMIT),
        cost_estimate=pl.CostEstimate(flops=2 * seq_len * seq_len * width + 8 * seq_len * hidden * width, bytes_accessed=8 * seq_len * hidden, transcendentals=seq_len * seq_len * heads // 2),
        name='attend',
    )(residual, gain_attn, gain_mlp, *side_inputs, *experts)


def mix_kernel(parts, shards, late_keys, next_keys, late_mats, *refs):
    refs = list(refs)
    num_late = len(late_keys)
    num_next = len(next_keys)
    r_ref, h_ref, ints_ref, gates_ref = refs[:4]
    del refs[:4]
    given = refs[:6 - num_late]
    del refs[:6 - num_late]
    late_own = own_blocks(refs[:3], late_keys)
    next_own = own_blocks(refs[:3], next_keys)
    del refs[:3]
    res_ref = refs.pop(0)
    late_all = refs[:num_late]
    del refs[:num_late]
    next_all = refs[:num_next]
    del refs[:num_next]
    hbuf, wbuf, acc, inbox, route, send_sem, recv_sem, w_sem, local_sem = refs
    mats = list(given)
    for position, ref in zip(late_mats, late_all):
        mats.insert(position, ref)

    me, left, right, _ = ring('mp', parts)
    to_left, to_right = {'mp': left}, {'mp': right}
    wire = Wire(send_sem, recv_sem)
    _, group, depth, ffn = mats[0].shape
    num_experts = 2 * group
    tokens, hidden = res_ref.shape
    half = tokens // 2
    low, high = pl.ds(0, half), pl.ds(half, half)
    steps = 16 * group
    gate_step = 4 * group - (SLOTS - 1)

    def place(step):
        turn = lax.div(step, group)
        second = lax.div(turn + 12, 16)
        third = lax.div(turn + 10, 16)
        fourth = lax.div(turn + 2, 16)
        main = lax.div(turn, 2) + 1
        buffer = turn - 2 * second + third * (main + 2 - turn) + fourth * (turn - 14 - main)
        late = second * (1 - third) + third * (1 - fourth) * lax.rem(turn, 2) + fourth
        return turn, buffer, late, lax.rem(step, group)

    def weight_copies(step, side):
        _, _, _, expert = place(step)
        slot = lax.rem(step, SLOTS)
        return [pltpu.make_async_copy(mats[2 * index + side].at[:, expert], wbuf.at[slot, index], w_sem.at[slot, index]) for index in range(3)]

    def start_weights(step):
        _, _, late, _ = place(step)
        for side in range(2):

            @pl.when(late == side)
            def _(side=side):
                for copy in weight_copies(step, side):
                    copy.start()

    late_fetch = [ShardGather(wire, 12 + index * ShardGather.COPIES, own, blocks, shards, local_sem.at[index]) for index, (own, blocks) in enumerate(zip(late_own, late_all))]
    base = 12 + num_late * ShardGather.COPIES
    next_fetch = [ShardGather(wire, base + index * ShardGather.COPIES, own, blocks, shards, local_sem.at[num_late + index]) for index, (own, blocks) in enumerate(zip(next_own, next_all))]
    for step in range(SLOTS - 1):
        start_weights(jnp.int32(step))
    meet([to_left, to_right] + (tok_devices(shards) if late_fetch or next_fetch else []))
    rows_in = ring_gather(wire, 0, h_ref, hbuf, 'mp', left, right, me)
    for name in FIRST:
        rows_in[name].start()
    for fetch in late_fetch:
        fetch.start()
    hbuf[me] = h_ref[...]
    expert_row = lax.broadcasted_iota(jnp.int32, (num_experts, 1), 0)
    for part in range(parts):
        share = jnp.zeros((num_experts, tokens), F32)
        for choice in range(2):
            share = share + jnp.where(ints_ref[part, 1 + choice:2 + choice] == expert_row, gates_ref[part, choice:choice + 1], 0.0)
        route[part] = share.T

    sends = {
        2: wire.copy(6, acc.at[2], inbox.at[0], to_left),
        3: wire.copy(7, acc.at[3], inbox.at[1], to_right),
        4: wire.copy(8, acc.at[4], inbox.at[2], to_right),
        5: wire.copy(9, acc.at[5], inbox.at[3], to_left),
        6: wire.copy(10, acc.at[6], inbox.at[4], to_right),
        7: wire.copy(11, acc.at[7], inbox.at[5], to_left),
    }
    tile_rows = min(256, half)
    tiles = half // tile_rows
    lane = lax.broadcasted_iota(jnp.int32, (tile_rows, num_experts), 1)

    def begin(turn, buffer):
        @pl.when((turn < 4) | ((turn > 5) & (turn < 14) & (lax.rem(turn, 2) == 0)))
        def _():
            acc[buffer] = jnp.zeros((half, hidden), F32)

        @pl.when(turn == 2)
        def _():
            rows_in['right_low'].wait_recv()
            rows_in['on_right'].start()
            for fetch in late_fetch:
                fetch.onward()

        @pl.when(turn == 3)
        def _():
            rows_in['left_high'].wait_recv()
            rows_in['on_left'].start()
            for fetch in late_fetch:
                fetch.share_near()

        @pl.when(turn == 5)
        def _():
            sends[2].start()

        @pl.when(turn == 6)
        def _():
            sends[3].start()
            rows_in['on_right'].wait_recv()

        @pl.when(turn == 8)
        def _():
            sends[4].start()
            rows_in['on_left'].wait_recv()

        @pl.when(turn == 10)
        def _():
            sends[5].start()
            rows_in['left_low'].wait_recv()
            for fetch in next_fetch:
                fetch.onward()
                fetch.share_near()

        @pl.when(turn == 12)
        def _():
            rows_in['right_high'].wait_recv()

        @pl.when(turn == 14)
        def _():
            sends[4].wait_recv()
            acc[6] += inbox[2]
            sends[6].start()
            sends[5].wait_recv()
            acc[7] += inbox[3]
            sends[7].start()
            for fetch in next_fetch:
                fetch.share_far()

    def expert_step(step, carry):
        turn, buffer, late, index = place(step)
        slot = lax.rem(step, SLOTS)
        expert = late * group + index
        pair = lax.div(buffer, 2)
        side = lax.rem(buffer, 2)
        odd = lax.rem(pair, 2)
        upper = lax.div(pair, 2)
        shift = odd * (upper * (1 + 2 * side) + (1 - upper) * (3 - 2 * side)) + (1 - odd) * 2 * upper
        source = lax.rem(me + shift, parts)
        start = pl.multiple_of(side * half, half)

        if late_fetch or next_fetch:

            @pl.when(step == gate_step)
            def _():
                for fetch in late_fetch:
                    fetch.share_far()
                for fetch in late_fetch:
                    fetch.finish()
                for fetch in next_fetch:
                    fetch.start()

        @pl.when(step + SLOTS - 1 < steps)
        def _():
            start_weights(step + SLOTS - 1)

        @pl.when(index == 0)
        def _():
            begin(turn, buffer)

        for copy in weight_copies(step, 0):
            copy.wait()

        def activate(tile):
            gate_w = wbuf[slot, 0].reshape(hidden, ffn)
            up_w = wbuf[slot, 1].reshape(hidden, ffn)
            x = hbuf[source, pl.ds(start + tile * tile_rows, tile_rows)]
            gate_pre = jnp.dot(x, gate_w, preferred_element_type=F32)
            up_pre = jnp.dot(x, up_w, preferred_element_type=F32)
            return (gate_pre * (1.0 / (1.0 + jnp.exp(-gate_pre))) * up_pre).astype(BF16)

        def contract(tile, act):
            down_w = wbuf[slot, 2].reshape(hidden, ffn)
            part_share = route[source, pl.ds(start + tile * tile_rows, tile_rows)]
            share = jnp.sum(jnp.where(lane == expert, part_share, 0.0), axis=1, keepdims=True)
            mixed = lax.dot_general(act, down_w, NT, preferred_element_type=F32)
            acc[buffer, tile * tile_rows:(tile + 1) * tile_rows] += share * mixed

        act = activate(0)
        for tile in range(tiles):
            following = activate(tile + 1) if tile + 1 < tiles else None
            contract(tile, act)
            act = following
        return carry

    lax.fori_loop(0, steps, expert_step, 0)

    sends[2].wait_recv()
    res_ref[low] = r_ref[low] + acc[0] + inbox[0]
    sends[3].wait_recv()
    res_ref[high] = r_ref[high] + acc[1] + inbox[1]
    sends[6].wait_recv()
    res_ref[low] += inbox[4]
    sends[7].wait_recv()
    res_ref[high] += inbox[5]
    for copy in list(rows_in.values()) + list(sends.values()):
        copy.wait_send()
    for fetch in next_fetch:
        fetch.finish()


def mix(layer, parts, shards, residual, normed, ints_all, gates_all, weights, experts, late_keys, late_mats, next_keys):
    tokens, hidden = residual.shape
    group, depth, ffn = weights[0].shape[1:]
    half = tokens // 2
    anywhere = pl.BlockSpec(memory_space=pl.ANY)
    vmem = pl.BlockSpec(memory_space=pltpu.VMEM)
    copies = 12 + (len(late_keys) + len(next_keys)) * ShardGather.COPIES
    return pl.pallas_call(
        functools.partial(mix_kernel, parts, shards, tuple(late_keys), tuple(next_keys), late_mats),
        in_specs=[vmem] * 4 + [anywhere] * (len(weights) + 3),
        out_specs=[vmem] + [anywhere] * (len(late_keys) + len(next_keys)),
        out_shape=[jax.ShapeDtypeStruct((tokens, hidden), F32)]
        + [jax.ShapeDtypeStruct((shards, group, depth, ffn), BF16)] * (len(late_keys) + len(next_keys)),
        scratch_shapes=[
            pltpu.VMEM((parts, tokens, hidden), BF16),
            pltpu.VMEM((SLOTS, 3, shards, depth, ffn), BF16),
            pltpu.VMEM((8, half, hidden), F32),
            pltpu.VMEM((6, half, hidden), F32),
            pltpu.VMEM((parts, tokens, 2 * group), F32),
            pltpu.SemaphoreType.DMA((copies,)),
            pltpu.SemaphoreType.DMA((copies,)),
            pltpu.SemaphoreType.DMA((SLOTS, 3)),
            pltpu.SemaphoreType.DMA((max(1, len(late_keys) + len(next_keys)),)),
        ],
        compiler_params=pltpu.CompilerParams(collective_id=2 * layer + 1, has_side_effects=True, vmem_limit_bytes=VMEM_LIMIT),
        cost_estimate=pl.CostEstimate(
            flops=12 * parts * tokens * hidden * ffn * group,
            bytes_accessed=96 * group * hidden * ffn,
            transcendentals=2 * parts * tokens * ffn * group,
        ),
        name='mix',
    )(residual, normed, ints_all, gates_all, *weights, *experts)


def solution(mesh):
    token_spec = P(('rep', 'tok', 'mp'))
    row_spec = P(('rep', 'tok', 'mp'), None)
    head_weight = P(None, 'tok', 'mp', None)
    in_specs = (row_spec, token_spec, row_spec, row_spec, head_weight, head_weight, head_weight, P(None, 'mp', None, 'tok'), P(None, None, 'tok', 'mp'), P(None, None, 'tok', 'mp'), P(None, None, 'mp', 'tok'), P(None, None), P(None, None))
    parts = mesh.shape['mp']
    shards = mesh.shape['tok']

    def device_step(hidden_in, seg_ids, expert_ids, expert_gates, w_query, w_key, w_value, w_out, w_gate, w_up, w_down, gain_attn, gain_mlp):
        num_layers, depth, heads, head_dim = w_query.shape
        tokens, _ = hidden_in.shape
        group = w_gate.shape[1] // 2
        width = heads * head_dim
        ffn = w_gate.shape[-1]

        experts_local = [w_gate, w_up, jnp.swapaxes(w_down, 2, 3)]
        halves = [[(layer, matrix, side) for matrix in range(3) for side in range(2)] for layer in range(num_layers)]

        qkv_local = jnp.concatenate([w.reshape(num_layers, depth, width) for w in (w_query, w_key, w_value)], axis=2)
        out_local = jnp.swapaxes(w_out.reshape(num_layers, width, depth), 1, 2)
        ints = jnp.concatenate([seg_ids[None, :], expert_ids.T, jnp.zeros((5, tokens), jnp.int32)], axis=0)
        gates = jnp.concatenate([expert_gates.T, jnp.zeros((6, tokens), F32)], axis=0)
        inv_freq = jnp.power(ROPE_BASE, -jnp.arange(head_dim // 2, dtype=F32) * 2.0 / head_dim)[:, None]

        shape = (group, depth, ffn)
        gathered = {}
        residual = hidden_in
        side_inputs = [inv_freq, ints, gates, qkv_local, out_local]
        plan = {0: [halves[0][0], halves[0][2], halves[0][4], halves[0][1]]}
        for layer in range(num_layers):
            first = layer == 0
            fetch = plan.get(layer, [])
            fetch = [key for key in fetch if key not in gathered]
            outs = attend(first, layer, parts, shards, heads, head_dim, residual, gain_attn[layer:layer + 1], gain_mlp[layer:layer + 1], side_inputs, experts_local, fetch, shape, ints.shape)
            residual, normed = outs[:2]
            outs = outs[2:]
            if first:
                ints_all, gates_all, qkv_all, out_all, cosines, sines, starts = outs[:7]
                outs = outs[7:]
                side_inputs = [cosines, sines, starts, qkv_all, out_all]
            gathered.update(zip(fetch, outs))
            late = [key for key in halves[layer] if key not in gathered]
            late_mats = tuple(halves[layer].index(key) for key in late)
            weights = [gathered[key] for key in halves[layer] if key in gathered]
            following = []
            if layer + 1 < num_layers:
                following = halves[layer + 1][:4]
                plan[layer + 1] = halves[layer + 1][4:]
            outs = mix(layer, parts, shards, residual, normed, ints_all, gates_all, weights, experts_local, late, late_mats, following)
            residual = outs[0]
            gathered.update(zip(late + following, outs[1:]))
        return residual

    return jax.shard_map(device_step, mesh=mesh, in_specs=in_specs, out_specs=row_spec, check_vma=False)
```

```python
import functools

import jax
import jax.numpy as jnp
from jax import lax
from jax.experimental import pallas as pl
from jax.experimental.pallas import tpu as pltpu
from jax.sharding import PartitionSpec as P

EPS = 1e-5
ROPE_BASE = 10000.0
NEG = -1e30
VMEM_LIMIT = 63 * 1024 * 1024
AHEAD = 2
SLOTS = 3
F32 = jnp.float32
BF16 = jnp.bfloat16
NT = (((1,), (1,)), ((), ()))
MESH = pl.DeviceIdType.MESH
FIRST = ('right_low', 'left_high', 'right_high', 'left_low')


def rms_norm(residual, gain):
    inv_rms = lax.rsqrt(jnp.mean(residual * residual, axis=-1, keepdims=True) + EPS)
    return (residual * inv_rms * gain.astype(F32)).astype(BF16)


class Wire:
    def __init__(self, send_sem, recv_sem):
        self.send_sem = send_sem
        self.recv_sem = recv_sem

    def copy(self, slot, src, dst, device):
        return pltpu.make_async_remote_copy(src_ref=src, dst_ref=dst, send_sem=self.send_sem.at[slot], recv_sem=self.recv_sem.at[slot], device_id=device, device_id_type=MESH)


def ring(axis, size):
    me = lax.axis_index(axis)
    return me, lax.rem(me + size - 1, size), lax.rem(me + 1, size), lax.rem(me + size // 2, size)


def meet(devices):
    barrier = pltpu.get_barrier_semaphore()
    for device in devices:
        pl.semaphore_signal(barrier, inc=1, device_id=device, device_id_type=MESH)
    pl.semaphore_wait(barrier, len(devices))


def ring_gather(wire, base, own, rows_all, axis, left, right, me):
    half = own.shape[0] // 2
    low, high = pl.ds(0, half), pl.ds(half, half)
    to_right, to_left = {axis: right}, {axis: left}
    return {
        'right_low': wire.copy(base, own.at[low], rows_all.at[me, low], to_right),
        'right_high': wire.copy(base + 1, own.at[high], rows_all.at[me, high], to_right),
        'left_high': wire.copy(base + 2, own.at[high], rows_all.at[me, high], to_left),
        'left_low': wire.copy(base + 3, own.at[low], rows_all.at[me, low], to_left),
        'on_right': wire.copy(base + 4, rows_all.at[left, low], rows_all.at[left, low], to_right),
        'on_left': wire.copy(base + 5, rows_all.at[right, high], rows_all.at[right, high], to_left),
    }


def tok_devices(shards):
    tok = lax.axis_index('tok')
    return [{'tok': tok + 1 - 2 * lax.rem(tok, 2)}, {'tok': lax.rem(tok + shards - 2, shards)}, {'tok': lax.rem(tok + 2, shards)}]


class ShardGather:
    COPIES = 10

    def __init__(self, wire, base, own, blocks, shards, store_sem=None):
        tok = lax.axis_index('tok')
        left = lax.rem(tok + shards - 2, shards)
        right = lax.rem(tok + 2, shards)
        far = lax.rem(tok + shards // 2, shards)
        partner = {'tok': tok + 1 - 2 * lax.rem(tok, 2)}
        self.rows = ring_gather(wire, base, own, blocks, 'tok', left, right, tok)
        self.cross = [wire.copy(base + 6, own, blocks.at[tok], partner)]
        for index, source in enumerate((left, right, far)):
            self.cross.append(wire.copy(base + 7 + index, blocks.at[source], blocks.at[source], partner))
        self.store = None if store_sem is None else pltpu.make_async_copy(own, blocks.at[tok], store_sem)

    def start(self):
        for name in FIRST:
            self.rows[name].start()
        self.cross[0].start()
        if self.store is not None:
            self.store.start()

    def onward(self):
        self.rows['right_low'].wait_recv()
        self.rows['on_right'].start()
        self.rows['left_high'].wait_recv()
        self.rows['on_left'].start()

    def share_near(self):
        self.rows['right_high'].wait_recv()
        self.cross[1].start()
        self.rows['left_low'].wait_recv()
        self.cross[2].start()

    def share_far(self):
        self.rows['on_right'].wait_recv()
        self.rows['on_left'].wait_recv()
        self.cross[3].start()

    def finish(self):
        for copy in self.cross:
            copy.wait_recv()
        for copy in list(self.rows.values()) + self.cross:
            copy.wait_send()
        if self.store is not None:
            self.store.wait()


class StagedGather(ShardGather):
    def __init__(self, wire, base, source, stage, out, shards, sems):
        tok = lax.axis_index('tok')
        super().__init__(wire, base, stage.at[tok], stage, shards)
        self.load = pltpu.make_async_copy(source, stage.at[tok], sems.at[0])
        self.writes = []
        order = []
        for step in (0, shards - 2, 2, shards // 2):
            order.append(lax.rem(tok + step, shards))
        order += [block + 1 - 2 * lax.rem(block, 2) for block in order]
        for index, block in enumerate(order):
            self.writes.append(pltpu.make_async_copy(stage.at[block], out.at[block], sems.at[1 + index]))

    def start(self):
        self.load.wait()
        super().start()
        self.writes[0].start()

    def share_near(self):
        super().share_near()
        self.writes[1].start()
        self.writes[2].start()

    def share_far(self):
        super().share_far()
        self.writes[3].start()

    def finish(self):
        for copy, write in zip(self.cross, self.writes[4:]):
            copy.wait_recv()
            write.start()
        for copy in list(self.rows.values()) + self.cross:
            copy.wait_send()
        for write in self.writes:
            write.wait()


def request_tables(parts, ints, inv_ref, cos_ref, sin_ref, start_ref):
    tokens = ints.shape[-1]
    half = tokens // 2
    lane = lax.broadcasted_iota(jnp.int32, (8, tokens), 1)
    carry = last = None
    for part in range(parts):
        seg = jnp.broadcast_to(ints[part, 0:1], (8, tokens))
        before = pltpu.roll(seg, 1, 1)
        if part == 0:
            fresh = (lane == 0) | (seg != before)
        else:
            fresh = seg != jnp.where(lane == 0, last, before)
        start = jnp.where(fresh, lane + part * tokens, 0)
        shift = 1
        while shift < tokens:
            start = jnp.maximum(start, jnp.where(lane >= shift, pltpu.roll(start, shift, 1), 0))
            shift *= 2
        if carry is not None:
            start = jnp.maximum(start, carry)
        carry = jnp.broadcast_to(start[:, tokens - 1:], (8, tokens))
        last = jnp.broadcast_to(seg[:, tokens - 1:], (8, tokens))
        angles = inv_ref[...] * (lane + part * tokens - start)[0:1].astype(F32)
        cosines = jnp.cos(angles)
        sines = jnp.sin(angles)
        for piece in range(2):
            span = slice(piece * half, (piece + 1) * half)
            start_ref[2 * part + piece] = start[:, span]
            cos_ref[2 * part + piece] = cosines[:, span]
            sin_ref[2 * part + piece] = sines[:, span]


def exchange_heads(wire, base, o_all, obuf, relay, me, left, right, far):
    width = o_all.shape[1]
    low, high = pl.ds(0, width // 2), pl.ds(width // 2, width // 2)
    to_left, to_right = {'mp': left}, {'mp': right}
    return [
        wire.copy(base, o_all.at[far, low], relay.at[0], to_right),
        wire.copy(base + 1, o_all.at[far, high], relay.at[1], to_left),
        wire.copy(base + 2, o_all.at[right], obuf.at[0], to_right),
        wire.copy(base + 3, o_all.at[left], obuf.at[1], to_left),
        wire.copy(base + 4, relay.at[0], obuf.at[2, low], to_right),
        wire.copy(base + 5, relay.at[1], obuf.at[2, high], to_left),
    ]


def own_blocks(experts, keys):
    group = experts[0].shape[1] // 2
    return [experts[matrix].at[layer, pl.ds(side * group, group)] for layer, matrix, side in keys]


def attend_kernel(first, layer, parts, shards, heads, head_dim, fetch_keys, *refs):
    refs = list(refs)
    num_fetch = len(fetch_keys)
    r_ref, gain_attn, gain_mlp = refs[:3]
    del refs[:3]
    if first:
        inv_ref, seg_ref, ids_ref, gates_ref, wq_ref, wk_ref, wv_ref, wo_in = refs[:8]
        del refs[:8]
    else:
        cos_in, sin_in, start_in, qkv_all, out_all = refs[:5]
        del refs[:5]
    fetch_own = own_blocks(refs[:3], fetch_keys)
    del refs[:3]
    res_ref, h_ref = refs[:2]
    del refs[:2]
    if first:
        ints_out, gates_out, qkv_all, out_all, cos_ref, sin_ref, start_ref = refs[:7]
        del refs[:7]
    fetch_all = refs[:num_fetch]
    del refs[:num_fetch]
    if not first:
        cos_ref, sin_ref, start_ref = refs[:3]
        del refs[:3]
    if first:
        ints_all, gates_all, qkv_pack, out_pack = refs[:4]
        del refs[:4]
    if num_fetch:
        stage, stage_sem = refs[:2]
        del refs[:2]
    hbuf, w_raw, w_sc, q_sc, k_sc, v_sc, m_sc, l_sc, acc_sc, s_sc, o_all, obuf, relay, wo_ref = refs[:14]
    send_sem, recv_sem, local_sem = refs[14:]

    me, left, right, far = ring('mp', parts)
    tok = lax.axis_index('tok')
    to_left, to_right = {'mp': left}, {'mp': right}
    wire = Wire(send_sem, recv_sem)
    tokens, hidden = res_ref.shape
    rows = tokens // 2
    width = heads * head_dim
    span = q_sc.shape[-1]
    pieces = rows // span
    tiles = 2 * parts
    units = [(head, piece) for head in range(heads) for piece in range(pieces)]

    fetches = [StagedGather(wire, 41 + index * ShardGather.COPIES, own, stage.at[index], blocks, shards, stage_sem.at[index]) for index, (own, blocks) in enumerate(zip(fetch_own, fetch_all))]
    for fetch in fetches:
        fetch.load.start()
    if first:
        for index, ref in enumerate((wq_ref, wk_ref, wv_ref)):
            qkv_pack[:, index * width:(index + 1) * width] = ref[...]
        for index in range(out_pack.shape[0]):
            out_pack[index] = wo_in[index].astype(F32).T.astype(BF16)
        ints_all[me, 0:1] = seg_ref[...]
        ints_all[me, 1:3] = ids_ref[...]
        gates_all[me, 0:2] = gates_ref[...]
        qkv = ShardGather(wire, 21, qkv_pack, qkv_all, shards, local_sem.at[3])
        out = ShardGather(wire, 31, out_all.at[tok], out_all, shards)
    meet([to_left, to_right] + tok_devices(shards))
    if first:
        qkv.start()
        small = [
            wire.copy(0, ints_all.at[me], ints_all.at[me], to_right),
            wire.copy(1, ints_all.at[me], ints_all.at[me], to_left),
            wire.copy(2, gates_all.at[me], gates_all.at[me], to_right),
            wire.copy(3, gates_all.at[me], gates_all.at[me], to_left),
            wire.copy(4, out_pack, out_all.at[tok, me], to_right),
            wire.copy(5, out_pack, out_all.at[tok, me], to_left),
        ]
        onward = [
            wire.copy(6, ints_all.at[left], ints_all.at[left], to_right),
            wire.copy(7, gates_all.at[right], gates_all.at[right], to_left),
            wire.copy(8, out_all.at[tok, left], out_all.at[tok, left], to_right),
        ]
        local = [pltpu.make_async_copy(out_pack, out_all.at[tok, me], local_sem.at[0])]
        for copy in small + local:
            copy.start()
    else:
        local = [
            pltpu.make_async_copy(qkv_all.at[:, layer], w_raw, local_sem.at[3]),
            pltpu.make_async_copy(cos_in, cos_ref, local_sem.at[0]),
            pltpu.make_async_copy(sin_in, sin_ref, local_sem.at[1]),
            pltpu.make_async_copy(start_in, start_ref, local_sem.at[2]),
        ]
        for copy in local:
            copy.start()
    hbuf[me] = rms_norm(r_ref[...].astype(F32), gain_attn[layer:layer + 1])
    rows_in = ring_gather(wire, 9, hbuf.at[me], hbuf, 'mp', left, right, me)
    for name in FIRST:
        rows_in[name].start()
    if first:
        for copy in small:
            copy.wait_recv()
        for copy in onward:
            copy.start()
        qkv.onward()
        onward[0].wait_recv()
        request_tables(parts, ints_all, inv_ref, cos_ref, sin_ref, start_ref)
        ints_out[...] = ints_all[...]
        onward[1].wait_recv()
        gates_out[...] = gates_all[...]
        onward[2].wait_recv()
        local[0].wait()
        out.start()
        fetches[0].start()
        qkv.share_near()
        qkv.share_far()
        qkv.finish()
        load = pltpu.make_async_copy(qkv_all.at[:, layer], w_raw, local_sem.at[4])
        load.start()
        load.wait()
    else:
        if fetches:
            fetches[0].start()
        for copy in local:
            copy.wait()
    depth = w_raw.shape[-1]
    for shard in range(shards):
        w_sc[:, shard * depth:(shard + 1) * depth] = w_raw[shard]

    half_dim = head_dim // 2
    scale = head_dim ** -0.5

    def tile_of(index):
        pair = index // 2
        odd = lax.rem(index, 2)
        between = (pair * (3 - pair)) // 2
        last_pair = (pair * (pair - 1) * (pair - 2)) // 6
        third = (pair * (pair - 1) * (3 - pair)) // 2
        chunk = lax.rem(me + between * (3 - 2 * odd) + 2 * last_pair, parts)
        side = odd + third * (1 - 2 * odd)
        return chunk, side

    def score(unit, query_tile, key_tile, keys):
        head, _ = units[unit]
        return jnp.dot(k_sc[key_tile, head, :keys], q_sc[query_tile, unit], preferred_element_type=F32)

    def absorb(unit, scores, query_tile, key_tile, causal):
        head, piece = units[unit]
        keys = scores.shape[0]
        key_row = lax.broadcasted_iota(jnp.int32, (keys, span), 0)
        allowed = key_row >= start_ref[query_tile, 0:1, piece * span:(piece + 1) * span] - key_tile * rows
        if causal:
            allowed = allowed & (key_row <= lax.broadcasted_iota(jnp.int32, (keys, span), 1) + piece * span)
        scores = jnp.where(allowed, scores, NEG)
        old_max = m_sc[query_tile, unit:unit + 1]
        new_max = jnp.maximum(old_max, jnp.max(scores, axis=0, keepdims=True))
        prob = jnp.exp(scores - new_max)
        fade = jnp.exp(old_max - new_max)
        m_sc[query_tile, unit:unit + 1] = new_max
        l_sc[query_tile, unit:unit + 1] = fade * l_sc[query_tile, unit:unit + 1] + jnp.sum(prob, axis=0, keepdims=True)
        value = v_sc[key_tile, head * head_dim:(head + 1) * head_dim, :keys]
        part = jnp.dot(value, prob.astype(BF16), preferred_element_type=F32)
        acc_sc[query_tile, unit] = acc_sc[query_tile, unit] * fade + part

    def block(query_tile, key_tile, following):
        diagonal = following is None

        def keys_of(unit):
            return (units[unit][1] + 1) * span if diagonal else rows

        waiting = [s_sc[unit, :keys_of(unit)] for unit in range(AHEAD)]
        for unit in range(len(units)):
            ahead = unit + AHEAD
            if ahead < len(units):
                waiting.append(score(ahead, query_tile, key_tile, keys_of(ahead)))
            elif not diagonal:
                s_sc[ahead - len(units)] = score(ahead - len(units), following[0], following[1], rows)
            absorb(unit, waiting.pop(0), query_tile, key_tile, diagonal)

    def arrive(index, carry):
        chunk, side = tile_of(index)
        tile = 2 * chunk + side

        @pl.when(index == 1)
        def _():
            if first:
                out.onward()
            for fetch in fetches[1:2]:
                fetch.start()

        @pl.when(index == 2)
        def _():
            rows_in['right_low'].wait_recv()
            rows_in['on_right'].start()

        @pl.when(index == 3)
        def _():
            rows_in['left_high'].wait_recv()
            rows_in['on_left'].start()

        @pl.when(index == 4)
        def _():
            rows_in['right_high'].wait_recv()
            for fetch in fetches[:1]:
                fetch.onward()
                fetch.share_near()
            for fetch in fetches[2:3]:
                fetch.start()
            if first:
                out.share_near()
                out.share_far()

        @pl.when(index == 5)
        def _():
            rows_in['left_low'].wait_recv()
            for fetch in fetches[3:4]:
                fetch.start()

        @pl.when(index == 6)
        def _():
            rows_in['on_right'].wait_recv()
            for fetch in fetches[1:2]:
                fetch.onward()
                fetch.share_near()
            for fetch in fetches[:1]:
                fetch.share_far()

        @pl.when(index == 7)
        def _():
            rows_in['on_left'].wait_recv()
            for fetch in fetches[2:3]:
                fetch.onward()

        x = hbuf[chunk, pl.ds(pl.multiple_of(side * rows, rows), rows)]
        qkv_rows = lax.dot_general(w_sc[...], x, NT, preferred_element_type=F32)
        cosines = cos_ref[tile]
        sines = sin_ref[tile]

        def rotate(base):
            one = qkv_rows[base:base + half_dim]
            two = qkv_rows[base + half_dim:base + head_dim]
            return jnp.concatenate([one * cosines - two * sines, two * cosines + one * sines], axis=0)

        for head in range(heads):
            base = head * head_dim
            query = (rotate(base).astype(BF16).astype(F32) * scale).astype(BF16)
            for piece in range(pieces):
                q_sc[tile, head * pieces + piece] = query[:, piece * span:(piece + 1) * span]
            k_sc[tile, head] = rotate(width + base).T.astype(BF16)
        v_sc[tile] = qkv_rows[2 * width:3 * width].astype(BF16)
        m_sc[tile] = jnp.full(m_sc.shape[1:], NEG, F32)
        l_sc[tile] = jnp.zeros(l_sc.shape[1:], F32)
        acc_sc[tile] = jnp.zeros(acc_sc.shape[1:], F32)

        def ordered(other):
            other_chunk, other_side = tile_of(other)
            other_tile = 2 * other_chunk + other_side
            ahead = (tile - other_tile + tiles) // tiles
            upper = other_tile + ahead * (tile - other_tile)
            return upper, tile + other_tile - upper

        upper, lower = ordered(jnp.int32(0))
        for unit in range(AHEAD):
            s_sc[unit] = score(unit, upper, lower, rows)

        def pair(other, inner):
            query_tile, key_tile = ordered(other)
            block(query_tile, key_tile, ordered(other + 1))
            return inner

        lax.fori_loop(0, index, pair, 0)
        block(tile, tile, None)
        return carry

    lax.fori_loop(0, tiles, arrive, 0)
    wo_copy = pltpu.make_async_copy(out_all.at[:, :, layer], wo_ref, local_sem.at[5])
    if first:
        out.finish()
    wo_copy.start()
    for tile in range(tiles):
        for unit, (head, piece) in enumerate(units):
            top = head * head_dim
            edge = (tile % 2) * rows + piece * span
            o_all[tile // 2, top:top + head_dim, edge:edge + span] = (acc_sc[tile, unit] / l_sc[tile, unit:unit + 1]).astype(BF16)

    exchange = exchange_heads(wire, 15, o_all, obuf, relay, me, left, right, far)
    for copy in exchange[:4]:
        copy.start()
    for fetch in fetches[3:4]:
        fetch.onward()
    exchange[0].wait_recv()
    exchange[4].start()
    exchange[1].wait_recv()
    exchange[5].start()
    for fetch in fetches[2:4]:
        fetch.share_near()
    wo_copy.wait()
    chunk = min(256, tokens)

    def project(sources, last):
        def step(index, carry):
            lanes = pl.ds(pl.multiple_of(index * chunk, chunk), chunk)
            total = None
            for source, piece in sources:
                weight = wo_ref[:, source].reshape(hidden, width)
                term = jnp.dot(weight, piece[:, lanes], preferred_element_type=F32)
                total = term if total is None else total + term
            residual = (res_ref[lanes] if last else r_ref[lanes].astype(F32)) + total.T
            res_ref[lanes] = residual
            if last:
                h_ref[lanes] = rms_norm(residual, gain_mlp[layer:layer + 1])
            return carry

        lax.fori_loop(0, tokens // chunk, step, 0)

    project([(me, o_all.at[me])], False)
    exchange[2].wait_recv()
    exchange[3].wait_recv()
    exchange[4].wait_recv()
    exchange[5].wait_recv()
    for fetch in fetches[1:3]:
        fetch.share_far()
    project([(left, obuf.at[0]), (right, obuf.at[1]), (far, obuf.at[2])], True)

    for fetch in fetches[3:4]:
        fetch.share_far()
    for fetch in fetches:
        fetch.finish()
    for copy in exchange + list(rows_in.values()):
        copy.wait_send()
    if first:
        for copy in small + onward:
            copy.wait_send()


def attend(first, layer, parts, shards, heads, head_dim, residual, gain_attn, gain_mlp, side_inputs, experts, fetch_keys, gathered_shape, ints_shape):
    tokens, hidden = residual.shape
    rows = tokens // 2
    width = heads * head_dim
    tiles = 2 * parts
    span = min(256, rows)
    units = heads * rows // span
    depth = hidden // shards
    num_layers = gain_attn.shape[0]
    anywhere = pl.BlockSpec(memory_space=pl.ANY)
    vmem = pl.BlockSpec(memory_space=pltpu.VMEM)
    num_fetch = len(fetch_keys)
    in_specs = [vmem] * 3 + ([vmem] * 8 if first else [anywhere] * 5) + [anywhere] * 3
    out_shape = [jax.ShapeDtypeStruct((tokens, hidden), F32), jax.ShapeDtypeStruct((tokens, hidden), BF16)]
    out_specs = [vmem, vmem]
    tables = [((tiles, head_dim // 2, rows), F32), ((tiles, head_dim // 2, rows), F32), ((tiles, 8, rows), jnp.int32)]
    if first:
        out_shape += [
            jax.ShapeDtypeStruct((parts,) + ints_shape, jnp.int32),
            jax.ShapeDtypeStruct((parts,) + ints_shape, F32),
            jax.ShapeDtypeStruct((shards, num_layers, 3 * width, depth), BF16),
            jax.ShapeDtypeStruct((shards, parts, num_layers, depth, width), BF16),
        ] + [jax.ShapeDtypeStruct(shape, dtype) for shape, dtype in tables]
        out_specs += [vmem, vmem, anywhere, anywhere] + [vmem] * 3
    out_shape += [jax.ShapeDtypeStruct((shards,) + gathered_shape, BF16)] * num_fetch
    out_specs += [anywhere] * num_fetch
    scratch = [
        pltpu.VMEM((parts,) + ints_shape, jnp.int32),
        pltpu.VMEM((parts,) + ints_shape, F32),
        pltpu.VMEM((num_layers, 3 * width, depth), BF16),
        pltpu.VMEM((num_layers, depth, width), BF16),
    ] if first else [pltpu.VMEM(shape, dtype) for shape, dtype in tables]
    copies = 41 + num_fetch * ShardGather.COPIES
    if num_fetch:
        scratch += [pltpu.VMEM((num_fetch, shards) + gathered_shape, BF16), pltpu.SemaphoreType.DMA((num_fetch, 1 + shards))]
    scratch += [
        pltpu.VMEM((parts, tokens, hidden), BF16),
        pltpu.VMEM((shards, 3 * width, depth), BF16),
        pltpu.VMEM((3 * width, hidden), BF16),
        pltpu.VMEM((tiles, units, head_dim, span), BF16),
        pltpu.VMEM((tiles, heads, rows, head_dim), BF16),
        pltpu.VMEM((tiles, width, rows), BF16),
        pltpu.VMEM((tiles, max(8, units), span), F32),
        pltpu.VMEM((tiles, max(8, units), span), F32),
        pltpu.VMEM((tiles, units, head_dim, span), F32),
        pltpu.VMEM((AHEAD, rows, span), F32),
        pltpu.VMEM((parts, width, tokens), BF16),
        pltpu.VMEM((3, width, tokens), BF16),
        pltpu.VMEM((2, width // 2, tokens), BF16),
        pltpu.VMEM((shards, parts, depth, width), BF16),
        pltpu.SemaphoreType.DMA((copies,)),
        pltpu.SemaphoreType.DMA((copies,)),
        pltpu.SemaphoreType.DMA((6,)),
    ]
    seq_len = parts * tokens
    return pl.pallas_call(
        functools.partial(attend_kernel, first, layer, parts, shards, heads, head_dim, tuple(fetch_keys)),
        in_specs=in_specs,
        out_specs=out_specs,
        out_shape=out_shape,
        scratch_shapes=scratch,
        compiler_params=pltpu.CompilerParams(collective_id=2 * layer, has_side_effects=True, vmem_limit_bytes=VMEM_LIMIT),
        cost_estimate=pl.CostEstimate(flops=2 * seq_len * seq_len * width + 8 * seq_len * hidden * width, bytes_accessed=8 * seq_len * hidden, transcendentals=seq_len * seq_len * heads // 2),
        name='attend',
    )(residual, gain_attn, gain_mlp, *side_inputs, *experts)


def mix_kernel(parts, shards, late_keys, next_keys, late_mats, *refs):
    refs = list(refs)
    num_late = len(late_keys)
    num_next = len(next_keys)
    r_ref, h_ref, ints_ref, gates_ref = refs[:4]
    del refs[:4]
    given = refs[:6 - num_late]
    del refs[:6 - num_late]
    late_own = own_blocks(refs[:3], late_keys)
    next_own = own_blocks(refs[:3], next_keys)
    del refs[:3]
    res_ref = refs.pop(0)
    late_all = refs[:num_late]
    del refs[:num_late]
    next_all = refs[:num_next]
    del refs[:num_next]
    hbuf, wbuf, acc, inbox, route, send_sem, recv_sem, w_sem, local_sem = refs
    mats = list(given)
    for position, ref in zip(late_mats, late_all):
        mats.insert(position, ref)

    me, left, right, _ = ring('mp', parts)
    to_left, to_right = {'mp': left}, {'mp': right}
    wire = Wire(send_sem, recv_sem)
    _, group, depth, ffn = mats[0].shape
    num_experts = 2 * group
    tokens, hidden = res_ref.shape
    half = tokens // 2
    low, high = pl.ds(0, half), pl.ds(half, half)
    steps = 16 * group
    waits_late = bool(late_keys)
    gate_step = (6 if waits_late else 4) * group - (SLOTS - 1)

    def place(step):
        turn = lax.div(step, group)
        odd = lax.rem(turn, 2)
        since = {edge: lax.div(turn + 16 - edge, 16) for edge in (4, 6, 8, 12, 14)}
        main = lax.div(turn, 2)
        if waits_late:
            buffer = turn + 2 * since[4] - 6 * since[6] + since[8] * (main - turn + 4) + since[12] * (turn - 6 - main) - 8 * since[14]
            late = since[6] * (1 - since[8]) + since[8] * (1 - since[12]) * odd + since[12]
        else:
            buffer = turn - 2 * since[4] + since[6] * (main + 3 - turn) + since[14] * (turn - 15 - main)
            late = since[4] * (1 - since[6]) + since[6] * (1 - since[14]) * odd + since[14]
        return turn, buffer, late, lax.rem(step, group)

    def weight_copies(step, side):
        _, _, _, expert = place(step)
        slot = lax.rem(step, SLOTS)
        return [pltpu.make_async_copy(mats[2 * index + side].at[:, expert], wbuf.at[slot, index], w_sem.at[slot, index]) for index in range(3)]

    def start_weights(step):
        _, _, late, _ = place(step)
        for side in range(2):

            @pl.when(late == side)
            def _(side=side):
                for copy in weight_copies(step, side):
                    copy.start()

    late_fetch = [ShardGather(wire, 12 + index * ShardGather.COPIES, own, blocks, shards, local_sem.at[index]) for index, (own, blocks) in enumerate(zip(late_own, late_all))]
    base = 12 + num_late * ShardGather.COPIES
    next_fetch = [ShardGather(wire, base + index * ShardGather.COPIES, own, blocks, shards, local_sem.at[num_late + index]) for index, (own, blocks) in enumerate(zip(next_own, next_all))]
    for step in range(SLOTS - 1):
        start_weights(jnp.int32(step))
    meet([to_left, to_right] + (tok_devices(shards) if late_fetch or next_fetch else []))
    rows_in = ring_gather(wire, 0, h_ref, hbuf, 'mp', left, right, me)
    for name in FIRST:
        rows_in[name].start()
    for fetch in late_fetch:
        fetch.start()
    hbuf[me] = h_ref[...]
    expert_row = lax.broadcasted_iota(jnp.int32, (num_experts, 1), 0)
    for part in range(parts):
        share = jnp.zeros((num_experts, tokens), F32)
        for choice in range(2):
            share = share + jnp.where(ints_ref[part, 1 + choice:2 + choice] == expert_row, gates_ref[part, choice:choice + 1], 0.0)
        route[part] = share.T

    sends = {
        2: wire.copy(6, acc.at[2], inbox.at[0], to_left),
        3: wire.copy(7, acc.at[3], inbox.at[1], to_right),
        4: wire.copy(8, acc.at[4], inbox.at[2], to_right),
        5: wire.copy(9, acc.at[5], inbox.at[3], to_left),
        6: wire.copy(10, acc.at[6], inbox.at[4], to_right),
        7: wire.copy(11, acc.at[7], inbox.at[5], to_left),
    }
    tile_rows = min(256, half)
    tiles = half // tile_rows
    lane = lax.broadcasted_iota(jnp.int32, (tile_rows, num_experts), 1)

    def rows_low_right():
        rows_in['right_low'].wait_recv()
        rows_in['on_right'].start()
        for fetch in late_fetch[:1]:
            fetch.onward()

    def rows_high_left():
        rows_in['left_high'].wait_recv()
        rows_in['on_left'].start()
        for fetch in late_fetch[1:]:
            fetch.onward()
        for fetch in late_fetch[:1]:
            fetch.share_near()

    def rows_low_left():
        rows_in['left_low'].wait_recv()
        for fetch in late_fetch[1:]:
            fetch.share_near()

    def next_near():
        for fetch in next_fetch:
            fetch.onward()
            fetch.share_near()

    def sums():
        sends[4].wait_recv()
        acc[6] += inbox[2]
        sends[6].start()
        sends[5].wait_recv()
        acc[7] += inbox[3]
        sends[7].start()
        for fetch in next_fetch:
            fetch.share_far()

    if waits_late:
        fresh = (0, 1, 2, 3, 4, 5, 8, 10)
        events = {
            2: [rows_low_right],
            3: [rows_high_left],
            4: [rows_low_left],
            5: [rows_in['right_high'].wait_recv],
            7: [sends[2].start],
            8: [sends[3].start, rows_in['on_right'].wait_recv],
            10: [sends[4].start, rows_in['on_left'].wait_recv],
            12: [sends[5].start, next_near],
            14: [sums],
        }
    else:
        fresh = (0, 1, 2, 3, 6, 8, 10, 12)
        events = {
            2: [rows_low_right],
            3: [rows_high_left],
            5: [sends[2].start],
            6: [sends[3].start, rows_in['on_right'].wait_recv],
            8: [sends[4].start, rows_in['on_left'].wait_recv],
            10: [sends[5].start, rows_low_left, next_near],
            12: [rows_in['right_high'].wait_recv],
            14: [sums],
        }

    def begin(turn, buffer):
        clear = turn == fresh[0]
        for other in fresh[1:]:
            clear = clear | (turn == other)

        @pl.when(clear)
        def _():
            acc[buffer] = jnp.zeros((half, hidden), F32)

        for when, actions in events.items():

            @pl.when(turn == when)
            def _(actions=actions):
                for action in actions:
                    action()

    def expert_step(step, carry):
        turn, buffer, late, index = place(step)
        slot = lax.rem(step, SLOTS)
        expert = late * group + index
        pair = lax.div(buffer, 2)
        side = lax.rem(buffer, 2)
        odd = lax.rem(pair, 2)
        upper = lax.div(pair, 2)
        shift = odd * (upper * (1 + 2 * side) + (1 - upper) * (3 - 2 * side)) + (1 - odd) * 2 * upper
        source = lax.rem(me + shift, parts)
        start = pl.multiple_of(side * half, half)

        if late_fetch or next_fetch:

            @pl.when(step == gate_step)
            def _():
                for fetch in late_fetch:
                    fetch.share_far()
                for fetch in late_fetch:
                    fetch.finish()
                for fetch in next_fetch:
                    fetch.start()

        @pl.when(step + SLOTS - 1 < steps)
        def _():
            start_weights(step + SLOTS - 1)

        @pl.when(index == 0)
        def _():
            begin(turn, buffer)

        for copy in weight_copies(step, 0):
            copy.wait()

        def activate(tile):
            gate_w = wbuf[slot, 0].reshape(hidden, ffn)
            up_w = wbuf[slot, 1].reshape(hidden, ffn)
            x = hbuf[source, pl.ds(start + tile * tile_rows, tile_rows)]
            gate_pre = jnp.dot(x, gate_w, preferred_element_type=F32)
            up_pre = jnp.dot(x, up_w, preferred_element_type=F32)
            return (gate_pre * (1.0 / (1.0 + jnp.exp(-gate_pre))) * up_pre).astype(BF16)

        def contract(tile, act):
            down_w = wbuf[slot, 2].reshape(hidden, ffn)
            part_share = route[source, pl.ds(start + tile * tile_rows, tile_rows)]
            share = jnp.sum(jnp.where(lane == expert, part_share, 0.0), axis=1, keepdims=True)
            mixed = lax.dot_general(act, down_w, NT, preferred_element_type=F32)
            acc[buffer, tile * tile_rows:(tile + 1) * tile_rows] += share * mixed

        act = activate(0)
        for tile in range(tiles):
            following = activate(tile + 1) if tile + 1 < tiles else None
            contract(tile, act)
            act = following
        return carry

    lax.fori_loop(0, steps, expert_step, 0)

    sends[2].wait_recv()
    res_ref[low] = r_ref[low] + acc[0] + inbox[0]
    sends[3].wait_recv()
    res_ref[high] = r_ref[high] + acc[1] + inbox[1]
    sends[6].wait_recv()
    res_ref[low] += inbox[4]
    sends[7].wait_recv()
    res_ref[high] += inbox[5]
    for copy in list(rows_in.values()) + list(sends.values()):
        copy.wait_send()
    for fetch in next_fetch:
        fetch.finish()


def mix(layer, parts, shards, residual, normed, ints_all, gates_all, weights, experts, late_keys, late_mats, next_keys):
    tokens, hidden = residual.shape
    group, depth, ffn = weights[0].shape[1:]
    half = tokens // 2
    anywhere = pl.BlockSpec(memory_space=pl.ANY)
    vmem = pl.BlockSpec(memory_space=pltpu.VMEM)
    copies = 12 + (len(late_keys) + len(next_keys)) * ShardGather.COPIES
    return pl.pallas_call(
        functools.partial(mix_kernel, parts, shards, tuple(late_keys), tuple(next_keys), late_mats),
        in_specs=[vmem] * 4 + [anywhere] * (len(weights) + 3),
        out_specs=[vmem] + [anywhere] * (len(late_keys) + len(next_keys)),
        out_shape=[jax.ShapeDtypeStruct((tokens, hidden), F32)]
        + [jax.ShapeDtypeStruct((shards, group, depth, ffn), BF16)] * (len(late_keys) + len(next_keys)),
        scratch_shapes=[
            pltpu.VMEM((parts, tokens, hidden), BF16),
            pltpu.VMEM((SLOTS, 3, shards, depth, ffn), BF16),
            pltpu.VMEM((8, half, hidden), F32),
            pltpu.VMEM((6, half, hidden), F32),
            pltpu.VMEM((parts, tokens, 2 * group), F32),
            pltpu.SemaphoreType.DMA((copies,)),
            pltpu.SemaphoreType.DMA((copies,)),
            pltpu.SemaphoreType.DMA((SLOTS, 3)),
            pltpu.SemaphoreType.DMA((max(1, len(late_keys) + len(next_keys)),)),
        ],
        compiler_params=pltpu.CompilerParams(collective_id=2 * layer + 1, has_side_effects=True, vmem_limit_bytes=VMEM_LIMIT),
        cost_estimate=pl.CostEstimate(
            flops=12 * parts * tokens * hidden * ffn * group,
            bytes_accessed=96 * group * hidden * ffn,
            transcendentals=2 * parts * tokens * ffn * group,
        ),
        name='mix',
    )(residual, normed, ints_all, gates_all, *weights, *experts)


def solution(mesh):
    token_spec = P(('rep', 'tok', 'mp'))
    row_spec = P(('rep', 'tok', 'mp'), None)
    head_weight = P(None, 'tok', 'mp', None)
    in_specs = (row_spec, token_spec, row_spec, row_spec, head_weight, head_weight, head_weight, P(None, 'mp', None, 'tok'), P(None, None, 'tok', 'mp'), P(None, None, 'tok', 'mp'), P(None, None, 'mp', 'tok'), P(None, None), P(None, None))
    parts = mesh.shape['mp']
    shards = mesh.shape['tok']

    def device_step(hidden_in, seg_ids, expert_ids, expert_gates, w_query, w_key, w_value, w_out, w_gate, w_up, w_down, gain_attn, gain_mlp):
        num_layers, depth, heads, head_dim = w_query.shape
        tokens, _ = hidden_in.shape
        group = w_gate.shape[1] // 2
        width = heads * head_dim
        ffn = w_gate.shape[-1]

        experts_local = [w_gate, w_up, jnp.swapaxes(w_down, 2, 3)]
        halves = [[(layer, matrix, side) for matrix in range(3) for side in range(2)] for layer in range(num_layers)]

        qkv_local = [jnp.transpose(w, (0, 2, 3, 1)).reshape(num_layers, width, depth) for w in (w_query, w_key, w_value)]
        out_local = w_out.reshape(num_layers, width, depth)
        inv_freq = jnp.power(ROPE_BASE, -jnp.arange(head_dim // 2, dtype=F32) * 2.0 / head_dim)[:, None]

        shape = (group, depth, ffn)
        gathered = {}
        residual = hidden_in
        side_inputs = [inv_freq, seg_ids[None, :], expert_ids.T, expert_gates.T] + qkv_local + [out_local]
        plan = {0: [halves[0][0], halves[0][2], halves[0][4], halves[0][1]]}
        for layer in range(num_layers):
            first = layer == 0
            fetch = plan.get(layer, [])
            fetch = [key for key in fetch if key not in gathered]
            outs = attend(first, layer, parts, shards, heads, head_dim, residual, gain_attn, gain_mlp, side_inputs, experts_local, fetch, shape, (8, tokens))
            residual, normed = outs[:2]
            outs = outs[2:]
            if first:
                ints_all, gates_all, qkv_all, out_all, cosines, sines, starts = outs[:7]
                outs = outs[7:]
                side_inputs = [cosines, sines, starts, qkv_all, out_all]
            gathered.update(zip(fetch, outs))
            late = [key for key in halves[layer] if key not in gathered]
            late_mats = tuple(halves[layer].index(key) for key in late)
            weights = [gathered[key] for key in halves[layer] if key in gathered]
            following = []
            if layer + 1 < num_layers:
                following = halves[layer + 1][:4]
                plan[layer + 1] = halves[layer + 1][4:]
            outs = mix(layer, parts, shards, residual, normed, ints_all, gates_all, weights, experts_local, late, late_mats, following)
            residual = outs[0]
            gathered.update(zip(late + following, outs[1:]))
        return residual

    return jax.shard_map(device_step, mesh=mesh, in_specs=in_specs, out_specs=row_spec, check_vma=False)
```

```python
import functools

import jax
import jax.numpy as jnp
from jax import lax
from jax.experimental import pallas as pl
from jax.experimental.pallas import tpu as pltpu
from jax.sharding import PartitionSpec as P

EPS = 1e-5
ROPE_BASE = 10000.0
NEG = -1e30
VMEM_LIMIT = 63 * 1024 * 1024
AHEAD = 2
SLOTS = 3
F32 = jnp.float32
BF16 = jnp.bfloat16
NT = (((1,), (1,)), ((), ()))
MESH = pl.DeviceIdType.MESH
FIRST = ('right_low', 'left_high', 'right_high', 'left_low')


def rms_norm(residual, gain):
    inv_rms = lax.rsqrt(jnp.mean(residual * residual, axis=-1, keepdims=True) + EPS)
    return (residual * inv_rms * gain.astype(F32)).astype(BF16)


class Wire:
    def __init__(self, send_sem, recv_sem):
        self.send_sem = send_sem
        self.recv_sem = recv_sem

    def copy(self, slot, src, dst, device):
        return pltpu.make_async_remote_copy(src_ref=src, dst_ref=dst, send_sem=self.send_sem.at[slot], recv_sem=self.recv_sem.at[slot], device_id=device, device_id_type=MESH)


def ring(axis, size):
    me = lax.axis_index(axis)
    return me, lax.rem(me + size - 1, size), lax.rem(me + 1, size), lax.rem(me + size // 2, size)


def meet(devices):
    barrier = pltpu.get_barrier_semaphore()
    for device in devices:
        pl.semaphore_signal(barrier, inc=1, device_id=device, device_id_type=MESH)
    pl.semaphore_wait(barrier, len(devices))


def ring_gather(wire, base, own, rows_all, axis, left, right, me):
    half = own.shape[0] // 2
    low, high = pl.ds(0, half), pl.ds(half, half)
    to_right, to_left = {axis: right}, {axis: left}
    return {
        'right_low': wire.copy(base, own.at[low], rows_all.at[me, low], to_right),
        'right_high': wire.copy(base + 1, own.at[high], rows_all.at[me, high], to_right),
        'left_high': wire.copy(base + 2, own.at[high], rows_all.at[me, high], to_left),
        'left_low': wire.copy(base + 3, own.at[low], rows_all.at[me, low], to_left),
        'on_right': wire.copy(base + 4, rows_all.at[left, low], rows_all.at[left, low], to_right),
        'on_left': wire.copy(base + 5, rows_all.at[right, high], rows_all.at[right, high], to_left),
    }


def tok_devices(shards):
    tok = lax.axis_index('tok')
    return [{'tok': tok + 1 - 2 * lax.rem(tok, 2)}, {'tok': lax.rem(tok + shards - 2, shards)}, {'tok': lax.rem(tok + 2, shards)}]


class ShardGather:
    COPIES = 10

    def __init__(self, wire, base, own, blocks, shards, store_sem=None):
        tok = lax.axis_index('tok')
        left = lax.rem(tok + shards - 2, shards)
        right = lax.rem(tok + 2, shards)
        far = lax.rem(tok + shards // 2, shards)
        partner = {'tok': tok + 1 - 2 * lax.rem(tok, 2)}
        self.rows = ring_gather(wire, base, own, blocks, 'tok', left, right, tok)
        self.cross = [wire.copy(base + 6, own, blocks.at[tok], partner)]
        for index, source in enumerate((left, right, far)):
            self.cross.append(wire.copy(base + 7 + index, blocks.at[source], blocks.at[source], partner))
        self.store = None if store_sem is None else pltpu.make_async_copy(own, blocks.at[tok], store_sem)

    def start(self):
        for name in FIRST:
            self.rows[name].start()
        self.cross[0].start()
        if self.store is not None:
            self.store.start()

    def onward(self):
        self.rows['right_low'].wait_recv()
        self.rows['on_right'].start()
        self.rows['left_high'].wait_recv()
        self.rows['on_left'].start()

    def share_near(self):
        self.rows['right_high'].wait_recv()
        self.cross[1].start()
        self.rows['left_low'].wait_recv()
        self.cross[2].start()

    def share_far(self):
        self.rows['on_right'].wait_recv()
        self.rows['on_left'].wait_recv()
        self.cross[3].start()

    def finish(self):
        for copy in self.cross:
            copy.wait_recv()
        for copy in list(self.rows.values()) + self.cross:
            copy.wait_send()
        if self.store is not None:
            self.store.wait()


class StagedGather(ShardGather):
    def __init__(self, wire, base, source, stage, out, shards, sems):
        tok = lax.axis_index('tok')
        super().__init__(wire, base, stage.at[tok], stage, shards)
        self.load = pltpu.make_async_copy(source, stage.at[tok], sems.at[0])
        self.writes = []
        order = []
        for step in (0, shards - 2, 2, shards // 2):
            order.append(lax.rem(tok + step, shards))
        order += [block + 1 - 2 * lax.rem(block, 2) for block in order]
        for index, block in enumerate(order):
            self.writes.append(pltpu.make_async_copy(stage.at[block], out.at[block], sems.at[1 + index]))

    def start(self):
        self.load.wait()
        super().start()
        self.writes[0].start()

    def share_near(self):
        super().share_near()
        self.writes[1].start()
        self.writes[2].start()

    def share_far(self):
        super().share_far()
        self.writes[3].start()

    def finish(self):
        for copy, write in zip(self.cross, self.writes[4:]):
            copy.wait_recv()
            write.start()
        for copy in list(self.rows.values()) + self.cross:
            copy.wait_send()
        for write in self.writes:
            write.wait()


def request_tables(parts, ints, inv_ref, cos_ref, sin_ref, start_ref):
    tokens = ints.shape[-1]
    half = tokens // 2
    lane = lax.broadcasted_iota(jnp.int32, (8, tokens), 1)
    carry = last = None
    for part in range(parts):
        seg = jnp.broadcast_to(ints[part, 0:1], (8, tokens))
        before = pltpu.roll(seg, 1, 1)
        if part == 0:
            fresh = (lane == 0) | (seg != before)
        else:
            fresh = seg != jnp.where(lane == 0, last, before)
        start = jnp.where(fresh, lane + part * tokens, 0)
        shift = 1
        while shift < tokens:
            start = jnp.maximum(start, jnp.where(lane >= shift, pltpu.roll(start, shift, 1), 0))
            shift *= 2
        if carry is not None:
            start = jnp.maximum(start, carry)
        carry = jnp.broadcast_to(start[:, tokens - 1:], (8, tokens))
        last = jnp.broadcast_to(seg[:, tokens - 1:], (8, tokens))
        angles = inv_ref[...] * (lane + part * tokens - start)[0:1].astype(F32)
        cosines = jnp.cos(angles)
        sines = jnp.sin(angles)
        for piece in range(2):
            span = slice(piece * half, (piece + 1) * half)
            start_ref[2 * part + piece] = start[:, span]
            cos_ref[2 * part + piece] = cosines[:, span]
            sin_ref[2 * part + piece] = sines[:, span]


def exchange_heads(wire, base, o_all, obuf, relay, me, left, right, far):
    width = o_all.shape[1]
    low, high = pl.ds(0, width // 2), pl.ds(width // 2, width // 2)
    to_left, to_right = {'mp': left}, {'mp': right}
    return [
        wire.copy(base, o_all.at[far, low], relay.at[0], to_right),
        wire.copy(base + 1, o_all.at[far, high], relay.at[1], to_left),
        wire.copy(base + 2, o_all.at[right], obuf.at[0], to_right),
        wire.copy(base + 3, o_all.at[left], obuf.at[1], to_left),
        wire.copy(base + 4, relay.at[0], obuf.at[2, low], to_right),
        wire.copy(base + 5, relay.at[1], obuf.at[2, high], to_left),
    ]


def own_blocks(experts, keys):
    group = experts[0].shape[1] // 2
    return [experts[matrix].at[layer, pl.ds(side * group, group)] for layer, matrix, side in keys]


def attend_kernel(first, layer, parts, shards, heads, head_dim, fetch_keys, *refs):
    refs = list(refs)
    num_fetch = len(fetch_keys)
    r_ref, gain_attn, gain_mlp = refs[:3]
    del refs[:3]
    if first:
        inv_ref, seg_ref, ids_ref, gates_ref, wq_ref, wk_ref, wv_ref, wo_in = refs[:8]
        del refs[:8]
    else:
        cos_in, sin_in, start_in, qkv_all, out_all = refs[:5]
        del refs[:5]
    fetch_own = own_blocks(refs[:3], fetch_keys)
    del refs[:3]
    res_ref, h_ref = refs[:2]
    del refs[:2]
    if first:
        ints_out, gates_out, qkv_all, out_all, qkv_rest, out_rest, cos_ref, sin_ref, start_ref = refs[:9]
        del refs[:9]
    fetch_all = refs[:num_fetch]
    del refs[:num_fetch]
    if not first:
        cos_ref, sin_ref, start_ref = refs[:3]
        del refs[:3]
    if first:
        ints_all, gates_all, qkv_pack, out_pack = refs[:4]
        del refs[:4]
    if num_fetch:
        stage, stage_sem = refs[:2]
        del refs[:2]
    hbuf, w_raw, w_sc, q_sc, k_sc, v_sc, m_sc, l_sc, acc_sc, s_sc, o_all, obuf, relay, wo_ref = refs[:14]
    send_sem, recv_sem, local_sem = refs[14:]

    me, left, right, far = ring('mp', parts)
    tok = lax.axis_index('tok')
    to_left, to_right = {'mp': left}, {'mp': right}
    wire = Wire(send_sem, recv_sem)
    tokens, hidden = res_ref.shape
    rows = tokens // 2
    width = heads * head_dim
    span = q_sc.shape[-1]
    pieces = rows // span
    tiles = 2 * parts
    units = [(head, piece) for head in range(heads) for piece in range(pieces)]

    fetches = [StagedGather(wire, 41 + index * ShardGather.COPIES, own, stage.at[index], blocks, shards, stage_sem.at[index]) for index, (own, blocks) in enumerate(zip(fetch_own, fetch_all))]
    for fetch in fetches:
        fetch.load.start()
    if first:
        for index, ref in enumerate((wq_ref, wk_ref, wv_ref)):
            qkv_pack[:, index * width:(index + 1) * width] = ref[...]
        for index in range(out_pack.shape[0]):
            out_pack[index] = wo_in[index].astype(F32).T.astype(BF16)
        ints_all[me, 0:1] = seg_ref[...]
        ints_all[me, 1:3] = ids_ref[...]
        gates_all[me, 0:2] = gates_ref[...]
        qkv = ShardGather(wire, 21, qkv_pack.at[layer], qkv_all, shards, local_sem.at[3])
        out = ShardGather(wire, 31, out_rest.at[layer], out_all, shards, local_sem.at[2])
    meet([to_left, to_right] + tok_devices(shards))
    if first:
        qkv.start()
        small = [
            wire.copy(0, ints_all.at[me], ints_all.at[me], to_right),
            wire.copy(1, ints_all.at[me], ints_all.at[me], to_left),
            wire.copy(2, gates_all.at[me], gates_all.at[me], to_right),
            wire.copy(3, gates_all.at[me], gates_all.at[me], to_left),
            wire.copy(4, out_pack, out_rest.at[:, me], to_right),
            wire.copy(5, out_pack, out_rest.at[:, me], to_left),
        ]
        onward = [
            wire.copy(6, ints_all.at[left], ints_all.at[left], to_right),
            wire.copy(7, gates_all.at[right], gates_all.at[right], to_left),
            wire.copy(8, out_rest.at[:, left], out_rest.at[:, left], to_right),
        ]
        local = [
            pltpu.make_async_copy(out_pack, out_rest.at[:, me], local_sem.at[0]),
            pltpu.make_async_copy(qkv_pack, qkv_rest, local_sem.at[1]),
        ]
        for copy in small + local:
            copy.start()
    else:
        local = [
            pltpu.make_async_copy(qkv_all, w_raw, local_sem.at[3]),
            pltpu.make_async_copy(cos_in, cos_ref, local_sem.at[0]),
            pltpu.make_async_copy(sin_in, sin_ref, local_sem.at[1]),
            pltpu.make_async_copy(start_in, start_ref, local_sem.at[2]),
        ]
        for copy in local:
            copy.start()
    hbuf[me] = rms_norm(r_ref[...].astype(F32), gain_attn[layer:layer + 1])
    rows_in = ring_gather(wire, 9, hbuf.at[me], hbuf, 'mp', left, right, me)
    for name in FIRST:
        rows_in[name].start()
    if first:
        for copy in small:
            copy.wait_recv()
        for copy in onward:
            copy.start()
        qkv.onward()
        onward[0].wait_recv()
        request_tables(parts, ints_all, inv_ref, cos_ref, sin_ref, start_ref)
        ints_out[...] = ints_all[...]
        onward[1].wait_recv()
        gates_out[...] = gates_all[...]
        onward[2].wait_recv()
        local[0].wait()
        out.start()
        fetches[0].start()
        qkv.share_near()
        qkv.share_far()
        qkv.finish()
        load = pltpu.make_async_copy(qkv_all, w_raw, local_sem.at[4])
        load.start()
        load.wait()
    else:
        if fetches:
            fetches[0].start()
        for copy in local:
            copy.wait()
    depth = w_raw.shape[-1]
    for shard in range(shards):
        w_sc[:, shard * depth:(shard + 1) * depth] = w_raw[shard]

    half_dim = head_dim // 2
    scale = head_dim ** -0.5

    def tile_of(index):
        pair = index // 2
        odd = lax.rem(index, 2)
        between = (pair * (3 - pair)) // 2
        last_pair = (pair * (pair - 1) * (pair - 2)) // 6
        third = (pair * (pair - 1) * (3 - pair)) // 2
        chunk = lax.rem(me + between * (3 - 2 * odd) + 2 * last_pair, parts)
        side = odd + third * (1 - 2 * odd)
        return chunk, side

    def score(unit, query_tile, key_tile, keys):
        head, _ = units[unit]
        return jnp.dot(k_sc[key_tile, head, :keys], q_sc[query_tile, unit], preferred_element_type=F32)

    def absorb(unit, scores, query_tile, key_tile, causal):
        head, piece = units[unit]
        keys = scores.shape[0]
        key_row = lax.broadcasted_iota(jnp.int32, (keys, span), 0)
        allowed = key_row >= start_ref[query_tile, 0:1, piece * span:(piece + 1) * span] - key_tile * rows
        if causal:
            allowed = allowed & (key_row <= lax.broadcasted_iota(jnp.int32, (keys, span), 1) + piece * span)
        scores = jnp.where(allowed, scores, NEG)
        old_max = m_sc[query_tile, unit:unit + 1]
        new_max = jnp.maximum(old_max, jnp.max(scores, axis=0, keepdims=True))
        prob = jnp.exp(scores - new_max)
        fade = jnp.exp(old_max - new_max)
        m_sc[query_tile, unit:unit + 1] = new_max
        l_sc[query_tile, unit:unit + 1] = fade * l_sc[query_tile, unit:unit + 1] + jnp.sum(prob, axis=0, keepdims=True)
        value = v_sc[key_tile, head * head_dim:(head + 1) * head_dim, :keys]
        part = jnp.dot(value, prob.astype(BF16), preferred_element_type=F32)
        acc_sc[query_tile, unit] = acc_sc[query_tile, unit] * fade + part

    def block(query_tile, key_tile, following):
        diagonal = following is None

        def keys_of(unit):
            return (units[unit][1] + 1) * span if diagonal else rows

        waiting = [s_sc[unit, :keys_of(unit)] for unit in range(AHEAD)]
        for unit in range(len(units)):
            ahead = unit + AHEAD
            if ahead < len(units):
                waiting.append(score(ahead, query_tile, key_tile, keys_of(ahead)))
            elif not diagonal:
                s_sc[ahead - len(units)] = score(ahead - len(units), following[0], following[1], rows)
            absorb(unit, waiting.pop(0), query_tile, key_tile, diagonal)

    def arrive(index, carry):
        chunk, side = tile_of(index)
        tile = 2 * chunk + side

        @pl.when(index == 1)
        def _():
            if first:
                out.onward()
            for fetch in fetches[1:2]:
                fetch.start()

        @pl.when(index == 2)
        def _():
            rows_in['right_low'].wait_recv()
            rows_in['on_right'].start()

        @pl.when(index == 3)
        def _():
            rows_in['left_high'].wait_recv()
            rows_in['on_left'].start()

        @pl.when(index == 4)
        def _():
            rows_in['right_high'].wait_recv()
            for fetch in fetches[:1]:
                fetch.onward()
                fetch.share_near()
            for fetch in fetches[2:3]:
                fetch.start()
            if first:
                out.share_near()
                out.share_far()

        @pl.when(index == 5)
        def _():
            rows_in['left_low'].wait_recv()
            for fetch in fetches[3:4]:
                fetch.start()

        @pl.when(index == 6)
        def _():
            rows_in['on_right'].wait_recv()
            for fetch in fetches[1:2]:
                fetch.onward()
                fetch.share_near()
            for fetch in fetches[:1]:
                fetch.share_far()

        @pl.when(index == 7)
        def _():
            rows_in['on_left'].wait_recv()
            for fetch in fetches[2:3]:
                fetch.onward()

        x = hbuf[chunk, pl.ds(pl.multiple_of(side * rows, rows), rows)]
        qkv_rows = lax.dot_general(w_sc[...], x, NT, preferred_element_type=F32)
        cosines = cos_ref[tile]
        sines = sin_ref[tile]

        def rotate(base):
            one = qkv_rows[base:base + half_dim]
            two = qkv_rows[base + half_dim:base + head_dim]
            return jnp.concatenate([one * cosines - two * sines, two * cosines + one * sines], axis=0)

        for head in range(heads):
            base = head * head_dim
            query = (rotate(base).astype(BF16).astype(F32) * scale).astype(BF16)
            for piece in range(pieces):
                q_sc[tile, head * pieces + piece] = query[:, piece * span:(piece + 1) * span]
            k_sc[tile, head] = rotate(width + base).T.astype(BF16)
        v_sc[tile] = qkv_rows[2 * width:3 * width].astype(BF16)
        m_sc[tile] = jnp.full(m_sc.shape[1:], NEG, F32)
        l_sc[tile] = jnp.zeros(l_sc.shape[1:], F32)
        acc_sc[tile] = jnp.zeros(acc_sc.shape[1:], F32)

        def ordered(other):
            other_chunk, other_side = tile_of(other)
            other_tile = 2 * other_chunk + other_side
            ahead = (tile - other_tile + tiles) // tiles
            upper = other_tile + ahead * (tile - other_tile)
            return upper, tile + other_tile - upper

        upper, lower = ordered(jnp.int32(0))
        for unit in range(AHEAD):
            s_sc[unit] = score(unit, upper, lower, rows)

        def pair(other, inner):
            query_tile, key_tile = ordered(other)
            block(query_tile, key_tile, ordered(other + 1))
            return inner

        lax.fori_loop(0, index, pair, 0)
        block(tile, tile, None)
        return carry

    lax.fori_loop(0, tiles, arrive, 0)
    wo_copy = pltpu.make_async_copy(out_all, wo_ref, local_sem.at[5])
    if first:
        out.finish()
    wo_copy.start()
    for tile in range(tiles):
        for unit, (head, piece) in enumerate(units):
            top = head * head_dim
            edge = (tile % 2) * rows + piece * span
            o_all[tile // 2, top:top + head_dim, edge:edge + span] = (acc_sc[tile, unit] / l_sc[tile, unit:unit + 1]).astype(BF16)

    exchange = exchange_heads(wire, 15, o_all, obuf, relay, me, left, right, far)
    for copy in exchange[:4]:
        copy.start()
    for fetch in fetches[3:4]:
        fetch.onward()
    exchange[0].wait_recv()
    exchange[4].start()
    exchange[1].wait_recv()
    exchange[5].start()
    for fetch in fetches[2:4]:
        fetch.share_near()
    wo_copy.wait()
    chunk = min(256, tokens)

    def project(sources, last):
        def step(index, carry):
            lanes = pl.ds(pl.multiple_of(index * chunk, chunk), chunk)
            total = None
            for source, piece in sources:
                weight = wo_ref[:, source].reshape(hidden, width)
                term = jnp.dot(weight, piece[:, lanes], preferred_element_type=F32)
                total = term if total is None else total + term
            residual = (res_ref[lanes] if last else r_ref[lanes].astype(F32)) + total.T
            res_ref[lanes] = residual
            if last:
                h_ref[lanes] = rms_norm(residual, gain_mlp[layer:layer + 1])
            return carry

        lax.fori_loop(0, tokens // chunk, step, 0)

    project([(me, o_all.at[me])], False)
    exchange[2].wait_recv()
    exchange[3].wait_recv()
    exchange[4].wait_recv()
    exchange[5].wait_recv()
    for fetch in fetches[1:3]:
        fetch.share_far()
    project([(left, obuf.at[0]), (right, obuf.at[1]), (far, obuf.at[2])], True)

    for fetch in fetches[3:4]:
        fetch.share_far()
    for fetch in fetches:
        fetch.finish()
    for copy in exchange + list(rows_in.values()):
        copy.wait_send()
    if first:
        for copy in small + onward:
            copy.wait_send()
        local[1].wait()


def attend(first, layer, parts, shards, heads, head_dim, residual, gain_attn, gain_mlp, side_inputs, experts, fetch_keys, gathered_shape, ints_shape):
    tokens, hidden = residual.shape
    rows = tokens // 2
    width = heads * head_dim
    tiles = 2 * parts
    span = min(256, rows)
    units = heads * rows // span
    depth = hidden // shards
    num_layers = gain_attn.shape[0]
    anywhere = pl.BlockSpec(memory_space=pl.ANY)
    vmem = pl.BlockSpec(memory_space=pltpu.VMEM)
    num_fetch = len(fetch_keys)
    in_specs = [vmem] * 3 + ([vmem] * 8 if first else [anywhere] * 5) + [anywhere] * 3
    out_shape = [jax.ShapeDtypeStruct((tokens, hidden), F32), jax.ShapeDtypeStruct((tokens, hidden), BF16)]
    out_specs = [vmem, vmem]
    tables = [((tiles, head_dim // 2, rows), F32), ((tiles, head_dim // 2, rows), F32), ((tiles, 8, rows), jnp.int32)]
    if first:
        out_shape += [
            jax.ShapeDtypeStruct((parts,) + ints_shape, jnp.int32),
            jax.ShapeDtypeStruct((parts,) + ints_shape, F32),
            jax.ShapeDtypeStruct((shards, 3 * width, depth), BF16),
            jax.ShapeDtypeStruct((shards, parts, depth, width), BF16),
            jax.ShapeDtypeStruct((num_layers, 3 * width, depth), BF16),
            jax.ShapeDtypeStruct((num_layers, parts, depth, width), BF16),
        ] + [jax.ShapeDtypeStruct(shape, dtype) for shape, dtype in tables]
        out_specs += [vmem, vmem] + [anywhere] * 4 + [vmem] * 3
    out_shape += [jax.ShapeDtypeStruct((shards,) + gathered_shape, BF16)] * num_fetch
    out_specs += [anywhere] * num_fetch
    scratch = [
        pltpu.VMEM((parts,) + ints_shape, jnp.int32),
        pltpu.VMEM((parts,) + ints_shape, F32),
        pltpu.VMEM((num_layers, 3 * width, depth), BF16),
        pltpu.VMEM((num_layers, depth, width), BF16),
    ] if first else [pltpu.VMEM(shape, dtype) for shape, dtype in tables]
    copies = 41 + num_fetch * ShardGather.COPIES
    if num_fetch:
        scratch += [pltpu.VMEM((num_fetch, shards) + gathered_shape, BF16), pltpu.SemaphoreType.DMA((num_fetch, 1 + shards))]
    scratch += [
        pltpu.VMEM((parts, tokens, hidden), BF16),
        pltpu.VMEM((shards, 3 * width, depth), BF16),
        pltpu.VMEM((3 * width, hidden), BF16),
        pltpu.VMEM((tiles, units, head_dim, span), BF16),
        pltpu.VMEM((tiles, heads, rows, head_dim), BF16),
        pltpu.VMEM((tiles, width, rows), BF16),
        pltpu.VMEM((tiles, max(8, units), span), F32),
        pltpu.VMEM((tiles, max(8, units), span), F32),
        pltpu.VMEM((tiles, units, head_dim, span), F32),
        pltpu.VMEM((AHEAD, rows, span), F32),
        pltpu.VMEM((parts, width, tokens), BF16),
        pltpu.VMEM((3, width, tokens), BF16),
        pltpu.VMEM((2, width // 2, tokens), BF16),
        pltpu.VMEM((shards, parts, depth, width), BF16),
        pltpu.SemaphoreType.DMA((copies,)),
        pltpu.SemaphoreType.DMA((copies,)),
        pltpu.SemaphoreType.DMA((6,)),
    ]
    seq_len = parts * tokens
    return pl.pallas_call(
        functools.partial(attend_kernel, first, layer, parts, shards, heads, head_dim, tuple(fetch_keys)),
        in_specs=in_specs,
        out_specs=out_specs,
        out_shape=out_shape,
        scratch_shapes=scratch,
        compiler_params=pltpu.CompilerParams(collective_id=2 * layer, has_side_effects=True, vmem_limit_bytes=VMEM_LIMIT),
        cost_estimate=pl.CostEstimate(flops=2 * seq_len * seq_len * width + 8 * seq_len * hidden * width, bytes_accessed=8 * seq_len * hidden, transcendentals=seq_len * seq_len * heads // 2),
        name='attend',
    )(residual, gain_attn, gain_mlp, *side_inputs, *experts)


def mix_kernel(layer, parts, shards, late_keys, next_keys, late_mats, *refs):
    refs = list(refs)
    num_late = len(late_keys)
    num_next = len(next_keys)
    r_ref, h_ref, ints_ref, gates_ref = refs[:4]
    del refs[:4]
    given = refs[:6 - num_late]
    del refs[:6 - num_late]
    late_own = own_blocks(refs[:3], late_keys)
    next_own = own_blocks(refs[:3], next_keys)
    del refs[:3]
    if next_keys:
        next_own += [refs[0].at[layer + 1], refs[1].at[layer + 1]]
        del refs[:2]
        num_next += 2
    res_ref = refs.pop(0)
    late_all = refs[:num_late]
    del refs[:num_late]
    next_all = refs[:num_next]
    del refs[:num_next]
    hbuf, wbuf, acc, inbox, route, send_sem, recv_sem, w_sem, local_sem = refs
    mats = list(given)
    for position, ref in zip(late_mats, late_all):
        mats.insert(position, ref)

    me, left, right, _ = ring('mp', parts)
    to_left, to_right = {'mp': left}, {'mp': right}
    wire = Wire(send_sem, recv_sem)
    _, group, depth, ffn = mats[0].shape
    num_experts = 2 * group
    tokens, hidden = res_ref.shape
    half = tokens // 2
    low, high = pl.ds(0, half), pl.ds(half, half)
    steps = 16 * group
    waits_late = bool(late_keys)
    gate_step = (8 if waits_late else 4) * group - (SLOTS - 1)

    def place(step):
        turn = lax.div(step, group)
        odd = lax.rem(turn, 2)
        since = {edge: lax.div(turn + 16 - edge, 16) for edge in (4, 6, 8, 14)}
        main = lax.div(turn, 2)
        if waits_late:
            buffer = turn + 2 * since[4] - 4 * since[6] - 4 * since[8] - 8 * since[14]
            late = since[8]
        else:
            buffer = turn - 2 * since[4] + since[6] * (main + 3 - turn) + since[14] * (turn - 15 - main)
            late = since[4] * (1 - since[6]) + since[6] * (1 - since[14]) * odd + since[14]
        return turn, buffer, late, lax.rem(step, group)

    def weight_copies(step, side):
        _, _, _, expert = place(step)
        slot = lax.rem(step, SLOTS)
        return [pltpu.make_async_copy(mats[2 * index + side].at[:, expert], wbuf.at[slot, index], w_sem.at[slot, index]) for index in range(3)]

    def start_weights(step):
        _, _, late, _ = place(step)
        for side in range(2):

            @pl.when(late == side)
            def _(side=side):
                for copy in weight_copies(step, side):
                    copy.start()

    late_fetch = [ShardGather(wire, 12 + index * ShardGather.COPIES, own, blocks, shards, local_sem.at[index]) for index, (own, blocks) in enumerate(zip(late_own, late_all))]
    base = 12 + num_late * ShardGather.COPIES
    next_fetch = [ShardGather(wire, base + index * ShardGather.COPIES, own, blocks, shards, local_sem.at[num_late + index]) for index, (own, blocks) in enumerate(zip(next_own, next_all))]
    for step in range(SLOTS - 1):
        start_weights(jnp.int32(step))
    meet([to_left, to_right] + (tok_devices(shards) if late_fetch or next_fetch else []))
    rows_in = ring_gather(wire, 0, h_ref, hbuf, 'mp', left, right, me)
    for name in FIRST:
        rows_in[name].start()
    for fetch in late_fetch:
        fetch.start()
    hbuf[me] = h_ref[...]
    expert_row = lax.broadcasted_iota(jnp.int32, (num_experts, 1), 0)
    for part in range(parts):
        share = jnp.zeros((num_experts, tokens), F32)
        for choice in range(2):
            share = share + jnp.where(ints_ref[part, 1 + choice:2 + choice] == expert_row, gates_ref[part, choice:choice + 1], 0.0)
        route[part] = share.T

    sends = {
        2: wire.copy(6, acc.at[2], inbox.at[0], to_left),
        3: wire.copy(7, acc.at[3], inbox.at[1], to_right),
        4: wire.copy(8, acc.at[4], inbox.at[2], to_right),
        5: wire.copy(9, acc.at[5], inbox.at[3], to_left),
        6: wire.copy(10, acc.at[6], inbox.at[4], to_right),
        7: wire.copy(11, acc.at[7], inbox.at[5], to_left),
    }
    tile_rows = min(256, half)
    tiles = half // tile_rows
    lane = lax.broadcasted_iota(jnp.int32, (tile_rows, num_experts), 1)

    def rows_low_right():
        rows_in['right_low'].wait_recv()
        rows_in['on_right'].start()
        for fetch in late_fetch[:1]:
            fetch.onward()

    def rows_high_left():
        rows_in['left_high'].wait_recv()
        rows_in['on_left'].start()
        for fetch in late_fetch[1:2]:
            fetch.onward()
        for fetch in late_fetch[:1]:
            fetch.share_near()

    def rows_low_left():
        rows_in['left_low'].wait_recv()
        for fetch in late_fetch[2:]:
            fetch.onward()
        for fetch in late_fetch[1:2]:
            fetch.share_near()

    def rows_high_right():
        rows_in['right_high'].wait_recv()
        for fetch in late_fetch[2:]:
            fetch.share_near()

    def rows_far_low():
        rows_in['on_right'].wait_recv()
        for fetch in late_fetch[:1]:
            fetch.share_far()

    def rows_far_high():
        rows_in['on_left'].wait_recv()
        for fetch in late_fetch[1:]:
            fetch.share_far()

    def next_near():
        for fetch in next_fetch:
            fetch.onward()
            fetch.share_near()

    def sums():
        sends[4].wait_recv()
        acc[6] += inbox[2]
        sends[6].start()
        sends[5].wait_recv()
        acc[7] += inbox[3]
        sends[7].start()
        for fetch in next_fetch:
            fetch.share_far()

    if waits_late:
        fresh = (0, 1, 2, 3, 4, 5, 6, 7)
        events = {
            2: [rows_low_right],
            3: [rows_high_left],
            4: [rows_low_left],
            5: [rows_high_right],
            6: [rows_far_low],
            7: [rows_far_high],
            9: [sends[2].start],
            10: [sends[3].start],
            11: [sends[4].start],
            12: [sends[5].start, next_near],
            14: [sums],
        }
    else:
        fresh = (0, 1, 2, 3, 6, 8, 10, 12)
        events = {
            2: [rows_low_right],
            3: [rows_high_left],
            5: [sends[2].start],
            6: [sends[3].start, rows_far_low],
            8: [sends[4].start, rows_far_high],
            10: [sends[5].start, rows_low_left, next_near],
            12: [rows_high_right],
            14: [sums],
        }

    def begin(turn, buffer):
        clear = turn == fresh[0]
        for other in fresh[1:]:
            clear = clear | (turn == other)

        @pl.when(clear)
        def _():
            acc[buffer] = jnp.zeros((half, hidden), F32)

        for when, actions in events.items():

            @pl.when(turn == when)
            def _(actions=actions):
                for action in actions:
                    action()

    def expert_step(step, carry):
        turn, buffer, late, index = place(step)
        slot = lax.rem(step, SLOTS)
        expert = late * group + index
        pair = lax.div(buffer, 2)
        side = lax.rem(buffer, 2)
        odd = lax.rem(pair, 2)
        upper = lax.div(pair, 2)
        shift = odd * (upper * (1 + 2 * side) + (1 - upper) * (3 - 2 * side)) + (1 - odd) * 2 * upper
        source = lax.rem(me + shift, parts)
        start = pl.multiple_of(side * half, half)

        if late_fetch or next_fetch:

            @pl.when(step == gate_step)
            def _():
                for fetch in late_fetch:
                    fetch.finish()
                for fetch in next_fetch:
                    fetch.start()

        @pl.when(step + SLOTS - 1 < steps)
        def _():
            start_weights(step + SLOTS - 1)

        @pl.when(index == 0)
        def _():
            begin(turn, buffer)

        for copy in weight_copies(step, 0):
            copy.wait()

        def activate(tile):
            gate_w = wbuf[slot, 0].reshape(hidden, ffn)
            up_w = wbuf[slot, 1].reshape(hidden, ffn)
            x = hbuf[source, pl.ds(start + tile * tile_rows, tile_rows)]
            gate_pre = jnp.dot(x, gate_w, preferred_element_type=F32)
            up_pre = jnp.dot(x, up_w, preferred_element_type=F32)
            return (gate_pre * (1.0 / (1.0 + jnp.exp(-gate_pre))) * up_pre).astype(BF16)

        def contract(tile, act):
            down_w = wbuf[slot, 2].reshape(hidden, ffn)
            part_share = route[source, pl.ds(start + tile * tile_rows, tile_rows)]
            share = jnp.sum(jnp.where(lane == expert, part_share, 0.0), axis=1, keepdims=True)
            mixed = lax.dot_general(act, down_w, NT, preferred_element_type=F32)
            acc[buffer, tile * tile_rows:(tile + 1) * tile_rows] += share * mixed

        act = activate(0)
        for tile in range(tiles):
            following = activate(tile + 1) if tile + 1 < tiles else None
            contract(tile, act)
            act = following
        return carry

    lax.fori_loop(0, steps, expert_step, 0)

    sends[2].wait_recv()
    res_ref[low] = r_ref[low] + acc[0] + inbox[0]
    sends[3].wait_recv()
    res_ref[high] = r_ref[high] + acc[1] + inbox[1]
    sends[6].wait_recv()
    res_ref[low] += inbox[4]
    sends[7].wait_recv()
    res_ref[high] += inbox[5]
    for copy in list(rows_in.values()) + list(sends.values()):
        copy.wait_send()
    for fetch in next_fetch:
        fetch.finish()


def mix(layer, parts, shards, residual, normed, ints_all, gates_all, weights, experts, late_keys, late_mats, next_keys, attention_packs):
    tokens, hidden = residual.shape
    group, depth, ffn = weights[0].shape[1:]
    half = tokens // 2
    anywhere = pl.BlockSpec(memory_space=pl.ANY)
    vmem = pl.BlockSpec(memory_space=pltpu.VMEM)
    packs = attention_packs if next_keys else []
    num_fetch = len(late_keys) + len(next_keys) + len(packs)
    copies = 12 + num_fetch * ShardGather.COPIES
    return pl.pallas_call(
        functools.partial(mix_kernel, layer, parts, shards, tuple(late_keys), tuple(next_keys), late_mats),
        in_specs=[vmem] * 4 + [anywhere] * (len(weights) + 3 + len(packs)),
        out_specs=[vmem] + [anywhere] * num_fetch,
        out_shape=[jax.ShapeDtypeStruct((tokens, hidden), F32)]
        + [jax.ShapeDtypeStruct((shards, group, depth, ffn), BF16)] * (len(late_keys) + len(next_keys))
        + [jax.ShapeDtypeStruct((shards,) + pack.shape[1:], BF16) for pack in packs],
        scratch_shapes=[
            pltpu.VMEM((parts, tokens, hidden), BF16),
            pltpu.VMEM((SLOTS, 3, shards, depth, ffn), BF16),
            pltpu.VMEM((8, half, hidden), F32),
            pltpu.VMEM((6, half, hidden), F32),
            pltpu.VMEM((parts, tokens, 2 * group), F32),
            pltpu.SemaphoreType.DMA((copies,)),
            pltpu.SemaphoreType.DMA((copies,)),
            pltpu.SemaphoreType.DMA((SLOTS, 3)),
            pltpu.SemaphoreType.DMA((max(1, num_fetch),)),
        ],
        compiler_params=pltpu.CompilerParams(collective_id=2 * layer + 1, has_side_effects=True, vmem_limit_bytes=VMEM_LIMIT),
        cost_estimate=pl.CostEstimate(
            flops=12 * parts * tokens * hidden * ffn * group,
            bytes_accessed=96 * group * hidden * ffn,
            transcendentals=2 * parts * tokens * ffn * group,
        ),
        name='mix',
    )(residual, normed, ints_all, gates_all, *weights, *experts, *packs)


def solution(mesh):
    token_spec = P(('rep', 'tok', 'mp'))
    row_spec = P(('rep', 'tok', 'mp'), None)
    head_weight = P(None, 'tok', 'mp', None)
    in_specs = (row_spec, token_spec, row_spec, row_spec, head_weight, head_weight, head_weight, P(None, 'mp', None, 'tok'), P(None, None, 'tok', 'mp'), P(None, None, 'tok', 'mp'), P(None, None, 'mp', 'tok'), P(None, None), P(None, None))
    parts = mesh.shape['mp']
    shards = mesh.shape['tok']

    def device_step(hidden_in, seg_ids, expert_ids, expert_gates, w_query, w_key, w_value, w_out, w_gate, w_up, w_down, gain_attn, gain_mlp):
        num_layers, depth, heads, head_dim = w_query.shape
        tokens, _ = hidden_in.shape
        group = w_gate.shape[1] // 2
        width = heads * head_dim
        ffn = w_gate.shape[-1]

        experts_local = [w_gate, w_up, jnp.swapaxes(w_down, 2, 3)]
        halves = [[(layer, matrix, side) for matrix in range(3) for side in range(2)] for layer in range(num_layers)]

        qkv_local = [jnp.transpose(w, (0, 2, 3, 1)).reshape(num_layers, width, depth) for w in (w_query, w_key, w_value)]
        out_local = w_out.reshape(num_layers, width, depth)
        inv_freq = jnp.power(ROPE_BASE, -jnp.arange(head_dim // 2, dtype=F32) * 2.0 / head_dim)[:, None]

        shape = (group, depth, ffn)
        gathered = {}
        residual = hidden_in
        side_inputs = [inv_freq, seg_ids[None, :], expert_ids.T, expert_gates.T] + qkv_local + [out_local]
        plan = {0: halves[0][::2]}
        for layer in range(num_layers):
            first = layer == 0
            fetch = plan.get(layer, [])
            fetch = [key for key in fetch if key not in gathered]
            outs = attend(first, layer, parts, shards, heads, head_dim, residual, gain_attn, gain_mlp, side_inputs, experts_local, fetch, shape, (8, tokens))
            residual, normed = outs[:2]
            outs = outs[2:]
            if first:
                ints_all, gates_all, _, _, qkv_rest, out_rest = outs[:6]
                tables = list(outs[6:9])
                outs = outs[9:]
            gathered.update(zip(fetch, outs))
            late = [key for key in halves[layer] if key not in gathered]
            late_mats = tuple(halves[layer].index(key) for key in late)
            weights = [gathered[key] for key in halves[layer] if key in gathered]
            following = []
            if layer + 1 < num_layers:
                following = halves[layer + 1][:4]
                plan[layer + 1] = halves[layer + 1][4:]
            outs = mix(layer, parts, shards, residual, normed, ints_all, gates_all, weights, experts_local, late, late_mats, following, [qkv_rest, out_rest])
            residual = outs[0]
            gathered.update(zip(late + following, outs[1:]))
            side_inputs = tables + list(outs[-2:])
        return residual

    return jax.shard_map(device_step, mesh=mesh, in_specs=in_specs, out_specs=row_spec, check_vma=False)
```

```python
import functools

import jax
import jax.numpy as jnp
from jax import lax
from jax.experimental import pallas as pl
from jax.experimental.pallas import tpu as pltpu
from jax.sharding import PartitionSpec as P

EPS = 1e-5
ROPE_BASE = 10000.0
NEG = -1e30
VMEM_LIMIT = 63 * 1024 * 1024
AHEAD = 2
SLOTS = 3
F32 = jnp.float32
BF16 = jnp.bfloat16
NT = (((1,), (1,)), ((), ()))
MESH = pl.DeviceIdType.MESH
FIRST = ('right_low', 'left_high', 'right_high', 'left_low')


def rms_norm(residual, gain):
    inv_rms = lax.rsqrt(jnp.mean(residual * residual, axis=-1, keepdims=True) + EPS)
    return (residual * inv_rms * gain.astype(F32)).astype(BF16)


class Wire:
    def __init__(self, send_sem, recv_sem):
        self.send_sem = send_sem
        self.recv_sem = recv_sem

    def copy(self, slot, src, dst, device):
        return pltpu.make_async_remote_copy(src_ref=src, dst_ref=dst, send_sem=self.send_sem.at[slot], recv_sem=self.recv_sem.at[slot], device_id=device, device_id_type=MESH)


def ring(axis, size):
    me = lax.axis_index(axis)
    return me, lax.rem(me + size - 1, size), lax.rem(me + 1, size), lax.rem(me + size // 2, size)


def meet(devices):
    barrier = pltpu.get_barrier_semaphore()
    for device in devices:
        pl.semaphore_signal(barrier, inc=1, device_id=device, device_id_type=MESH)
    pl.semaphore_wait(barrier, len(devices))


def ring_gather(wire, base, own, rows_all, axis, left, right, me):
    half = own.shape[0] // 2
    low, high = pl.ds(0, half), pl.ds(half, half)
    to_right, to_left = {axis: right}, {axis: left}
    return {
        'right_low': wire.copy(base, own.at[low], rows_all.at[me, low], to_right),
        'right_high': wire.copy(base + 1, own.at[high], rows_all.at[me, high], to_right),
        'left_high': wire.copy(base + 2, own.at[high], rows_all.at[me, high], to_left),
        'left_low': wire.copy(base + 3, own.at[low], rows_all.at[me, low], to_left),
        'on_right': wire.copy(base + 4, rows_all.at[left, low], rows_all.at[left, low], to_right),
        'on_left': wire.copy(base + 5, rows_all.at[right, high], rows_all.at[right, high], to_left),
    }


def tok_devices(shards):
    tok = lax.axis_index('tok')
    return [{'tok': tok + 1 - 2 * lax.rem(tok, 2)}, {'tok': lax.rem(tok + shards - 2, shards)}, {'tok': lax.rem(tok + 2, shards)}]


class ShardGather:
    COPIES = 10

    def __init__(self, wire, base, own, blocks, shards, store_sem=None):
        tok = lax.axis_index('tok')
        left = lax.rem(tok + shards - 2, shards)
        right = lax.rem(tok + 2, shards)
        far = lax.rem(tok + shards // 2, shards)
        partner = {'tok': tok + 1 - 2 * lax.rem(tok, 2)}
        self.rows = ring_gather(wire, base, own, blocks, 'tok', left, right, tok)
        self.cross = [wire.copy(base + 6, own, blocks.at[tok], partner)]
        for index, source in enumerate((left, right, far)):
            self.cross.append(wire.copy(base + 7 + index, blocks.at[source], blocks.at[source], partner))
        self.store = None if store_sem is None else pltpu.make_async_copy(own, blocks.at[tok], store_sem)

    def start(self):
        for name in FIRST:
            self.rows[name].start()
        self.cross[0].start()
        if self.store is not None:
            self.store.start()

    def onward(self):
        self.rows['right_low'].wait_recv()
        self.rows['on_right'].start()
        self.rows['left_high'].wait_recv()
        self.rows['on_left'].start()

    def share_near(self):
        self.rows['right_high'].wait_recv()
        self.cross[1].start()
        self.rows['left_low'].wait_recv()
        self.cross[2].start()

    def share_far(self):
        self.rows['on_right'].wait_recv()
        self.rows['on_left'].wait_recv()
        self.cross[3].start()

    def finish(self):
        for copy in self.cross:
            copy.wait_recv()
        for copy in list(self.rows.values()) + self.cross:
            copy.wait_send()
        if self.store is not None:
            self.store.wait()


class StagedGather(ShardGather):
    def __init__(self, wire, base, source, stage, out, shards, sems):
        tok = lax.axis_index('tok')
        super().__init__(wire, base, stage.at[tok], stage, shards)
        self.load = pltpu.make_async_copy(source, stage.at[tok], sems.at[0])
        self.writes = []
        order = []
        for step in (0, shards - 2, 2, shards // 2):
            order.append(lax.rem(tok + step, shards))
        order += [block + 1 - 2 * lax.rem(block, 2) for block in order]
        for index, block in enumerate(order):
            self.writes.append(pltpu.make_async_copy(stage.at[block], out.at[block], sems.at[1 + index]))

    def start(self):
        self.load.wait()
        super().start()
        self.writes[0].start()

    def share_near(self):
        super().share_near()
        self.writes[1].start()
        self.writes[2].start()

    def share_far(self):
        super().share_far()
        self.writes[3].start()

    def finish(self):
        for copy, write in zip(self.cross, self.writes[4:]):
            copy.wait_recv()
            write.start()
        for copy in list(self.rows.values()) + self.cross:
            copy.wait_send()
        for write in self.writes:
            write.wait()


def request_tables(parts, ints, inv_ref, cos_ref, sin_ref, start_ref):
    tokens = ints.shape[-1]
    half = tokens // 2
    lane = lax.broadcasted_iota(jnp.int32, (8, tokens), 1)
    carry = last = None
    for part in range(parts):
        seg = jnp.broadcast_to(ints[part, 0:1], (8, tokens))
        before = pltpu.roll(seg, 1, 1)
        if part == 0:
            fresh = (lane == 0) | (seg != before)
        else:
            fresh = seg != jnp.where(lane == 0, last, before)
        start = jnp.where(fresh, lane + part * tokens, 0)
        shift = 1
        while shift < tokens:
            start = jnp.maximum(start, jnp.where(lane >= shift, pltpu.roll(start, shift, 1), 0))
            shift *= 2
        if carry is not None:
            start = jnp.maximum(start, carry)
        carry = jnp.broadcast_to(start[:, tokens - 1:], (8, tokens))
        last = jnp.broadcast_to(seg[:, tokens - 1:], (8, tokens))
        angles = inv_ref[...] * (lane + part * tokens - start)[0:1].astype(F32)
        cosines = jnp.cos(angles)
        sines = jnp.sin(angles)
        for piece in range(2):
            span = slice(piece * half, (piece + 1) * half)
            start_ref[2 * part + piece] = start[:, span]
            cos_ref[2 * part + piece] = cosines[:, span]
            sin_ref[2 * part + piece] = sines[:, span]


def exchange_heads(wire, base, o_all, obuf, relay, me, left, right, far):
    width = o_all.shape[1]
    low, high = pl.ds(0, width // 2), pl.ds(width // 2, width // 2)
    to_left, to_right = {'mp': left}, {'mp': right}
    return [
        wire.copy(base, o_all.at[far, low], relay.at[0], to_right),
        wire.copy(base + 1, o_all.at[far, high], relay.at[1], to_left),
        wire.copy(base + 2, o_all.at[right], obuf.at[0], to_right),
        wire.copy(base + 3, o_all.at[left], obuf.at[1], to_left),
        wire.copy(base + 4, relay.at[0], obuf.at[2, low], to_right),
        wire.copy(base + 5, relay.at[1], obuf.at[2, high], to_left),
    ]


def own_blocks(experts, keys):
    group = experts[0].shape[1] // 2
    return [experts[matrix].at[layer, pl.ds(side * group, group)] for layer, matrix, side in keys]


def attend_kernel(first, layer, parts, shards, heads, head_dim, fetch_keys, *refs):
    refs = list(refs)
    num_fetch = len(fetch_keys)
    r_ref, gain_attn, gain_mlp = refs[:3]
    del refs[:3]
    if first:
        inv_ref, seg_ref, ids_ref, gates_ref, wq_ref, wk_ref, wv_ref, wo_in = refs[:8]
        del refs[:8]
    else:
        cos_in, sin_in, start_in, qkv_all, out_all = refs[:5]
        del refs[:5]
    fetch_own = own_blocks(refs[:3], fetch_keys)
    del refs[:3]
    res_ref, h_ref = refs[:2]
    del refs[:2]
    if first:
        ints_out, gates_out, qkv_all, out_all, qkv_rest, out_rest, cos_ref, sin_ref, start_ref = refs[:9]
        del refs[:9]
    fetch_all = refs[:num_fetch]
    del refs[:num_fetch]
    if not first:
        cos_ref, sin_ref, start_ref = refs[:3]
        del refs[:3]
    if first:
        ints_all, gates_all, qkv_pack, out_pack = refs[:4]
        del refs[:4]
    if num_fetch:
        stage, stage_sem = refs[:2]
        del refs[:2]
    hbuf, w_raw, w_sc, q_sc, k_sc, v_sc, m_sc, l_sc, acc_sc, s_sc, o_all, obuf, relay, wo_ref = refs[:14]
    send_sem, recv_sem, local_sem = refs[14:]

    me, left, right, far = ring('mp', parts)
    tok = lax.axis_index('tok')
    to_left, to_right = {'mp': left}, {'mp': right}
    wire = Wire(send_sem, recv_sem)
    tokens, hidden = res_ref.shape
    rows = tokens // 2
    width = heads * head_dim
    span = q_sc.shape[-1]
    pieces = rows // span
    tiles = 2 * parts
    units = [(head, piece) for head in range(heads) for piece in range(pieces)]

    fetches = [StagedGather(wire, 41 + index * ShardGather.COPIES, own, stage.at[index], blocks, shards, stage_sem.at[index]) for index, (own, blocks) in enumerate(zip(fetch_own, fetch_all))]
    for fetch in fetches:
        fetch.load.start()
    if first:
        for index, ref in enumerate((wq_ref, wk_ref, wv_ref)):
            qkv_pack[:, index * width:(index + 1) * width] = ref[...]
        for index in range(out_pack.shape[0]):
            out_pack[index] = wo_in[index].astype(F32).T.astype(BF16)
        ints_all[me, 0:1] = seg_ref[...]
        ints_all[me, 1:3] = ids_ref[...]
        gates_all[me, 0:2] = gates_ref[...]
        qkv = ShardGather(wire, 21, qkv_pack.at[layer], qkv_all, shards, local_sem.at[3])
        out = ShardGather(wire, 31, out_rest.at[layer], out_all, shards, local_sem.at[2])
    meet([to_left, to_right] + tok_devices(shards))
    if first:
        qkv.start()
        small = [
            wire.copy(0, ints_all.at[me], ints_all.at[me], to_right),
            wire.copy(1, ints_all.at[me], ints_all.at[me], to_left),
            wire.copy(2, gates_all.at[me], gates_all.at[me], to_right),
            wire.copy(3, gates_all.at[me], gates_all.at[me], to_left),
            wire.copy(4, out_pack, out_rest.at[:, me], to_right),
            wire.copy(5, out_pack, out_rest.at[:, me], to_left),
        ]
        onward = [
            wire.copy(6, ints_all.at[left], ints_all.at[left], to_right),
            wire.copy(7, gates_all.at[right], gates_all.at[right], to_left),
            wire.copy(8, out_rest.at[:, left], out_rest.at[:, left], to_right),
        ]
        local = [
            pltpu.make_async_copy(out_pack, out_rest.at[:, me], local_sem.at[0]),
            pltpu.make_async_copy(qkv_pack, qkv_rest, local_sem.at[1]),
        ]
        for copy in small + local:
            copy.start()
    else:
        local = [
            pltpu.make_async_copy(qkv_all, w_raw, local_sem.at[3]),
            pltpu.make_async_copy(cos_in, cos_ref, local_sem.at[0]),
            pltpu.make_async_copy(sin_in, sin_ref, local_sem.at[1]),
            pltpu.make_async_copy(start_in, start_ref, local_sem.at[2]),
        ]
        for copy in local:
            copy.start()
    hbuf[me] = rms_norm(r_ref[...].astype(F32), gain_attn[layer:layer + 1])
    rows_in = ring_gather(wire, 9, hbuf.at[me], hbuf, 'mp', left, right, me)
    for name in FIRST:
        rows_in[name].start()
    if first:
        for copy in small:
            copy.wait_recv()
        for copy in onward:
            copy.start()
        qkv.onward()
        onward[0].wait_recv()
        request_tables(parts, ints_all, inv_ref, cos_ref, sin_ref, start_ref)
        ints_out[...] = ints_all[...]
        onward[1].wait_recv()
        gates_out[...] = gates_all[...]
        onward[2].wait_recv()
        local[0].wait()
        out.start()
        qkv.share_near()
        qkv.share_far()
        qkv.finish()
        load = pltpu.make_async_copy(qkv_all, w_raw, local_sem.at[4])
        load.start()
        load.wait()
    else:
        if fetches:
            fetches[0].start()
        for copy in local:
            copy.wait()
    depth = w_raw.shape[-1]
    for shard in range(shards):
        w_sc[:, shard * depth:(shard + 1) * depth] = w_raw[shard]

    half_dim = head_dim // 2
    scale = head_dim ** -0.5

    def tile_of(index):
        pair = index // 2
        odd = lax.rem(index, 2)
        between = (pair * (3 - pair)) // 2
        last_pair = (pair * (pair - 1) * (pair - 2)) // 6
        third = (pair * (pair - 1) * (3 - pair)) // 2
        chunk = lax.rem(me + between * (3 - 2 * odd) + 2 * last_pair, parts)
        side = odd + third * (1 - 2 * odd)
        return chunk, side

    def score(unit, query_tile, key_tile, keys):
        head, _ = units[unit]
        return jnp.dot(k_sc[key_tile, head, :keys], q_sc[query_tile, unit], preferred_element_type=F32)

    def absorb(unit, scores, query_tile, key_tile, causal):
        head, piece = units[unit]
        keys = scores.shape[0]
        key_row = lax.broadcasted_iota(jnp.int32, (keys, span), 0)
        allowed = key_row >= start_ref[query_tile, 0:1, piece * span:(piece + 1) * span] - key_tile * rows
        if causal:
            allowed = allowed & (key_row <= lax.broadcasted_iota(jnp.int32, (keys, span), 1) + piece * span)
        scores = jnp.where(allowed, scores, NEG)
        old_max = m_sc[query_tile, unit:unit + 1]
        new_max = jnp.maximum(old_max, jnp.max(scores, axis=0, keepdims=True))
        prob = jnp.exp(scores - new_max)
        fade = jnp.exp(old_max - new_max)
        m_sc[query_tile, unit:unit + 1] = new_max
        l_sc[query_tile, unit:unit + 1] = fade * l_sc[query_tile, unit:unit + 1] + jnp.sum(prob, axis=0, keepdims=True)
        value = v_sc[key_tile, head * head_dim:(head + 1) * head_dim, :keys]
        part = jnp.dot(value, prob.astype(BF16), preferred_element_type=F32)
        acc_sc[query_tile, unit] = acc_sc[query_tile, unit] * fade + part

    def block(query_tile, key_tile, following):
        diagonal = following is None

        def keys_of(unit):
            return (units[unit][1] + 1) * span if diagonal else rows

        waiting = [s_sc[unit, :keys_of(unit)] for unit in range(AHEAD)]
        for unit in range(len(units)):
            ahead = unit + AHEAD
            if ahead < len(units):
                waiting.append(score(ahead, query_tile, key_tile, keys_of(ahead)))
            elif not diagonal:
                s_sc[ahead - len(units)] = score(ahead - len(units), following[0], following[1], rows)
            absorb(unit, waiting.pop(0), query_tile, key_tile, diagonal)

    def arrive(index, carry):
        chunk, side = tile_of(index)
        tile = 2 * chunk + side

        @pl.when(index == 1)
        def _():
            if first:
                out.onward()
            for fetch in fetches[1:2]:
                fetch.start()

        @pl.when(index == 2)
        def _():
            rows_in['right_low'].wait_recv()
            rows_in['on_right'].start()

        @pl.when(index == 3)
        def _():
            rows_in['left_high'].wait_recv()
            rows_in['on_left'].start()

        @pl.when(index == 4)
        def _():
            rows_in['right_high'].wait_recv()
            for fetch in fetches[:1]:
                fetch.onward()
                fetch.share_near()
            if first:
                out.share_near()
                out.share_far()

        @pl.when(index == 5)
        def _():
            rows_in['left_low'].wait_recv()

        @pl.when(index == 6)
        def _():
            rows_in['on_right'].wait_recv()

        @pl.when(index == 7)
        def _():
            rows_in['on_left'].wait_recv()

        x = hbuf[chunk, pl.ds(pl.multiple_of(side * rows, rows), rows)]
        qkv_rows = lax.dot_general(w_sc[...], x, NT, preferred_element_type=F32)
        cosines = cos_ref[tile]
        sines = sin_ref[tile]

        def rotate(base):
            one = qkv_rows[base:base + half_dim]
            two = qkv_rows[base + half_dim:base + head_dim]
            return jnp.concatenate([one * cosines - two * sines, two * cosines + one * sines], axis=0)

        for head in range(heads):
            base = head * head_dim
            query = (rotate(base).astype(BF16).astype(F32) * scale).astype(BF16)
            for piece in range(pieces):
                q_sc[tile, head * pieces + piece] = query[:, piece * span:(piece + 1) * span]
            k_sc[tile, head] = rotate(width + base).T.astype(BF16)
        v_sc[tile] = qkv_rows[2 * width:3 * width].astype(BF16)
        m_sc[tile] = jnp.full(m_sc.shape[1:], NEG, F32)
        l_sc[tile] = jnp.zeros(l_sc.shape[1:], F32)
        acc_sc[tile] = jnp.zeros(acc_sc.shape[1:], F32)

        def ordered(other):
            other_chunk, other_side = tile_of(other)
            other_tile = 2 * other_chunk + other_side
            ahead = (tile - other_tile + tiles) // tiles
            upper = other_tile + ahead * (tile - other_tile)
            return upper, tile + other_tile - upper

        upper, lower = ordered(jnp.int32(0))
        for unit in range(AHEAD):
            s_sc[unit] = score(unit, upper, lower, rows)

        def pair(other, inner):
            query_tile, key_tile = ordered(other)
            block(query_tile, key_tile, ordered(other + 1))
            return inner

        lax.fori_loop(0, index, pair, 0)
        block(tile, tile, None)
        return carry

    lax.fori_loop(0, tiles, arrive, 0)
    wo_copy = pltpu.make_async_copy(out_all, wo_ref, local_sem.at[5])
    if first:
        out.finish()
    wo_copy.start()
    for tile in range(tiles):
        for unit, (head, piece) in enumerate(units):
            top = head * head_dim
            edge = (tile % 2) * rows + piece * span
            o_all[tile // 2, top:top + head_dim, edge:edge + span] = (acc_sc[tile, unit] / l_sc[tile, unit:unit + 1]).astype(BF16)

    exchange = exchange_heads(wire, 15, o_all, obuf, relay, me, left, right, far)
    for copy in exchange[:4]:
        copy.start()
    exchange[0].wait_recv()
    exchange[4].start()
    exchange[1].wait_recv()
    exchange[5].start()
    for fetch in fetches[1:]:
        fetch.onward()
        fetch.share_near()
    for fetch in fetches[:1]:
        fetch.share_far()
    wo_copy.wait()
    chunk = min(256, tokens)

    def project(sources, last):
        def step(index, carry):
            lanes = pl.ds(pl.multiple_of(index * chunk, chunk), chunk)
            total = None
            for source, piece in sources:
                weight = wo_ref[:, source].reshape(hidden, width)
                term = jnp.dot(weight, piece[:, lanes], preferred_element_type=F32)
                total = term if total is None else total + term
            residual = (res_ref[lanes] if last else r_ref[lanes].astype(F32)) + total.T
            res_ref[lanes] = residual
            if last:
                h_ref[lanes] = rms_norm(residual, gain_mlp[layer:layer + 1])
            return carry

        lax.fori_loop(0, tokens // chunk, step, 0)

    project([(me, o_all.at[me])], False)
    exchange[2].wait_recv()
    exchange[3].wait_recv()
    exchange[4].wait_recv()
    exchange[5].wait_recv()
    project([(left, obuf.at[0]), (right, obuf.at[1]), (far, obuf.at[2])], True)

    for fetch in fetches[1:]:
        fetch.share_far()
    for fetch in fetches:
        fetch.finish()
    for copy in exchange + list(rows_in.values()):
        copy.wait_send()
    if first:
        for copy in small + onward:
            copy.wait_send()
        local[1].wait()


def attend(first, layer, parts, shards, heads, head_dim, residual, gain_attn, gain_mlp, side_inputs, experts, fetch_keys, gathered_shape, ints_shape):
    tokens, hidden = residual.shape
    rows = tokens // 2
    width = heads * head_dim
    tiles = 2 * parts
    span = min(256, rows)
    units = heads * rows // span
    depth = hidden // shards
    num_layers = gain_attn.shape[0]
    anywhere = pl.BlockSpec(memory_space=pl.ANY)
    vmem = pl.BlockSpec(memory_space=pltpu.VMEM)
    num_fetch = len(fetch_keys)
    in_specs = [vmem] * 3 + ([vmem] * 8 if first else [anywhere] * 5) + [anywhere] * 3
    out_shape = [jax.ShapeDtypeStruct((tokens, hidden), F32), jax.ShapeDtypeStruct((tokens, hidden), BF16)]
    out_specs = [vmem, vmem]
    tables = [((tiles, head_dim // 2, rows), F32), ((tiles, head_dim // 2, rows), F32), ((tiles, 8, rows), jnp.int32)]
    if first:
        out_shape += [
            jax.ShapeDtypeStruct((parts,) + ints_shape, jnp.int32),
            jax.ShapeDtypeStruct((parts,) + ints_shape, F32),
            jax.ShapeDtypeStruct((shards, 3 * width, depth), BF16),
            jax.ShapeDtypeStruct((shards, parts, depth, width), BF16),
            jax.ShapeDtypeStruct((num_layers, 3 * width, depth), BF16),
            jax.ShapeDtypeStruct((num_layers, parts, depth, width), BF16),
        ] + [jax.ShapeDtypeStruct(shape, dtype) for shape, dtype in tables]
        out_specs += [vmem, vmem] + [anywhere] * 4 + [vmem] * 3
    out_shape += [jax.ShapeDtypeStruct((shards,) + gathered_shape, BF16)] * num_fetch
    out_specs += [anywhere] * num_fetch
    scratch = [
        pltpu.VMEM((parts,) + ints_shape, jnp.int32),
        pltpu.VMEM((parts,) + ints_shape, F32),
        pltpu.VMEM((num_layers, 3 * width, depth), BF16),
        pltpu.VMEM((num_layers, depth, width), BF16),
    ] if first else [pltpu.VMEM(shape, dtype) for shape, dtype in tables]
    copies = 41 + num_fetch * ShardGather.COPIES
    if num_fetch:
        scratch += [pltpu.VMEM((num_fetch, shards) + gathered_shape, BF16), pltpu.SemaphoreType.DMA((num_fetch, 1 + shards))]
    scratch += [
        pltpu.VMEM((parts, tokens, hidden), BF16),
        pltpu.VMEM((shards, 3 * width, depth), BF16),
        pltpu.VMEM((3 * width, hidden), BF16),
        pltpu.VMEM((tiles, units, head_dim, span), BF16),
        pltpu.VMEM((tiles, heads, rows, head_dim), BF16),
        pltpu.VMEM((tiles, width, rows), BF16),
        pltpu.VMEM((tiles, max(8, units), span), F32),
        pltpu.VMEM((tiles, max(8, units), span), F32),
        pltpu.VMEM((tiles, units, head_dim, span), F32),
        pltpu.VMEM((AHEAD, rows, span), F32),
        pltpu.VMEM((parts, width, tokens), BF16),
        pltpu.VMEM((3, width, tokens), BF16),
        pltpu.VMEM((2, width // 2, tokens), BF16),
        pltpu.VMEM((shards, parts, depth, width), BF16),
        pltpu.SemaphoreType.DMA((copies,)),
        pltpu.SemaphoreType.DMA((copies,)),
        pltpu.SemaphoreType.DMA((6,)),
    ]
    seq_len = parts * tokens
    return pl.pallas_call(
        functools.partial(attend_kernel, first, layer, parts, shards, heads, head_dim, tuple(fetch_keys)),
        in_specs=in_specs,
        out_specs=out_specs,
        out_shape=out_shape,
        scratch_shapes=scratch,
        compiler_params=pltpu.CompilerParams(collective_id=2 * layer, has_side_effects=True, vmem_limit_bytes=VMEM_LIMIT),
        cost_estimate=pl.CostEstimate(flops=2 * seq_len * seq_len * width + 8 * seq_len * hidden * width, bytes_accessed=8 * seq_len * hidden, transcendentals=seq_len * seq_len * heads // 2),
        name='attend',
    )(residual, gain_attn, gain_mlp, *side_inputs, *experts)


def mix_kernel(layer, parts, shards, late_keys, next_keys, late_mats, *refs):
    refs = list(refs)
    num_late = len(late_keys)
    num_next = len(next_keys)
    r_ref, h_ref, ints_ref, gates_ref = refs[:4]
    del refs[:4]
    given = refs[:6 - num_late]
    del refs[:6 - num_late]
    late_own = own_blocks(refs[:3], late_keys)
    next_own = own_blocks(refs[:3], next_keys)
    del refs[:3]
    if next_keys:
        next_own += [refs[0].at[layer + 1], refs[1].at[layer + 1]]
        del refs[:2]
        num_next += 2
    res_ref = refs.pop(0)
    late_all = refs[:num_late]
    del refs[:num_late]
    next_all = refs[:num_next]
    del refs[:num_next]
    hbuf, wbuf, acc, inbox, route, send_sem, recv_sem, w_sem, local_sem = refs
    mats = list(given)
    for position, ref in zip(late_mats, late_all):
        mats.insert(position, ref)

    me, left, right, _ = ring('mp', parts)
    to_left, to_right = {'mp': left}, {'mp': right}
    wire = Wire(send_sem, recv_sem)
    _, group, depth, ffn = mats[0].shape
    num_experts = 2 * group
    tokens, hidden = res_ref.shape
    half = tokens // 2
    low, high = pl.ds(0, half), pl.ds(half, half)
    steps = 16 * group
    waits_late = bool(late_keys)
    gate_step = (8 if waits_late else 4) * group - (SLOTS - 1)

    def place(step):
        turn = lax.div(step, group)
        odd = lax.rem(turn, 2)
        since = {edge: lax.div(turn + 16 - edge, 16) for edge in (4, 6, 8, 14)}
        main = lax.div(turn, 2)
        if waits_late:
            buffer = turn + 2 * since[4] - 4 * since[6] - 4 * since[8] - 8 * since[14]
            late = since[8]
        else:
            buffer = turn - 2 * since[4] + since[6] * (main + 3 - turn) + since[14] * (turn - 15 - main)
            late = since[4] * (1 - since[6]) + since[6] * (1 - since[14]) * odd + since[14]
        return turn, buffer, late, lax.rem(step, group)

    def weight_copies(step, side):
        _, _, _, expert = place(step)
        slot = lax.rem(step, SLOTS)
        return [pltpu.make_async_copy(mats[2 * index + side].at[:, expert], wbuf.at[slot, index], w_sem.at[slot, index]) for index in range(3)]

    def start_weights(step):
        _, _, late, _ = place(step)
        for side in range(2):

            @pl.when(late == side)
            def _(side=side):
                for copy in weight_copies(step, side):
                    copy.start()

    late_fetch = [ShardGather(wire, 12 + index * ShardGather.COPIES, own, blocks, shards, local_sem.at[index]) for index, (own, blocks) in enumerate(zip(late_own, late_all))]
    base = 12 + num_late * ShardGather.COPIES
    next_fetch = [ShardGather(wire, base + index * ShardGather.COPIES, own, blocks, shards, local_sem.at[num_late + index]) for index, (own, blocks) in enumerate(zip(next_own, next_all))]
    for step in range(SLOTS - 1):
        start_weights(jnp.int32(step))
    meet([to_left, to_right] + (tok_devices(shards) if late_fetch or next_fetch else []))
    rows_in = ring_gather(wire, 0, h_ref, hbuf, 'mp', left, right, me)
    for name in FIRST:
        rows_in[name].start()
    for fetch in late_fetch:
        fetch.start()
    hbuf[me] = h_ref[...]
    expert_row = lax.broadcasted_iota(jnp.int32, (num_experts, 1), 0)
    for part in range(parts):
        share = jnp.zeros((num_experts, tokens), F32)
        for choice in range(2):
            share = share + jnp.where(ints_ref[part, 1 + choice:2 + choice] == expert_row, gates_ref[part, choice:choice + 1], 0.0)
        route[part] = share.T

    sends = {
        2: wire.copy(6, acc.at[2], inbox.at[0], to_left),
        3: wire.copy(7, acc.at[3], inbox.at[1], to_right),
        4: wire.copy(8, acc.at[4], inbox.at[2], to_right),
        5: wire.copy(9, acc.at[5], inbox.at[3], to_left),
        6: wire.copy(10, acc.at[6], inbox.at[4], to_right),
        7: wire.copy(11, acc.at[7], inbox.at[5], to_left),
    }
    tile_rows = min(256, half)
    tiles = half // tile_rows
    lane = lax.broadcasted_iota(jnp.int32, (tile_rows, num_experts), 1)

    def rows_low_right():
        rows_in['right_low'].wait_recv()
        rows_in['on_right'].start()
        for fetch in late_fetch[:1]:
            fetch.onward()

    def rows_high_left():
        rows_in['left_high'].wait_recv()
        rows_in['on_left'].start()
        for fetch in late_fetch[1:2]:
            fetch.onward()
        for fetch in late_fetch[:1]:
            fetch.share_near()

    def rows_low_left():
        rows_in['left_low'].wait_recv()
        for fetch in late_fetch[2:]:
            fetch.onward()
        for fetch in late_fetch[1:2]:
            fetch.share_near()

    def rows_high_right():
        rows_in['right_high'].wait_recv()
        for fetch in late_fetch[2:]:
            fetch.share_near()

    def rows_far_low():
        rows_in['on_right'].wait_recv()
        for fetch in late_fetch[:1]:
            fetch.share_far()

    def rows_far_high():
        rows_in['on_left'].wait_recv()
        for fetch in late_fetch[1:]:
            fetch.share_far()

    def next_near():
        for fetch in next_fetch:
            fetch.onward()
            fetch.share_near()

    def sums():
        sends[4].wait_recv()
        acc[6] += inbox[2]
        sends[6].start()
        sends[5].wait_recv()
        acc[7] += inbox[3]
        sends[7].start()
        for fetch in next_fetch:
            fetch.share_far()

    if waits_late:
        fresh = (0, 1, 2, 3, 4, 5, 6, 7)
        events = {
            2: [rows_low_right],
            3: [rows_high_left],
            4: [rows_low_left],
            5: [rows_high_right],
            6: [rows_far_low],
            7: [rows_far_high],
            9: [sends[2].start],
            10: [sends[3].start],
            11: [sends[4].start],
            12: [sends[5].start, next_near],
            14: [sums],
        }
    else:
        fresh = (0, 1, 2, 3, 6, 8, 10, 12)
        events = {
            2: [rows_low_right],
            3: [rows_high_left],
            5: [sends[2].start],
            6: [sends[3].start, rows_far_low],
            8: [sends[4].start, rows_far_high],
            10: [sends[5].start, rows_low_left, next_near],
            12: [rows_high_right],
            14: [sums],
        }

    def begin(turn, buffer):
        clear = turn == fresh[0]
        for other in fresh[1:]:
            clear = clear | (turn == other)

        @pl.when(clear)
        def _():
            acc[buffer] = jnp.zeros((half, hidden), F32)

        for when, actions in events.items():

            @pl.when(turn == when)
            def _(actions=actions):
                for action in actions:
                    action()

    def expert_step(step, carry):
        turn, buffer, late, index = place(step)
        slot = lax.rem(step, SLOTS)
        expert = late * group + index
        pair = lax.div(buffer, 2)
        side = lax.rem(buffer, 2)
        odd = lax.rem(pair, 2)
        upper = lax.div(pair, 2)
        shift = odd * (upper * (1 + 2 * side) + (1 - upper) * (3 - 2 * side)) + (1 - odd) * 2 * upper
        source = lax.rem(me + shift, parts)
        start = pl.multiple_of(side * half, half)

        if late_fetch or next_fetch:

            @pl.when(step == gate_step)
            def _():
                for fetch in late_fetch:
                    fetch.finish()
                for fetch in next_fetch:
                    fetch.start()

        @pl.when(step + SLOTS - 1 < steps)
        def _():
            start_weights(step + SLOTS - 1)

        @pl.when(index == 0)
        def _():
            begin(turn, buffer)

        for copy in weight_copies(step, 0):
            copy.wait()

        def activate(tile):
            gate_w = wbuf[slot, 0].reshape(hidden, ffn)
            up_w = wbuf[slot, 1].reshape(hidden, ffn)
            x = hbuf[source, pl.ds(start + tile * tile_rows, tile_rows)]
            gate_pre = jnp.dot(x, gate_w, preferred_element_type=F32)
            up_pre = jnp.dot(x, up_w, preferred_element_type=F32)
            return (gate_pre * (1.0 / (1.0 + jnp.exp(-gate_pre))) * up_pre).astype(BF16)

        def contract(tile, act):
            down_w = wbuf[slot, 2].reshape(hidden, ffn)
            part_share = route[source, pl.ds(start + tile * tile_rows, tile_rows)]
            share = jnp.sum(jnp.where(lane == expert, part_share, 0.0), axis=1, keepdims=True)
            mixed = lax.dot_general(act, down_w, NT, preferred_element_type=F32)
            acc[buffer, tile * tile_rows:(tile + 1) * tile_rows] += share * mixed

        act = activate(0)
        for tile in range(tiles):
            following = activate(tile + 1) if tile + 1 < tiles else None
            contract(tile, act)
            act = following
        return carry

    lax.fori_loop(0, steps, expert_step, 0)

    sends[2].wait_recv()
    res_ref[low] = r_ref[low] + acc[0] + inbox[0]
    sends[3].wait_recv()
    res_ref[high] = r_ref[high] + acc[1] + inbox[1]
    sends[6].wait_recv()
    res_ref[low] += inbox[4]
    sends[7].wait_recv()
    res_ref[high] += inbox[5]
    for copy in list(rows_in.values()) + list(sends.values()):
        copy.wait_send()
    for fetch in next_fetch:
        fetch.finish()


def mix(layer, parts, shards, residual, normed, ints_all, gates_all, weights, experts, late_keys, late_mats, next_keys, attention_packs):
    tokens, hidden = residual.shape
    group, depth, ffn = weights[0].shape[1:]
    half = tokens // 2
    anywhere = pl.BlockSpec(memory_space=pl.ANY)
    vmem = pl.BlockSpec(memory_space=pltpu.VMEM)
    packs = attention_packs if next_keys else []
    num_fetch = len(late_keys) + len(next_keys) + len(packs)
    copies = 12 + num_fetch * ShardGather.COPIES
    return pl.pallas_call(
        functools.partial(mix_kernel, layer, parts, shards, tuple(late_keys), tuple(next_keys), late_mats),
        in_specs=[vmem] * 4 + [anywhere] * (len(weights) + 3 + len(packs)),
        out_specs=[vmem] + [anywhere] * num_fetch,
        out_shape=[jax.ShapeDtypeStruct((tokens, hidden), F32)]
        + [jax.ShapeDtypeStruct((shards, group, depth, ffn), BF16)] * (len(late_keys) + len(next_keys))
        + [jax.ShapeDtypeStruct((shards,) + pack.shape[1:], BF16) for pack in packs],
        scratch_shapes=[
            pltpu.VMEM((parts, tokens, hidden), BF16),
            pltpu.VMEM((SLOTS, 3, shards, depth, ffn), BF16),
            pltpu.VMEM((8, half, hidden), F32),
            pltpu.VMEM((6, half, hidden), F32),
            pltpu.VMEM((parts, tokens, 2 * group), F32),
            pltpu.SemaphoreType.DMA((copies,)),
            pltpu.SemaphoreType.DMA((copies,)),
            pltpu.SemaphoreType.DMA((SLOTS, 3)),
            pltpu.SemaphoreType.DMA((max(1, num_fetch),)),
        ],
        compiler_params=pltpu.CompilerParams(collective_id=2 * layer + 1, has_side_effects=True, vmem_limit_bytes=VMEM_LIMIT),
        cost_estimate=pl.CostEstimate(
            flops=12 * parts * tokens * hidden * ffn * group,
            bytes_accessed=96 * group * hidden * ffn,
            transcendentals=2 * parts * tokens * ffn * group,
        ),
        name='mix',
    )(residual, normed, ints_all, gates_all, *weights, *experts, *packs)


def solution(mesh):
    token_spec = P(('rep', 'tok', 'mp'))
    row_spec = P(('rep', 'tok', 'mp'), None)
    head_weight = P(None, 'tok', 'mp', None)
    in_specs = (row_spec, token_spec, row_spec, row_spec, head_weight, head_weight, head_weight, P(None, 'mp', None, 'tok'), P(None, None, 'tok', 'mp'), P(None, None, 'tok', 'mp'), P(None, None, 'mp', 'tok'), P(None, None), P(None, None))
    parts = mesh.shape['mp']
    shards = mesh.shape['tok']

    def device_step(hidden_in, seg_ids, expert_ids, expert_gates, w_query, w_key, w_value, w_out, w_gate, w_up, w_down, gain_attn, gain_mlp):
        num_layers, depth, heads, head_dim = w_query.shape
        tokens, _ = hidden_in.shape
        group = w_gate.shape[1] // 2
        width = heads * head_dim
        ffn = w_gate.shape[-1]

        experts_local = [w_gate, w_up, jnp.swapaxes(w_down, 2, 3)]
        halves = [[(layer, matrix, side) for matrix in range(3) for side in range(2)] for layer in range(num_layers)]

        qkv_local = [jnp.transpose(w, (0, 2, 3, 1)).reshape(num_layers, width, depth) for w in (w_query, w_key, w_value)]
        out_local = w_out.reshape(num_layers, width, depth)
        inv_freq = jnp.power(ROPE_BASE, -jnp.arange(head_dim // 2, dtype=F32) * 2.0 / head_dim)[:, None]

        shape = (group, depth, ffn)
        gathered = {}
        residual = hidden_in
        side_inputs = [inv_freq, seg_ids[None, :], expert_ids.T, expert_gates.T] + qkv_local + [out_local]
        plan = {}
        for layer, matrix, side in halves[0][::2]:
            gathered[layer, matrix, side] = lax.all_gather(experts_local[matrix][layer, :group], 'tok', axis=0)
        for layer in range(num_layers):
            first = layer == 0
            fetch = plan.get(layer, [])
            fetch = [key for key in fetch if key not in gathered]
            outs = attend(first, layer, parts, shards, heads, head_dim, residual, gain_attn, gain_mlp, side_inputs, experts_local, fetch, shape, (8, tokens))
            residual, normed = outs[:2]
            outs = outs[2:]
            if first:
                ints_all, gates_all, _, _, qkv_rest, out_rest = outs[:6]
                tables = list(outs[6:9])
                outs = outs[9:]
            gathered.update(zip(fetch, outs))
            late = [key for key in halves[layer] if key not in gathered]
            late_mats = tuple(halves[layer].index(key) for key in late)
            weights = [gathered[key] for key in halves[layer] if key in gathered]
            following = []
            if layer + 1 < num_layers:
                following = halves[layer + 1][:4]
                plan[layer + 1] = halves[layer + 1][4:]
            outs = mix(layer, parts, shards, residual, normed, ints_all, gates_all, weights, experts_local, late, late_mats, following, [qkv_rest, out_rest])
            residual = outs[0]
            gathered.update(zip(late + following, outs[1:]))
            side_inputs = tables + list(outs[-2:])
        return residual

    return jax.shard_map(device_step, mesh=mesh, in_specs=in_specs, out_specs=row_spec, check_vma=False)
```
